128 devices in a mesh: dp: 64 (over z, y, x), tp: 2 (over core).
Axes of the slice: x: 4, y: 4, z: 4, core: 2. Of those that a mesh axis runs over, the one named last changes fastest.
Arguments:
- x_teach: bfloat16 [128, 128, 1024], P('dp', 'tp')
- x_stud: bfloat16 [128, 128, 384], P(('dp', 'tp'))
- w_up_t: bfloat16 [32, 1024, 4096], P(None, None, 'tp')
- w_down_t: bfloat16 [32, 4096, 1024], P(None, 'tp')
- gain_t: float32 [32, 1024], replicated
- head_t: bfloat16 [1024, 30592], P(None, 'tp')
- w_up_s: bfloat16 [2, 384, 1536], replicated
- w_down_s: bfloat16 [2, 1536, 384], replicated
- gain_s: float32 [2, 384], replicated
- proj_s: bfloat16 [2, 384, 1024], replicated
- head_s: bfloat16 [384, 30592], replicated
Outputs:
- output 1: float32 [], replicated
- output 2: float32 [2, 384, 1536], replicated
- output 3: float32 [2, 1536, 384], replicated
- output 4: float32 [2, 384], replicated
- output 5: float32 [2, 384, 1024], replicated
- output 6: float32 [384, 30592], replicated
All inputs are finite; a program needn't handle non-finite values.
Results may differ from the reference program's by a relative error of at most 0.00469935.
Values are sent between devices in bfloat16 or wider.
A program may use at most 1.5 GiB of HBM per device.

```python
import jax
import jax.numpy as jnp
from jax import lax

BATCH = 128
SEQ_LEN = 128
D_TEACH = 1024
D_STUD = 384
VOCAB_SIZE = 30592
FEAT_LAYERS = 2
TEACH_LAYERS = 32
NORM_EPS = 1e-6


def setup_inputs(seed: int = 0) -> dict:
    rng_keys = jax.random.split(jax.random.key(seed), 11)
    ff_teach = 4 * D_TEACH
    ff_stud = 4 * D_STUD

    def normal_bf16(rng_key, arr_shape, std_scale):
        return (jax.random.normal(rng_key, arr_shape, jnp.float32) * std_scale).astype(jnp.bfloat16)

    return {
        'x_teach': normal_bf16(rng_keys[0], (BATCH, SEQ_LEN, D_TEACH), 1.0),
        'x_stud': normal_bf16(rng_keys[1], (BATCH, SEQ_LEN, D_STUD), 1.0),
        'w_up_t': normal_bf16(rng_keys[2], (TEACH_LAYERS, D_TEACH, ff_teach), D_TEACH ** -0.5),
        'w_down_t': normal_bf16(rng_keys[3], (TEACH_LAYERS, ff_teach, D_TEACH), ff_teach ** -0.5),
        'gain_t': jax.random.uniform(rng_keys[4], (TEACH_LAYERS, D_TEACH), jnp.float32, 0.5, 1.5),
        'head_t': normal_bf16(rng_keys[5], (D_TEACH, VOCAB_SIZE), D_TEACH ** -0.5),
        'w_up_s': normal_bf16(rng_keys[6], (FEAT_LAYERS, D_STUD, ff_stud), D_STUD ** -0.5),
        'w_down_s': normal_bf16(rng_keys[7], (FEAT_LAYERS, ff_stud, D_STUD), ff_stud ** -0.5),
        'gain_s': jax.random.uniform(rng_keys[8], (FEAT_LAYERS, D_STUD), jnp.float32, 0.5, 1.5),
        'proj_s': normal_bf16(rng_keys[9], (FEAT_LAYERS, D_STUD, D_TEACH), D_STUD ** -0.5),
        'head_s': normal_bf16(rng_keys[10], (D_STUD, VOCAB_SIZE), D_STUD ** -0.5),
    }


def rms_norm(values):
    vals32 = values.astype(jnp.float32)
    return vals32 * lax.rsqrt(jnp.mean(vals32 * vals32, axis=-1, keepdims=True) + NORM_EPS)


def as_bf16(values):
    return values.astype(jnp.bfloat16).astype(jnp.float32)


def gelu_tanh(values):
    return jax.nn.gelu(values, approximate=True)


def teacher_tokens(teach_blk, w_up_t, w_down_t, gain_t, head_t):
    per_feat = TEACH_LAYERS // FEAT_LAYERS
    up_groups = w_up_t.reshape(FEAT_LAYERS, per_feat, D_TEACH, 4 * D_TEACH)
    down_groups = w_down_t.reshape(FEAT_LAYERS, per_feat, 4 * D_TEACH, D_TEACH)
    gain_groups = gain_t.reshape(FEAT_LAYERS, per_feat, D_TEACH)

    def one_layer(hidden, layer_w):
        w_up, w_down, gain_row = layer_w
        normed = (rms_norm(hidden) * gain_row).astype(jnp.bfloat16)
        hidden_act = gelu_tanh(jnp.dot(normed, w_up, preferred_element_type=jnp.float32)).astype(jnp.bfloat16)
        layer_out = jnp.dot(hidden_act, w_down, preferred_element_type=jnp.float32).astype(jnp.bfloat16)
        return hidden + layer_out, None

    def one_feature(hidden, group_w):
        hidden, _ = lax.scan(one_layer, hidden, group_w)
        return hidden, hidden

    hidden, features = lax.scan(one_feature, teach_blk, (up_groups, down_groups, gain_groups))
    teach_logits = jnp.dot(rms_norm(hidden).astype(jnp.bfloat16), head_t, preferred_element_type=jnp.float32)
    return features, teach_logits


def student_loss(params, stud_blk, features, teach_logits, feat_coef, kl_coef):
    w_up, w_down, gains, proj, head_w = params

    def one_block(residual, layer_w):
        up_j, down_j, gain_j, proj_j, feat_j = layer_w
        normed = as_bf16(rms_norm(residual) * gain_j)
        hidden_act = as_bf16(gelu_tanh(jnp.dot(normed, up_j, preferred_element_type=jnp.float32)))
        residual = residual + jnp.dot(hidden_act, down_j, preferred_element_type=jnp.float32)
        proj_in = as_bf16(rms_norm(residual))
        feat_err = jnp.dot(proj_in, proj_j, preferred_element_type=jnp.float32) - feat_j.astype(jnp.float32)
        return residual, jnp.sum(feat_err * feat_err)

    residual, err_sums = lax.scan(one_block, stud_blk.astype(jnp.float32), (w_up, w_down, gains, proj, features))
    stud_logits = jnp.dot(as_bf16(rms_norm(residual)), head_w, preferred_element_type=jnp.float32)
    log_teach = jax.nn.log_softmax(teach_logits, axis=-1)
    log_stud = jax.nn.log_softmax(stud_logits, axis=-1)
    kl_sum = jnp.sum(jnp.exp(log_teach) * (log_teach - log_stud))
    return feat_coef * jnp.sum(err_sums) + kl_coef * kl_sum


def reference(x_teach, x_stud, w_up_t, w_down_t, gain_t, head_t, w_up_s, w_down_s, gain_s, proj_s, head_s):
    block_len = 128
    n_tokens = BATCH * SEQ_LEN
    n_blocks = n_tokens // block_len
    teach_blocks = x_teach.reshape(n_blocks, block_len, D_TEACH)
    stud_blocks = x_stud.reshape(n_blocks, block_len, D_STUD)
    params = (w_up_s.astype(jnp.float32), w_down_s.astype(jnp.float32), gain_s.astype(jnp.float32),
              proj_s.astype(jnp.float32), head_s.astype(jnp.float32))
    feat_coef = 1.0 / (FEAT_LAYERS * n_tokens * D_TEACH)
    kl_coef = 1.0 / n_tokens
    loss_and_grad = jax.value_and_grad(student_loss)

    def one_block(scan_carry, token_blks):
        loss_acc, grad_acc = scan_carry
        teach_blk, stud_blk = token_blks
        features, teach_logits = teacher_tokens(teach_blk, w_up_t, w_down_t, gain_t, head_t)
        loss_val, grad_vals = loss_and_grad(params, stud_blk, features, teach_logits, feat_coef, kl_coef)
        return (loss_acc + loss_val, jax.tree.map(jnp.add, grad_acc, grad_vals)), None

    start_carry = (jnp.zeros((), jnp.float32), jax.tree.map(jnp.zeros_like, params))
    (total_loss, grad_vals), _ = lax.scan(one_block, start_carry, (teach_blocks, stud_blocks))
    grad_up, grad_down, grad_gain, grad_proj, grad_head = grad_vals
    return (total_loss, grad_up, grad_down, grad_gain, grad_proj, grad_head)
```

```python
import functools

import jax
import jax.numpy as jnp
from jax import lax
from jax.experimental import pallas as pl
from jax.experimental.pallas import tpu as pltpu
from jax.sharding import PartitionSpec as P

NORM_EPS = 1e-6
MESH = pl.DeviceIdType.MESH


def rms_parts(values):
    vals32 = values.astype(jnp.float32)
    inv_rms = lax.rsqrt(jnp.mean(vals32 * vals32, axis=-1, keepdims=True) + NORM_EPS)
    return vals32 * inv_rms, inv_rms


def rms_back(normed, inv_rms, grad_out):
    return inv_rms * (grad_out - normed * jnp.mean(grad_out * normed, axis=-1, keepdims=True))


def gelu_tanh(values):
    return jax.nn.gelu(values, approximate=True)


def gelu_back(pre_act, grad_out):
    return jax.vjp(gelu_tanh, pre_act)[1](grad_out)[0]


def mat_mul(subscripts, lhs_arr, rhs_arr):
    return jnp.einsum(subscripts, lhs_arr, rhs_arr, preferred_element_type=jnp.float32)


def gelu_act(u):
    inner = u * (0.7978845608028654 + 0.035677408136300125 * (u * u))
    half = 0.5 * u
    return half + half * jnp.tanh(inner)


def teacher_kernel(n_layers, feat_at, up_blk, dn_blk, slots_w,
                   x_ref, gain_ref, wup_hbm, wdn_hbm,
                   feat_ref, hout_ref,
                   h, nrm, act, wu, wd, part, got,
                   wsem, xsem, ssem, rsem):
    me = lax.axis_index('tp')
    peer = {'tp': 1 - me}
    rows, seq_half, d_model = x_ref.shape
    n_tok = 2 * seq_half
    d_ff = wu.shape[-1]
    n_up = d_ff // up_blk
    n_dn = d_model // dn_blk

    def up_copy(layer, slot):
        return pltpu.make_async_copy(wup_hbm.at[layer], wu.at[slot], wsem.at[0, slot])

    def down_copy(layer, slot):
        return pltpu.make_async_copy(wdn_hbm.at[layer], wd.at[slot], wsem.at[1, slot])

    for i in range(slots_w):
        up_copy(i, i).start()
        down_copy(i, i).start()

    barrier = pltpu.get_barrier_semaphore()
    pl.semaphore_signal(barrier, inc=1, device_id=peer, device_id_type=MESH)
    pl.semaphore_wait(barrier, 1)

    mine = pl.ds(pl.multiple_of(me * seq_half, seq_half), seq_half)
    xcopy = pltpu.make_async_remote_copy(
        src_ref=x_ref, dst_ref=h.at[:, mine], send_sem=xsem.at[0], recv_sem=xsem.at[1],
        device_id=peer, device_id_type=MESH)
    xcopy.start()
    h[:, mine] = x_ref[...]
    xcopy.wait()

    def p_copy(ck, slot, n):
        return pltpu.make_async_remote_copy(
            src_ref=part.at[ck, slot, n], dst_ref=got.at[ck, slot, n],
            send_sem=ssem.at[ck, slot, n], recv_sem=rsem.at[ck, slot, n],
            device_id=peer, device_id_type=MESH)

    def update(ck, slot):
        for n in range(n_dn):
            p_copy(ck, slot, n).wait()
            cols = slice(n * dn_blk, (n + 1) * dn_blk)
            total = part[ck, slot, n] + got[ck, slot, n]
            new = h[ck, :, cols].astype(jnp.float32) + total.astype(jnp.bfloat16).astype(jnp.float32)
            h[ck, :, cols] = new.astype(jnp.bfloat16)

    def layer_step(layer, _):
        slot = lax.rem(layer, 2)
        prev = 1 - slot
        ws = lax.rem(layer, slots_w)
        for ck in range(rows):
            @pl.when(layer > 0)
            def _():
                update(ck, prev)

            @pl.when((layer == feat_at) & (me == ck))
            def _():
                feat_ref[...] = h[ck]

            hv = h[ck].astype(jnp.float32)
            inv = lax.rsqrt(jnp.mean(hv * hv, axis=-1, keepdims=True) + NORM_EPS)
            nrm[...] = ((hv * inv) * gain_ref[pl.ds(layer, 1), :]).astype(jnp.bfloat16)
            if ck == 0:
                up_copy(layer, ws).wait()
            for n in range(n_up):
                cols = slice(n * up_blk, (n + 1) * up_blk)
                u = jnp.dot(nrm[...], wu[ws, :, cols], preferred_element_type=jnp.float32)
                act[:, cols] = gelu_act(u).astype(jnp.bfloat16)
            if ck == rows - 1:
                @pl.when(layer + slots_w < n_layers)
                def _():
                    up_copy(layer + slots_w, ws).start()
            if ck == 0:
                down_copy(layer, ws).wait()
            for n in range(n_dn):
                cols = slice(n * dn_blk, (n + 1) * dn_blk)
                part[ck, slot, n] = jnp.dot(act[...], wd[ws, :, cols], preferred_element_type=jnp.float32)
                p_copy(ck, slot, n).start()
            if ck == rows - 1:
                @pl.when(layer + slots_w < n_layers)
                def _():
                    down_copy(layer + slots_w, ws).start()
        return 0

    lax.fori_loop(0, n_layers, layer_step, 0)
    last = (n_layers - 1) % 2
    for ck in range(rows):
        update(ck, last)
        hout_ref[ck] = h[ck]


def teacher(x_teach, gain_t, w_up_t, w_down_t, feat_at, up_blk=2048, dn_blk=1024, slots_w=3, collective_id=0):
    n_layers, d_model, d_ff = w_up_t.shape
    rows, seq_half, _ = x_teach.shape
    n_tok = 2 * seq_half
    n_dn = d_model // dn_blk
    f32, bf = jnp.float32, jnp.bfloat16
    vm = pl.BlockSpec(memory_space=pltpu.VMEM)
    hb = pl.BlockSpec(memory_space=pl.ANY)
    flops = 2 * 2 * rows * n_tok * d_model * d_ff * n_layers
    return pl.pallas_call(
        functools.partial(teacher_kernel, n_layers, feat_at, up_blk, dn_blk, slots_w),
        out_shape=(jax.ShapeDtypeStruct((n_tok, d_model), bf), jax.ShapeDtypeStruct((rows, n_tok, d_model), bf)),
        in_specs=[vm, vm, hb, hb],
        out_specs=(vm, vm),
        scratch_shapes=[
            pltpu.VMEM((rows, n_tok, d_model), bf),
            pltpu.VMEM((n_tok, d_model), bf),
            pltpu.VMEM((n_tok, d_ff), bf),
            pltpu.VMEM((slots_w, d_model, d_ff), bf),
            pltpu.VMEM((slots_w, d_ff, d_model), bf),
            pltpu.VMEM((rows, 2, n_dn, n_tok, dn_blk), f32),
            pltpu.VMEM((rows, 2, n_dn, n_tok, dn_blk), f32),
            pltpu.SemaphoreType.DMA((2, slots_w)),
            pltpu.SemaphoreType.DMA((2,)),
            pltpu.SemaphoreType.DMA((rows, 2, n_dn)),
            pltpu.SemaphoreType.DMA((rows, 2, n_dn)),
        ],
        compiler_params=pltpu.CompilerParams(collective_id=collective_id, has_side_effects=True,
                                             vmem_limit_bytes=48 * 1024 * 1024),
        cost_estimate=pl.CostEstimate(flops=flops, bytes_accessed=4 * n_layers * d_model * d_ff, transcendentals=0),
        name='teacher',
    )(x_teach, gain_t, w_up_t, w_down_t)


def student_forward(x_stud, w_up_s, w_down_s, gain_s, proj_s, features):
    residual = x_stud.astype(jnp.float32)
    norm_cur, inv_cur = rms_parts(residual)
    saved_acts = []
    err_total = jnp.zeros((), jnp.float32)
    for layer_idx in range(w_up_s.shape[0]):
        normed = (norm_cur * gain_s[layer_idx]).astype(jnp.bfloat16)
        pre_act = mat_mul('bsd,df->bsf', normed, w_up_s[layer_idx])
        hidden_act = gelu_tanh(pre_act).astype(jnp.bfloat16)
        residual = residual + mat_mul('bsf,fd->bsd', hidden_act, w_down_s[layer_idx])
        norm_next, inv_next = rms_parts(residual)
        proj_in = norm_next.astype(jnp.bfloat16)
        feat_err = mat_mul('bsd,de->bse', proj_in, proj_s[layer_idx]) - features[layer_idx]
        err_total = err_total + jnp.sum(feat_err * feat_err)
        saved_acts.append((norm_cur, inv_cur, normed, pre_act, hidden_act, norm_next, inv_next, proj_in, feat_err))
        norm_cur, inv_cur = norm_next, inv_next
    return saved_acts, err_total


def student_backward(saved_acts, w_up_s, w_down_s, gain_s, proj_s, feat_coef, head_in_grad):
    n_layers = len(saved_acts)
    up_grads = []
    down_grads = []
    gain_grads = []
    proj_grads = []
    resid_grad = None
    for layer_idx in reversed(range(n_layers)):
        norm_cur, inv_cur, normed, pre_act, hidden_act, norm_next, inv_next, proj_in, feat_err = saved_acts[layer_idx]
        err_grad = (2.0 * feat_coef * feat_err).astype(jnp.bfloat16)
        proj_grads.append(mat_mul('bsd,bse->de', proj_in, err_grad))
        out_grad = mat_mul('bse,de->bsd', err_grad, proj_s[layer_idx])
        if resid_grad is None:
            resid_grad = rms_back(norm_next, inv_next, out_grad + head_in_grad)
        else:
            resid_grad = resid_grad + rms_back(norm_next, inv_next, out_grad)
        resid_bf = resid_grad.astype(jnp.bfloat16)
        down_grads.append(mat_mul('bsf,bsd->fd', hidden_act, resid_bf))
        act_grad = mat_mul('bsd,fd->bsf', resid_bf, w_down_s[layer_idx])
        pre_grad = gelu_back(pre_act, act_grad).astype(jnp.bfloat16)
        up_grads.append(mat_mul('bsd,bsf->df', normed, pre_grad))
        norm_grad = mat_mul('bsf,df->bsd', pre_grad, w_up_s[layer_idx])
        gain_grads.append(jnp.sum(norm_grad * norm_cur, axis=(0, 1)))
        if layer_idx > 0:
            resid_grad = resid_grad + rms_back(norm_cur, inv_cur, norm_grad * gain_s[layer_idx])
    return (jnp.stack(up_grads[::-1]), jnp.stack(down_grads[::-1]),
            jnp.stack(gain_grads[::-1]), jnp.stack(proj_grads[::-1]))


def solution(mesh):
    dp_size = mesh.shape['dp']
    tp_size = mesh.shape['tp']

    def local_step(x_teach, x_stud, w_up_t, w_down_t, gain_t, head_t, w_up_s, w_down_s, gain_s, proj_s, head_s):
        n_feat = w_up_s.shape[0]
        per_feat = w_up_t.shape[0] // n_feat
        feat_first, hidden = teacher(x_teach, gain_t, w_up_t, w_down_t, per_feat)
        own_row = lax.dynamic_slice_in_dim(hidden, lax.axis_index('tp'), 1, axis=0)
        features = [feat_first[None], own_row]
        final_full = rms_parts(hidden)[0].astype(jnp.bfloat16)
        teach_logits = mat_mul('bsd,dv->bsv', final_full, head_t)

        n_tokens = x_stud.shape[0] * x_stud.shape[1] * dp_size * tp_size
        feat_coef = 1.0 / (n_feat * n_tokens * head_t.shape[0])
        kl_coef = 1.0 / n_tokens
        saved_acts, err_total = student_forward(x_stud, w_up_s, w_down_s, gain_s, proj_s, features)
        head_in = saved_acts[-1][7]
        stud_full = lax.all_gather(head_in, 'tp', axis=0, tiled=True)
        vocab_part = head_t.shape[1]
        head_cols = lax.dynamic_slice_in_dim(head_s, lax.axis_index('tp') * vocab_part, vocab_part, axis=1)
        stud_logits = mat_mul('bsd,dv->bsv', stud_full, head_cols)
        peak_vals = lax.pmax(jnp.stack([jnp.max(teach_logits, axis=-1), jnp.max(stud_logits, axis=-1)]), 'tp')
        teach_exp = jnp.exp(teach_logits - peak_vals[0][..., None])
        stud_exp = jnp.exp(stud_logits - peak_vals[1][..., None])
        sum_vals = lax.psum(jnp.stack([jnp.sum(teach_exp, axis=-1), jnp.sum(stud_exp, axis=-1)]), 'tp')
        log_norms = peak_vals + jnp.log(sum_vals)
        teach_prob = teach_exp / sum_vals[0][..., None]
        stud_prob = stud_exp / sum_vals[1][..., None]
        log_ratio = teach_logits - stud_logits - (log_norms[0] - log_norms[1])[..., None]
        kl_local = jnp.sum(teach_prob * log_ratio)
        logit_grad = (kl_coef * (stud_prob - teach_prob)).astype(jnp.bfloat16)
        head_part = mat_mul('bsd,bsv->dv', stud_full, logit_grad)
        head_grad = lax.all_gather(lax.psum(head_part, 'dp'), 'tp', axis=1, tiled=True)
        full_in_grad = mat_mul('bsv,dv->bsd', logit_grad, head_cols)
        head_in_grad = lax.psum_scatter(full_in_grad, 'tp', scatter_dimension=0, tiled=True)
        local_grads = student_backward(saved_acts, w_up_s, w_down_s, gain_s, proj_s, feat_coef, head_in_grad)
        grad_up, grad_down, grad_gain, grad_proj = lax.psum(local_grads, ('dp', 'tp'))
        total_loss = lax.psum(feat_coef * err_total + kl_coef * kl_local, ('dp', 'tp'))
        return total_loss, grad_up, grad_down, grad_gain, grad_proj, head_grad

    in_specs = (P('dp', 'tp', None), P(('dp', 'tp'), None, None), P(None, None, 'tp'), P(None, 'tp', None),
                P(), P(None, 'tp'), P(), P(), P(), P(), P())
    out_specs = (P(), P(), P(), P(), P(), P())
    return jax.shard_map(local_step, mesh=mesh, in_specs=in_specs, out_specs=out_specs, check_vma=False)
```

```python
import functools

import jax
import jax.numpy as jnp
from jax import lax
from jax.experimental import pallas as pl
from jax.experimental.pallas import tpu as pltpu
from jax.sharding import PartitionSpec as P

NORM_EPS = 1e-6
MESH = pl.DeviceIdType.MESH
F32, BF16 = jnp.float32, jnp.bfloat16
DMA = pltpu.SemaphoreType.DMA
IN_VMEM = pl.BlockSpec(memory_space=pltpu.VMEM)
IN_HBM = pl.BlockSpec(memory_space=pl.ANY)
LANES = 128
SUBS = 8
SIDE = 4
MIB = 1 << 20
HERE, RIGHT, FAR, LEFT = range(SIDE)
X, Y, Z = AXES = tuple(range(SIDE - RIGHT))
PARTS = AXES
ORDERS = ((X, Y, Z), (Y, Z, X), (Z, X, Y))
CORES = PAIR = (0, 1)
WAYS = (RIGHT, LEFT)


def chip_coords():
    chip = lax.axis_index('dp')
    return lax.rem(chip, SIDE), lax.rem(chip // SIDE, SIDE), chip // (SIDE * SIDE)


def device(coords, core):
    x, y, z = coords
    return {'dp': (z * SIDE + y) * SIDE + x, 'tp': core}


def moved(coords, axis, step):
    out = list(coords)
    out[axis] = lax.rem(out[axis] + step, SIDE)
    return tuple(out)


def remote(src, dst, send_sem, recv_sem, target):
    return pltpu.make_async_remote_copy(src_ref=src, dst_ref=dst, send_sem=send_sem, recv_sem=recv_sem,
                                        device_id=target, device_id_type=MESH)


def greet(targets):
    barrier = pltpu.get_barrier_semaphore()
    for target in targets:
        pl.semaphore_signal(barrier, device_id=target, device_id_type=MESH)
    pl.semaphore_wait(barrier, len(targets))


def group_targets(coords, core):
    return [device(moved(coords, X, step), abs(core - flip)) for step in range(SIDE) for flip in CORES if step or flip]


def near_targets(coords, core):
    return [device(moved(coords, axis, step), core) for axis in AXES for step in WAYS] + [device(coords, 1 - core)]


def lane_slice(k, width):
    return slice(k * width, k * width + width)


def rms_unit(values):
    inv = lax.rsqrt(jnp.mean(values * values, axis=-1, keepdims=True) + NORM_EPS)
    return values * inv, inv


def rms_back(normed, inv_rms, grad_out):
    return inv_rms * (grad_out - normed * jnp.mean(grad_out * normed, axis=-1, keepdims=True))


GELU_C = 0.7978845608028654
GELU_K = 0.044715


def gelu_act(u):
    half = 0.5 * u
    return half + half * jnp.tanh(u * (GELU_C + (GELU_C * GELU_K) * (u * u)))


def gelu_slope(u):
    sq = u * u
    t = jnp.tanh(u * (GELU_C + (GELU_C * GELU_K) * sq))
    return 0.5 * (1 + t) + (0.5 * u) * (1 - t * t) * (GELU_C + (3 * GELU_C * GELU_K) * sq)


def dot(a, b):
    return jnp.dot(a, b, preferred_element_type=F32)


def dot_right_t(a, b):
    return lax.dot_general(a, b, (((1,), (1,)), ((), ())), preferred_element_type=F32)


def dot_left_t(a, b):
    return lax.dot_general(a, b, (((0,), (0,)), ((), ())), preferred_element_type=F32)


def student_layers(x_ref, gain_ref, up_ref, down_ref):
    residual = x_ref[...].astype(F32)
    unit, inv = rms_unit(residual)
    saved = []
    for j in range(up_ref.shape[0]):
        normed = (unit * gain_ref[j:j + 1, :]).astype(BF16)
        pre = dot(normed, up_ref[j])
        act = gelu_act(pre).astype(BF16)
        residual = residual + dot(act, down_ref[j])
        unit_next, inv_next = rms_unit(residual)
        saved.append((unit, inv, normed, pre, act, unit_next, inv_next))
        unit, inv = unit_next, inv_next
    return saved, unit.astype(BF16)


def teacher_kernel(feat_at, slots_w,
                   x_ref, xs_ref, gs_ref, ups_ref, dns_ref, gain_ref, wup_hbm, wdn_hbm,
                   feat_ref, last_ref, state_ref, group_ref,
                   h, nrm, act, wu, wd, part, got, r_own,
                   usem, dsem, xsend, xrecv, ssem, rsem, gsend, grecv):
    me = lax.axis_index('tp')
    coords = chip_coords()
    peer = device(coords, 1 - me)
    n_layers = gain_ref.shape[0]
    rows, seq_half, d_model = x_ref.shape

    def up_copy(layer, slot):
        return pltpu.make_async_copy(wup_hbm.at[layer], wu.at[slot], usem.at[slot])

    def down_copy(layer, slot):
        return pltpu.make_async_copy(wdn_hbm.at[layer], wd.at[slot], dsem.at[slot])

    for i in range(slots_w):
        up_copy(i, i).start()
        down_copy(i, i).start()
    targets = group_targets(coords, me)
    greet(targets)
    mine = pl.ds(pl.multiple_of(me * seq_half, seq_half), seq_half)
    xcopy = remote(x_ref, h.at[:, mine], xsend, xrecv, peer)
    xcopy.start()
    h[:, mine] = x_ref[...]

    _, head_in = student_layers(xs_ref, gs_ref, ups_ref, dns_ref)
    r_own[...] = head_in
    r_copies = [remote(r_own, group_ref.at[coords[X], me], gsend.at[i], grecv.at[i], target) for i, target in enumerate(targets)]
    for copy in r_copies:
        copy.start()
    group_ref[coords[X], me] = head_in
    xcopy.wait()

    def p_copy(ck, slot):
        return remote(part.at[ck, slot], got.at[ck, slot], ssem.at[ck, slot], rsem.at[ck, slot], peer)

    def update(ck, slot):
        p_copy(ck, slot).wait()
        total = part[ck, slot] + got[ck, slot]
        h[ck] = (h[ck].astype(F32) + total.astype(BF16).astype(F32)).astype(BF16)

    def layer_step(layer, _):
        slot = lax.rem(layer, len(PAIR))
        ws = lax.rem(layer, slots_w)
        for ck in range(rows):
            first, last = ck == 0, ck == rows - 1

            @pl.when(layer > 0)
            def _():
                update(ck, 1 - slot)

            @pl.when((layer == feat_at) & (me == ck))
            def _():
                feat_ref[...] = h[ck]

            unit, _ = rms_unit(h[ck].astype(F32))
            nrm[...] = (unit * gain_ref[pl.ds(layer, 1), :]).astype(BF16)
            if first:
                up_copy(layer, ws).wait()
            act[...] = gelu_act(dot(nrm[...], wu[ws])).astype(BF16)
            if last:
                @pl.when(layer + slots_w < n_layers)
                def _():
                    up_copy(layer + slots_w, ws).start()
            if first:
                down_copy(layer, ws).wait()
            part[ck, slot] = dot(act[...], wd[ws])
            p_copy(ck, slot).start()
            if last:
                @pl.when(layer + slots_w < n_layers)
                def _():
                    down_copy(layer + slots_w, ws).start()
        return 0

    lax.fori_loop(0, n_layers, layer_step, 0)
    for ck in range(rows):
        update(ck, (n_layers - 1) % len(PAIR))

        @pl.when(me == ck)
        def _():
            last_ref[...] = h[ck]

        state_ref[ck] = rms_unit(h[ck].astype(F32))[0].astype(BF16)
    for copy in r_copies:
        copy.wait()


def teacher(x_teach, x_stud, gain_s, w_up_s, w_down_s, gain_t, w_up_t, w_down_t, feat_at, collective_id, slots_w=3):
    n_layers, d_model, d_ff = w_up_t.shape
    rows, seq_half, _ = x_teach.shape
    n_tok = len(PAIR) * seq_half
    n_peers = SIDE * len(PAIR) - 1
    feat = jax.ShapeDtypeStruct((n_tok, d_model), BF16)
    slots = (rows, len(PAIR))
    weights = n_layers * d_model * d_ff
    return pl.pallas_call(
        functools.partial(teacher_kernel, feat_at, slots_w),
        out_shape=(feat, feat, jax.ShapeDtypeStruct((rows, n_tok, d_model), BF16),
                   jax.ShapeDtypeStruct((SIDE, len(PAIR)) + x_stud.shape, BF16)),
        in_specs=[IN_VMEM] * 6 + [IN_HBM] * len(PAIR),
        out_specs=(IN_VMEM,) * SIDE,
        scratch_shapes=[
            pltpu.VMEM((rows, n_tok, d_model), BF16), pltpu.VMEM((n_tok, d_model), BF16), pltpu.VMEM((n_tok, d_ff), BF16),
            pltpu.VMEM((slots_w, d_model, d_ff), BF16), pltpu.VMEM((slots_w, d_ff, d_model), BF16),
            pltpu.VMEM(slots + (n_tok, d_model), F32), pltpu.VMEM(slots + (n_tok, d_model), F32),
            pltpu.VMEM(x_stud.shape, BF16),
            DMA((slots_w,)), DMA((slots_w,)), DMA, DMA, DMA(slots), DMA(slots), DMA((n_peers,)), DMA((n_peers,)),
        ],
        compiler_params=pltpu.CompilerParams(collective_id=collective_id, has_side_effects=True, vmem_limit_bytes=52 * MIB),
        cost_estimate=pl.CostEstimate(flops=SIDE * rows * n_tok * weights, bytes_accessed=SIDE * weights, transcendentals=0),
        name='teacher',
    )(x_teach, x_stud, gain_s, w_up_s, w_down_s, gain_t, w_up_t, w_down_t)


NEG = -1e38
MAX_T, SUM_T, MAX_S, SUM_S = STATS = range(SIDE)
TEACH, STUD = PAIR


def heads_kernel(kl_coef, chunk,
                 t_ref, r_ref, ht_hbm, hs_hbm,
                 dw_hbm, dx_ref, kl_ref,
                 tg, rt, ht, hs, zt, zs, mx, sm, st_send, st_all, lcol, grad, dx, px, ds, dr,
                 ht_sem, hs_sem, ring_send, ring_recv, peer_send, peer_recv, st_send_sem, st_recv_sem, dx_send, dx_recv, out_sem):
    coords = chip_coords()
    x = coords[X]
    core = lax.axis_index('tp')
    peer = device(coords, 1 - core)
    rows, n_tok, d_model = t_ref.shape
    d_stud, cols = hs.shape
    n_tiles = cols // LANES
    blk = rows * n_tok
    n_all = SIDE * blk
    half_tile = LANES // 2
    last_x = SIDE - 1

    first_tile = n_tiles * x + core * (n_tiles * SIDE - 1)
    hs_copy = pltpu.make_async_copy(hs_hbm.at[:, pl.ds(pl.multiple_of(first_tile * LANES, LANES), cols)], hs, hs_sem)
    hs_copy.start()
    cut_low = (core == 1) & (x == 0)
    cut_high = (core == 0) & (x == last_x)

    def ht_copy(src, dst, n):
        return pltpu.make_async_copy(ht_hbm.at[pl.ds(src, n)], ht.at[pl.ds(dst, n)], ht_sem)

    def each_ht(act):
        @pl.when(jnp.logical_not(cut_low | cut_high))
        def _():
            act(ht_copy(pl.multiple_of(cols * x - half_tile * core, half_tile), 0, cols))

        @pl.when(cut_low)
        def _():
            act(ht_copy(0, half_tile, cols - half_tile))

        @pl.when(cut_high)
        def _():
            act(ht_copy(last_x * cols, 0, cols - half_tile))

    each_ht(lambda copy: copy.start())
    targets = group_targets(coords, core)
    greet(targets)

    far_rows = n_tok // 2

    def at(step):
        return lax.rem(x + step, SIDE)

    def ring(k, src, dst, step):
        return remote(src, dst, ring_send.at[k], ring_recv.at[k], device(moved(coords, X, step), core))

    def onward(k, step, way):
        piece = tg.at[at(step), core, pl.ds(k * far_rows, far_rows)]
        return ring(k + len(PAIR), piece, piece, way)

    def first(k, step, way):
        return ring(k, t_ref.at[core], tg.at[at(step), core], way)

    def across(step, side):
        piece = tg.at[at(step), side]
        return remote(piece, piece, peer_send.at[step - 1], peer_recv.at[step - 1], peer)

    opposite = (LEFT, RIGHT)
    for k, way in enumerate(WAYS):
        first(k, HERE, way).start()
    tg[x] = t_ref[...]
    rt[...] = r_ref[...].T
    lane = lax.broadcasted_iota(jnp.int32, (blk, LANES), 1)
    low = jnp.where(cut_low, half_tile, 0)
    high = jnp.where(cut_high, half_tile, LANES)

    def finish(kind, b, ref):
        head, tail = lane_slice(0, LANES), lane_slice(n_tiles - 1, LANES)
        ref[b, :, head] = jnp.where(lane >= low, ref[b, :, head], NEG)
        ref[b, :, tail] = jnp.where(lane < high, ref[b, :, tail], NEG)
        tiles = [lane_slice(k, LANES) for k in range(n_tiles)]
        peak = functools.reduce(jnp.maximum, [ref[b, :, t] for t in tiles])
        mx[kind, b] = peak
        sm[kind, b] = functools.reduce(jnp.add, [jnp.exp(ref[b, :, t] - peak) for t in tiles])

    def tokens(b):
        return pl.ds(pl.multiple_of(b * blk, blk), blk)

    def student_logits(b, _):
        zs[b] = dot(r_ref[tokens(b), :], hs[...])
        finish(STUD, b, zs)
        return 0

    hs_copy.wait()
    lax.fori_loop(0, FAR, student_logits, 0)
    for k, way in enumerate(WAYS):
        first(k, opposite[k], way).wait_recv()
        onward(k, opposite[k], way).start()
        across(opposite[k], core).start()
    lax.fori_loop(FAR, SIDE, student_logits, 0)
    for k, way in enumerate(WAYS):
        onward(k, FAR, way).wait_recv()
    across(FAR, core).start()
    each_ht(lambda copy: copy.wait())

    def teacher_logits(i, _):
        for step, turn in ((RIGHT, 1), (LEFT, 2), (FAR, 3)):
            @pl.when(i == turn)
            def _():
                across(step, 1 - core).wait_recv()

        b = at(jnp.where(i < FAR, i, SIDE + 1 - i))
        zt[b] = dot_right_t(tg[b].reshape(blk, d_model), ht[...])
        finish(TEACH, b, zt)
        return 0

    lax.fori_loop(0, SIDE, teacher_logits, 0)

    def merge(b, _):
        out = jnp.zeros((blk, LANES), F32)
        for kind in PAIR:
            peak = jnp.max(mx[kind, b], axis=-1, keepdims=True)
            total = jnp.sum(sm[kind, b] * jnp.exp(mx[kind, b] - peak), axis=-1, keepdims=True)
            out = jnp.where(lane == 2 * kind, peak, jnp.where(lane == 2 * kind + 1, total, out))
        st_send[:, tokens(b)] = out.T[:SUBS, :]
        return 0

    lax.fori_loop(0, SIDE, merge, 0)
    n_peers = len(targets)
    stats = [remote(st_send, st_all.at[i], st_send_sem.at[i], st_recv_sem.at[i], target) for i, target in enumerate(targets)]
    for copy in stats:
        copy.start()
    st_all[n_peers] = st_send[...]
    for copy in stats:
        copy.wait()
    sub = lax.broadcasted_iota(jnp.int32, (LANES, n_all), 0)
    both = jnp.zeros((LANES, n_all), F32)
    for kind in PAIR:
        peaks, totals = st_all[:, 2 * kind, :], st_all[:, 2 * kind + 1, :]
        peak = jnp.max(peaks, axis=0, keepdims=True)
        norm = peak + jnp.log(jnp.sum(totals * jnp.exp(peaks - peak), axis=0, keepdims=True))
        both = jnp.where(sub == kind, norm, both)
    lcol[...] = both.T
    kl_ref[...] = jnp.zeros_like(kl_ref)
    dx[...] = jnp.zeros_like(dx)

    def grad_step(j, _):
        lanes = pl.ds(pl.multiple_of(j * chunk, LANES), chunk)

        def block(b, _):
            tok = tokens(b)
            log_pt = zt[b, :, lanes] - lcol[tok, TEACH:TEACH + 1]
            log_ps = zs[b, :, lanes] - lcol[tok, STUD:STUD + 1]
            pt = jnp.exp(log_pt)
            grad[tok, :] = (kl_coef * (jnp.exp(log_ps) - pt)).astype(BF16)
            kl = pt * (log_pt - log_ps)
            kl = functools.reduce(jnp.add, [kl[:, lane_slice(k, LANES)] for k in range(chunk // LANES)])
            kl_ref[...] += functools.reduce(jnp.add, [kl[lane_slice(k, SUBS)] for k in range(blk // SUBS)])
            return 0

        lax.fori_loop(0, SIDE, block, 0)
        dw = dot(rt[...], grad[...])
        zt[0, :, lanes] = dw[:blk]
        zt[1, :d_stud - blk, lanes] = dw[blk:]
        dx[...] += dot_right_t(grad[...], hs[:, lanes])
        return 0

    lax.fori_loop(0, cols // chunk, grad_step, 0)
    outs = [pltpu.make_async_copy(zt.at[k, pl.ds(0, n)], dw_hbm.at[pl.ds(k * blk, n)], out_sem.at[k])
            for k, n in enumerate((blk, d_stud - blk))]
    for copy in outs:
        copy.start()

    for s in range(SIDE):
        for c in CORES:
            ds[c, s] = dx[lane_slice(2 * s + c, n_tok)]
    swap = remote(ds.at[1 - core], px, dx_send.at[HERE], dx_recv.at[HERE], peer)
    swap.start()
    swap.wait()
    ds[core] = ds[core] + px[...]
    passes = [remote(ds.at[core, at(step)], dr.at[step - 1], dx_send.at[step], dx_recv.at[step], device(moved(coords, X, step), core))
              for step in (RIGHT, FAR, LEFT)]
    for copy in passes:
        copy.start()
    for copy in passes:
        copy.wait()
    dx_ref[...] = functools.reduce(jnp.add, [dr[i] for i in range(last_x)], ds[core, x])
    for k, way in enumerate(WAYS):
        first(k, HERE, way).wait_send()
        onward(k, opposite[k], way).wait_send()
    for step in (RIGHT, FAR, LEFT):
        across(step, core).wait_send()
    for copy in outs:
        copy.wait()


def heads(states, stud_all, head_t, head_s, kl_coef, collective_id, chunk=768):
    rows, n_tok, d_model = states.shape
    n_all, d_stud = stud_all.shape
    cols = -(-head_t.shape[1] // (LANES * SIDE)) * LANES
    blk = rows * n_tok
    n_peers = SIDE * len(PAIR) - 1
    v = pltpu.VMEM
    hops = (SIDE - 1,)
    return pl.pallas_call(
        functools.partial(heads_kernel, kl_coef, chunk),
        out_shape=(jax.ShapeDtypeStruct((d_stud, cols), F32), jax.ShapeDtypeStruct((n_tok, d_stud), F32),
                   jax.ShapeDtypeStruct((SUBS, LANES), F32)),
        in_specs=[IN_VMEM, IN_VMEM, IN_HBM, IN_HBM],
        out_specs=(IN_HBM, IN_VMEM, IN_VMEM),
        scratch_shapes=[
            v((SIDE, rows, n_tok, d_model), BF16), v((d_stud, n_all), BF16), v((cols, d_model), BF16), v((d_stud, cols), BF16),
            v((SIDE, blk, cols), F32), v((SIDE, blk, cols), F32),
            v((len(PAIR), SIDE, blk, LANES), F32), v((len(PAIR), SIDE, blk, LANES), F32),
            v((SUBS, n_all), F32), v((n_peers + 1, SUBS, n_all), F32), v((n_all, LANES), F32),
            v((n_all, chunk), BF16), v((n_all, d_stud), F32), v((SIDE, n_tok, d_stud), F32),
            v((len(PAIR), SIDE, n_tok, d_stud), F32), v(hops + (n_tok, d_stud), F32),
            DMA, DMA, DMA((SIDE,)), DMA((SIDE,)), DMA(hops), DMA(hops), DMA((n_peers,)), DMA((n_peers,)),
            DMA((SIDE,)), DMA((SIDE,)), DMA((len(PAIR),)),
        ],
        compiler_params=pltpu.CompilerParams(collective_id=collective_id, has_side_effects=True, vmem_limit_bytes=63 * MIB),
        cost_estimate=pl.CostEstimate(flops=d_model * n_all * cols, bytes_accessed=d_model * cols, transcendentals=0),
        name='heads',
    )(states, stud_all, head_t.T, head_s)


class RingSum:
    def __init__(self, coords, core, src, dims, order, lanes, bufs):
        self.coords, self.core, self.order, self.lanes = coords, core, order, lanes
        self.phases = []
        for axis, (half, full, mid, send, recv) in zip(order, bufs):
            self.phases.append((src, dims, axis, half, full, mid, send, recv))
            src, dims = mid, tuple(d for d in dims if d != axis)

    @staticmethod
    def shapes(dims, order, rows, width):
        out = []
        for _ in order:
            dims = dims[1:]
            lead = (SIDE,) * len(dims)
            part = (SIDE // 2,) + lead[1:] + (rows, width) if lead else (rows, -(-width // (2 * LANES)) * LANES)
            out += [pltpu.VMEM(PAIR_DIM + part, F32), pltpu.VMEM(PAIR_DIM + lead + (rows, width), F32),
                    pltpu.VMEM(lead + (rows, width), F32), DMA((3 * len(PAIR),)), DMA((3 * len(PAIR),))]
        return out

    def place(self, axis, step):
        return lax.rem(self.coords[axis] + step, SIDE)

    def split(self, k, side):
        _, dims, _, half, full, _, _, _ = self.phases[k]
        width, cut = full.shape[-1], half.shape[-1]
        if len(dims) > 1:
            return (pl.ds(side * (SIDE // 2), SIDE // 2),) + (slice(None),) * (len(dims) - 2), (0, width)
        return (), ((cut, width - cut) if side else (0, cut))

    def pick(self, k, at, side):
        src, dims, axis = self.phases[k][:3]
        lead, (lo, n) = ((slice(None),) * (len(dims) - 1), (0, self.phases[k][4].shape[-1])) if side is None else self.split(k, side)
        lead = list(lead)
        lead.insert(dims.index(axis), at)
        base = self.lanes if k == 0 else 0
        return src, tuple(lead) + (slice(None), pl.ds(base + lo, n))

    def copy(self, k, turn, d):
        _, _, axis, half, full, _, send, recv = self.phases[k]
        way = WAYS[d]
        i = turn * len(PAIR) + d
        side = d if turn != 1 else 1 - d
        lead, (lo, n) = self.split(k, side)
        window = (slice(None), pl.ds(lo, n))
        if turn == 0:
            ref, idx = self.pick(k, self.place(axis, FAR), side)
            src, dst = ref.at[idx], half.at[d, ..., pl.ds(0, n)]
        elif turn == 1:
            ref, idx = self.pick(k, self.place(axis, way), side)
            src, dst = ref.at[idx], full.at[(d,) + lead + window]
        else:
            src, dst = half.at[d, ..., pl.ds(0, n)], full.at[(d,) + lead + window]
        return remote(src, dst, send.at[i], recv.at[i], device(moved(self.coords, axis, way), self.core))

    def start(self, k):
        for turn in PAIR:
            for d in PAIR:
                self.copy(k, turn, d).start()

    def middle(self, k):
        _, _, axis, half, _, _, _, _ = self.phases[k]
        for d in PAIR:
            self.copy(k, 0, d).wait_recv()
            ref, idx = self.pick(k, self.place(axis, WAYS[d]), d)
            n = self.split(k, d)[1][1]
            half[d, ..., :n] = half[d, ..., :n] + ref[idx]
            self.copy(k, len(PAIR), d).start()

    def finish(self, k):
        _, _, axis, _, full, mid, _, _ = self.phases[k]
        for d in PAIR:
            for turn in (1, len(PAIR)):
                self.copy(k, turn, d).wait_recv()
        ref, idx = self.pick(k, self.coords[axis], None)
        mid[...] = ref[idx] + full[0] + full[1]

    def drain(self):
        for k in range(len(self.order)):
            for turn in range(3):
                for d in PAIR:
                    self.copy(k, turn, d).wait_send()


PAIR_DIM = (len(PAIR),)


def small_places(n_feat, d_in, d_mid, d_teach):
    groups_up = d_in // SUBS
    yz = SIDE * SIDE
    per_up = n_feat * groups_up // yz
    lanes_u, lanes_p = d_mid // SIDE, d_teach // SIDE
    per_p = groups_up // yz
    span = per_up // per_p * lanes_u + lanes_p
    return groups_up, yz, per_up, lanes_u, lanes_p, per_p, span


def reduce_kernel(feat_coef, kl_coef, small_parts,
                  dw, dx_ref, feat_a, feat_b, xs_ref, gs_ref, ups_ref, dns_ref, proj_ref, kl_ref,
                  own, small, got, swap_send, swap_recv, *bufs):
    coords = chip_coords()
    core = lax.axis_index('tp')
    peer = device(coords, 1 - core)
    greet(near_targets(coords, core))
    cols = dw.shape[-1]
    bufs = list(bufs)

    def take(n):
        out = [tuple(bufs[5 * i:5 * i + 5]) for i in range(n)]
        del bufs[:5 * n]
        return out

    head_jobs = [RingSum(coords, core, dw, (Y, Z), order, k * (cols // 2), take(2)) for k, order in enumerate(((Y, Z), (Z, Y)))]
    for job in head_jobs:
        job.start(0)

    saved, _ = student_layers(xs_ref, gs_ref, ups_ref, dns_ref)
    feats = (feat_a, feat_b)
    n_feat, d_in, d_mid = ups_ref.shape
    groups, yz, per_up, lanes_u, lanes_p, per_p, span = small_places(n_feat, d_in, d_mid, proj_ref.shape[-1])
    two = per_up // per_p
    err_rows = jnp.zeros((SUBS, LANES), F32)
    resid_grad = None
    gain_rows = []

    def put(keep, chip_x, group, per, base, lanes, value):
        block, g = divmod(group, per)
        y, z = divmod(block, SIDE)
        part, q = divmod(g, per // per_p)
        small[keep, chip_x, y, z, :, part * span + base + q * lanes:part * span + base + q * lanes + lanes] = value

    for j in reversed(range(n_feat)):
        unit, inv, normed, pre, act, unit_next, inv_next = saved[j]
        proj_in = unit_next.astype(BF16)
        err = dot(proj_in, proj_ref[j]) - feats[j][...].astype(F32)
        sq = err * err
        sq = functools.reduce(jnp.add, [sq[:, lane_slice(k, LANES)] for k in range(sq.shape[1] // LANES)])
        err_rows = err_rows + functools.reduce(jnp.add, [sq[lane_slice(k, SUBS)] for k in range(sq.shape[0] // SUBS)])
        err_grad = ((2 * feat_coef) * err).astype(BF16)
        g_proj = dot_left_t(proj_in, err_grad)
        for i in range(groups):
            for cx in range(SIDE):
                put(j, cx, i, per_p, two * lanes_u, lanes_p, g_proj[lane_slice(i, SUBS), lane_slice(cx, lanes_p)])
        out_grad = dot_right_t(err_grad, proj_ref[j])
        if resid_grad is None:
            resid_grad = rms_back(unit_next, inv_next, out_grad + dx_ref[...])
        else:
            resid_grad = resid_grad + rms_back(unit_next, inv_next, out_grad)
        resid_bf = resid_grad.astype(BF16)
        g_down = dot_left_t(act, resid_bf)
        n_down = d_mid // SUBS
        for i in range(n_down):
            cx, rest = divmod(j * n_down + i, n_feat * n_down // SIDE)
            put(1, cx, rest, per_up, 0, lanes_u, g_down[lane_slice(i, SUBS), :])
        pre_grad = (gelu_slope(pre) * dot_right_t(resid_bf, dns_ref[j])).astype(BF16)
        g_up = dot_left_t(normed, pre_grad)
        for i in range(groups):
            for cx in range(SIDE):
                put(0, cx, j * groups + i, per_up, 0, lanes_u, g_up[lane_slice(i, SUBS), lane_slice(cx, lanes_u)])
        norm_grad = dot_right_t(pre_grad, ups_ref[j])
        g_gain = jnp.sum(norm_grad * unit, axis=0, keepdims=True)
        gain_rows = [g_gain[:, lane_slice(k, LANES)] for k in range(d_in // LANES)] + gain_rows
        if j > 0:
            resid_grad = resid_grad + rms_back(unit, inv, norm_grad * gs_ref[j:j + 1, :])

    swaps = [remote(small.at[1 - core, cx], got.at[cx], swap_send.at[cx], swap_recv.at[cx], peer) for cx in range(SIDE)]
    for copy in swaps:
        copy.start()
    for job in head_jobs:
        job.middle(0)
    for cx, copy in enumerate(swaps):
        copy.wait()
        got[cx] = got[cx] + small[core, cx]
    lo = 0
    small_jobs = []
    for order, width in zip(ORDERS, small_parts):
        small_jobs.append(RingSum(coords, core, got, AXES, order, lo, take(3)))
        lo += width
    for job in small_jobs:
        job.start(0)
    for job in head_jobs:
        job.finish(0)
        job.start(1)
    for job in small_jobs:
        job.middle(0)
    for job in head_jobs:
        job.middle(1)
    for job in small_jobs:
        job.finish(0)
        job.start(1)
    for job in head_jobs:
        job.finish(1)
    for job in small_jobs:
        job.middle(1)
    for job in small_jobs:
        job.finish(1)
        job.start(2)
    for job in small_jobs:
        job.middle(2)
    for job in small_jobs:
        job.finish(2)
    for p in PARTS:
        for k, job in enumerate(head_jobs):
            own[p, :, lane_slice(k, cols // 2)] = job.phases[-1][5][lane_slice(p, SUBS), :]
    pieces = [(order_i, t) for order_i, width in enumerate(small_parts) for t in range(width // LANES)]
    for n, (which, t) in enumerate(pieces):
        p, at = divmod(n * LANES, span)
        own[p, :, cols + at:cols + at + LANES] = small_jobs[which].phases[-1][5][:, lane_slice(t, LANES)]
    loss_row = jnp.sum(feat_coef * err_rows + kl_coef * kl_ref[...], axis=0, keepdims=True)
    for p in PARTS:
        own[p, :, cols + span:] = jnp.zeros((SUBS, LANES), F32)
    for i, row in enumerate(gain_rows + [loss_row]):
        own[0, i:i + 1, cols + span:] = row
    for job in head_jobs + small_jobs:
        job.drain()


def reduce_grads(dw, dx, feats, x_stud, gain_s, w_up_s, w_down_s, proj_s, kl_tiles, feat_coef, kl_coef, collective_id,
                 small_parts=(2048, 512, 512)):
    rows, cols = dw.shape[2:]
    span = sum(small_parts) // len(PARTS)
    width = cols // 2
    scratch = [pltpu.VMEM((len(PAIR), SIDE, SIDE, SIDE, SUBS, sum(small_parts)), F32),
               pltpu.VMEM((SIDE, SIDE, SIDE, SUBS, sum(small_parts)), F32), DMA((SIDE,)), DMA((SIDE,))]
    for _ in PAIR:
        scratch += RingSum.shapes((Y, Z), (Y, Z), rows, width)
    for part in small_parts:
        scratch += RingSum.shapes(AXES, AXES, SUBS, part)
    return pl.pallas_call(
        functools.partial(reduce_kernel, feat_coef, kl_coef, small_parts),
        out_shape=jax.ShapeDtypeStruct((len(PARTS), SUBS, cols + span + LANES), F32),
        in_specs=[IN_VMEM] * 10,
        out_specs=IN_VMEM,
        scratch_shapes=scratch,
        compiler_params=pltpu.CompilerParams(collective_id=collective_id, has_side_effects=True, vmem_limit_bytes=62 * MIB),
        cost_estimate=pl.CostEstimate(flops=MIB * MIB, bytes_accessed=dw.size, transcendentals=0),
        name='reduce',
    )(dw, dx, *feats, x_stud, gain_s, w_up_s, w_down_s, proj_s, kl_tiles)


ALL = pl.ds(0, SIDE)


def gather_kernel(cut, own_ref, full, own_sem, send_sem, recv_sem, peer_send, peer_recv):
    coords = chip_coords()
    core = lax.axis_index('tp')
    peer = device(coords, 1 - core)
    width = own_ref.shape[-1]
    widths = (width, width - LANES, width - LANES)
    here = [pltpu.make_async_copy(own_ref.at[p], full.at[(core,) + coords + (p,)], own_sem.at[p]) for p in PARTS]
    for copy in here:
        copy.start()
    greet(near_targets(coords, core))
    whole, low, high = range(3)

    def lanes(part, span):
        return pl.ds(cut if span == high else 0, (widths[part], cut, widths[part] - cut)[span])

    def at_of(part, phase, step):
        return lax.rem(coords[ORDERS[part][phase]] + step, SIDE)

    def block(part, phase, step, span):
        idx = list(coords)
        for k, axis in enumerate(ORDERS[part][:phase + 1]):
            idx[axis] = ALL if k < phase else at_of(part, phase, step)
        return full.at[(core,) + tuple(idx) + (part, slice(None), lanes(part, span))]

    def ring(part, phase, slot, step, span):
        dst = block(part, phase, step, span)
        src = own_ref.at[part, :, lanes(part, span)] if phase == 0 and step == HERE else dst
        return remote(src, dst, send_sem.at[part, phase, slot], recv_sem.at[part, phase, slot],
                      device(moved(coords, ORDERS[part][phase], WAYS[slot % 2]), core))

    def first(part, phase, d, step):
        return ring(part, phase, d, step, whole)

    def onward(part, phase, d, step):
        return ring(part, phase, d + 2, step, (low, high)[d])

    def across(part, phase, step):
        src = block(part, phase, step, whole)
        return remote(src, src, peer_send.at[part, phase, step], peer_recv.at[part, phase, step], peer)

    def own_across(part):
        dst = block(part, 0, HERE, whole)
        return remote(own_ref.at[part, :, lanes(part, whole)], dst, peer_send.at[part, 0, HERE], peer_recv.at[part, 0, HERE], peer)

    source = (LEFT, RIGHT)
    for part in PARTS:
        for d in PAIR:
            first(part, 0, d, HERE).start()
        own_across(part).start()
    for phase in AXES:
        for part in PARTS:
            for d in PAIR:
                first(part, phase, d, source[d]).wait_recv()
                onward(part, phase, d, source[d]).start()
                across(part, phase, source[d]).start()
        for part in PARTS:
            for d in PAIR:
                onward(part, phase, d, FAR).wait_recv()
            if phase == 0:
                here[part].wait()
            if phase < AXES[-1]:
                for d in PAIR:
                    first(part, phase + 1, d, HERE).start()
            across(part, phase, FAR).start()
    for part in PARTS:
        for phase in AXES:
            for d in PAIR:
                first(part, phase, d, HERE).wait_send()
                onward(part, phase, d, source[d]).wait_send()
            for step in (LEFT, RIGHT, FAR):
                across(part, phase, step).wait()
        own_across(part).wait()


def gather_blocks(own, cut, collective_id):
    sems = DMA((len(PARTS), len(AXES), SIDE))
    return pl.pallas_call(
        functools.partial(gather_kernel, cut),
        out_shape=jax.ShapeDtypeStruct((len(PAIR), SIDE, SIDE, SIDE) + own.shape, F32),
        in_specs=[IN_VMEM],
        out_specs=IN_HBM,
        scratch_shapes=[DMA((len(PARTS),)), sems, sems, sems, sems],
        compiler_params=pltpu.CompilerParams(collective_id=collective_id, has_side_effects=True),
        cost_estimate=pl.CostEstimate(flops=MIB * MIB, bytes_accessed=SIDE * LANES * own.size, transcendentals=0),
        name='gather',
    )(own)


N_BUF = 6
N_LATE = N_BUF // 2


def place_kernel(n_head, lanes_u, lanes_p,
                 full, head, up, down, proj, total,
                 bufs, edge, wide, narrow, tiles,
                 in_sem, out_sem, edge_sem, wide_in, wide_out, narrow_in, narrow_out, tile_sem):
    last_x = SIDE - 1
    per = wide.shape[3]
    copy = pltpu.make_async_copy
    narrow_at = n_head + per * lanes_u
    tile_copy = copy(full.at[:, :, :, 0, :, pl.ds(narrow_at + lanes_p, LANES)], tiles, tile_sem)
    tile_copy.start()
    owners = [(c, x) for c in CORES for x in range(SIDE)]
    jobs = [owner + (s,) for owner in owners for s in range(SIDE)]

    def fetch(i):
        c, x, s = jobs[i]
        slot = i % N_BUF
        blocks = pl.ds(s * SIDE, SIDE)
        out = [copy(full.at[c, x, blocks, :, :, pl.ds(0, n_head)], bufs.at[slot], in_sem.at[slot])]
        if (c, x) == PAIR[::-1]:
            out.append(copy(full.at[0, last_x, blocks, :, :, pl.ds(n_head - LANES, LANES)], edge.at[slot], edge_sem.at[slot]))
        return out

    def put(i):
        c, x, s = jobs[i]
        slot = i % N_BUF
        n = n_head - LANES if (c, x) == (0, last_x) else n_head
        at = (c * SIDE + x) * n_head - c * LANES
        return copy(bufs.at[slot, :, :, :, pl.ds(0, n)], head.at[pl.ds(s * SIDE, SIDE), :, :, pl.ds(at, n)], out_sem.at[slot])

    def small_fetch(i):
        c, x = owners[i]
        slot = i % 2
        out = [copy(full.at[c, x, :, :, :, pl.ds(n_head + q * lanes_u, lanes_u)], wide.at[slot, :, :, q], wide_in.at[slot, q])
               for q in range(per)]
        return out + [copy(full.at[c, x, :, :, :, pl.ds(narrow_at, lanes_p)], narrow.at[slot], narrow_in.at[slot])]

    def small_put(i):
        c, x = owners[i]
        slot = i % 2
        dst = down.at[x] if c else up.at[:, :, :, :, pl.ds(x * lanes_u, lanes_u)]
        return [copy(wide.at[slot], dst, wide_out.at[slot]),
                copy(narrow.at[slot], proj.at[c, :, :, :, pl.ds(x * lanes_p, lanes_p)], narrow_out.at[slot])]

    def each(copies, act):
        for one in copies:
            act(one)

    start, wait = (lambda one: one.start()), (lambda one: one.wait())
    for i in range(N_LATE):
        each(fetch(i), start)
    each(small_fetch(0), start)
    for i in range(len(jobs)):
        nxt = i + N_LATE
        if nxt < len(jobs):
            if nxt >= N_BUF:
                wait(put(nxt - N_BUF))
            each(fetch(nxt), start)
        each(fetch(i), wait)
        if jobs[i][:2] == PAIR[::-1]:
            slot = i % N_BUF
            bufs[slot, :, :, :, :LANES] = bufs[slot, :, :, :, :LANES] + edge[slot]
        start(put(i))
        if i % SIDE == SIDE - 1:
            k = i // SIDE
            each(small_fetch(k), wait)
            each(small_put(k), start)
            if k:
                each(small_put(k - 1), wait)
            if k + 1 < len(owners):
                each(small_fetch(k + 1), start)
    tile_copy.wait()
    sums = jnp.sum(tiles[...].reshape(-1, SUBS, LANES), axis=0)
    total[...] = sums
    for i in range(len(jobs) - N_BUF, len(jobs)):
        wait(put(i))
    each(small_put(len(owners) - 1), wait)


def place_blocks(full, n_head, lanes_u, lanes_p, vocab):
    _, _, n_yz, n_part, subs, _ = full.shape
    per = len(PAIR)
    v = pltpu.VMEM
    pair = (len(PAIR),)
    shapes = ((n_yz, n_part, subs, vocab), (n_yz, n_part, per, subs, SIDE * lanes_u), (SIDE, n_yz, n_part, per, subs, lanes_u),
              pair + (n_yz, n_part, subs, SIDE * lanes_p), (subs, LANES))
    return pl.pallas_call(
        functools.partial(place_kernel, n_head, lanes_u, lanes_p),
        out_shape=tuple(jax.ShapeDtypeStruct(s, F32) for s in shapes),
        in_specs=[IN_HBM],
        out_specs=(IN_HBM,) * SIDE + (IN_VMEM,),
        scratch_shapes=[v((N_BUF, SIDE, n_part, subs, n_head), F32), v((N_BUF, SIDE, n_part, subs, LANES), F32),
                        v(pair + (n_yz, n_part, per, subs, lanes_u), F32), v(pair + (n_yz, n_part, subs, lanes_p), F32),
                        v(pair + (SIDE, n_yz, subs, LANES), F32),
                        DMA((N_BUF,)), DMA((N_BUF,)), DMA((N_BUF,)), DMA(pair + (per,)), DMA(pair), DMA(pair), DMA(pair), DMA],
        compiler_params=pltpu.CompilerParams(has_side_effects=True, vmem_limit_bytes=56 * MIB),
        name='place',
    )(full)


def solution(mesh):
    n_dev = mesh.shape['dp'] * mesh.shape['tp']

    def local_step(x_teach, x_stud, w_up_t, w_down_t, gain_t, head_t, w_up_s, w_down_s, gain_s, proj_s, head_s):
        n_feat, d_in, d_mid = w_up_s.shape
        d_teach = proj_s.shape[-1]
        n_tokens = x_stud.shape[0] * x_stud.shape[1] * n_dev
        feat_coef = 1.0 / (n_feat * n_tokens * d_teach)
        kl_coef = 1.0 / n_tokens
        xs = x_stud[0]
        feat_one, feat_two, states, stud_all = teacher(x_teach, xs, gain_s, w_up_s, w_down_s, gain_t, w_up_t, w_down_t,
                                                       w_up_t.shape[0] // n_feat, 0)
        head_part, head_in_grad, kl_tiles = heads(states, stud_all.reshape(-1, d_in), head_t, head_s, kl_coef, 1)
        cols = head_part.shape[1]
        own = reduce_grads(head_part.reshape(SIDE, SIDE, -1, cols), head_in_grad, (feat_one, feat_two), xs, gain_s, w_up_s, w_down_s,
                           proj_s, kl_tiles, feat_coef, kl_coef, 2)
        blocks = gather_blocks(own, 20 * LANES, 3)
        blocks = blocks.reshape(blocks.shape[:2] + (SIDE * SIDE,) + blocks.shape[-3:])
        head_grad, up, down, proj, total = place_blocks(blocks, cols, d_mid // SIDE, d_teach // SIDE, head_s.shape[1])
        n_gain = n_feat * d_in // LANES
        return (jnp.sum(total[n_gain]), up.reshape(w_up_s.shape), down.reshape(w_down_s.shape), total[:n_gain].reshape(gain_s.shape),
                proj.reshape(proj_s.shape), head_grad.reshape(head_s.shape))

    in_specs = (P('dp', 'tp', None), P(('dp', 'tp'), None, None), P(None, None, 'tp'), P(None, 'tp', None),
                P(), P(None, 'tp'), P(), P(), P(), P(), P())
    out_specs = (P(), P(), P(), P(), P(), P())
    return jax.shard_map(local_step, mesh=mesh, in_specs=in_specs, out_specs=out_specs, check_vma=False)
```

```python
import functools

import jax
import jax.numpy as jnp
from jax import lax
from jax.experimental import pallas as pl
from jax.experimental.pallas import tpu as pltpu
from jax.sharding import PartitionSpec as P

NORM_EPS = 1e-6
MESH = pl.DeviceIdType.MESH
F32, BF16 = jnp.float32, jnp.bfloat16
DMA = pltpu.SemaphoreType.DMA
IN_VMEM = pl.BlockSpec(memory_space=pltpu.VMEM)
IN_HBM = pl.BlockSpec(memory_space=pl.ANY)
LANES = 128
SUBS = 8
SIDE = 4
MIB = 1 << 20
HERE, RIGHT, FAR, LEFT = range(SIDE)
X, Y, Z = AXES = tuple(range(SIDE - RIGHT))
PARTS = AXES
ORDERS = ((X, Y, Z), (Y, Z, X), (Z, X, Y))
CORES = PAIR = (0, 1)
WAYS = (RIGHT, LEFT)


def chip_coords():
    chip = lax.axis_index('dp')
    return lax.rem(chip, SIDE), lax.rem(chip // SIDE, SIDE), chip // (SIDE * SIDE)


def device(coords, core):
    x, y, z = coords
    return {'dp': (z * SIDE + y) * SIDE + x, 'tp': core}


def moved(coords, axis, step):
    out = list(coords)
    out[axis] = lax.rem(out[axis] + step, SIDE)
    return tuple(out)


def remote(src, dst, send_sem, recv_sem, target):
    return pltpu.make_async_remote_copy(src_ref=src, dst_ref=dst, send_sem=send_sem, recv_sem=recv_sem,
                                        device_id=target, device_id_type=MESH)


def greet(targets):
    barrier = pltpu.get_barrier_semaphore()
    for target in targets:
        pl.semaphore_signal(barrier, device_id=target, device_id_type=MESH)
    pl.semaphore_wait(barrier, len(targets))


def group_targets(coords, core):
    return [device(moved(coords, X, step), abs(core - flip)) for step in range(SIDE) for flip in CORES if step or flip]


def near_targets(coords, core):
    return [device(moved(coords, axis, step), core) for axis in AXES for step in WAYS] + [device(coords, 1 - core)]


def lane_slice(k, width):
    return slice(k * width, k * width + width)


def rms_unit(values):
    inv = lax.rsqrt(jnp.mean(values * values, axis=-1, keepdims=True) + NORM_EPS)
    return values * inv, inv


def rms_back(normed, inv_rms, grad_out):
    return inv_rms * (grad_out - normed * jnp.mean(grad_out * normed, axis=-1, keepdims=True))


GELU_C = 0.7978845608028654
GELU_K = 0.044715


def gelu_act(u):
    half = 0.5 * u
    return half + half * jnp.tanh(u * (GELU_C + (GELU_C * GELU_K) * (u * u)))


def gelu_slope(u):
    sq = u * u
    t = jnp.tanh(u * (GELU_C + (GELU_C * GELU_K) * sq))
    return 0.5 * (1 + t) + (0.5 * u) * (1 - t * t) * (GELU_C + (3 * GELU_C * GELU_K) * sq)


def dot(a, b):
    return jnp.dot(a, b, preferred_element_type=F32)


def dot_right_t(a, b):
    return lax.dot_general(a, b, (((1,), (1,)), ((), ())), preferred_element_type=F32)


def dot_left_t(a, b):
    return lax.dot_general(a, b, (((0,), (0,)), ((), ())), preferred_element_type=F32)


def student_layers(x_ref, gain_ref, up_ref, down_ref):
    residual = x_ref[...].astype(F32)
    unit, inv = rms_unit(residual)
    saved = []
    for j in range(up_ref.shape[0]):
        normed = (unit * gain_ref[j:j + 1, :]).astype(BF16)
        pre = dot(normed, up_ref[j])
        act = gelu_act(pre).astype(BF16)
        residual = residual + dot(act, down_ref[j])
        unit_next, inv_next = rms_unit(residual)
        saved.append((unit, inv, normed, pre, act, unit_next, inv_next))
        unit, inv = unit_next, inv_next
    return saved, unit.astype(BF16)


def teacher_kernel(feat_at, slots_w,
                   x_ref, xs_ref, gs_ref, ups_ref, dns_ref, gain_ref, wup_hbm, wdn_hbm,
                   feat_ref, last_ref, state_ref, group_ref,
                   h, nrm, act, wu, wd, part, got, r_own,
                   usem, dsem, xsend, xrecv, ssem, rsem, gsend, grecv):
    me = lax.axis_index('tp')
    coords = chip_coords()
    peer = device(coords, 1 - me)
    n_layers = gain_ref.shape[0]
    rows, seq_half, d_model = x_ref.shape

    def up_copy(layer, slot):
        return pltpu.make_async_copy(wup_hbm.at[layer], wu.at[slot], usem.at[slot])

    def down_copy(layer, slot):
        return pltpu.make_async_copy(wdn_hbm.at[layer], wd.at[slot], dsem.at[slot])

    for i in range(slots_w):
        up_copy(i, i).start()
        down_copy(i, i).start()
    targets = group_targets(coords, me)
    greet(targets)
    mine = pl.ds(pl.multiple_of(me * seq_half, seq_half), seq_half)
    xcopy = remote(x_ref, h.at[:, mine], xsend, xrecv, peer)
    xcopy.start()
    h[:, mine] = x_ref[...]

    _, head_in = student_layers(xs_ref, gs_ref, ups_ref, dns_ref)
    r_own[...] = head_in
    r_copies = [remote(r_own, group_ref.at[coords[X], me], gsend.at[i], grecv.at[i], target) for i, target in enumerate(targets)]
    for copy in r_copies:
        copy.start()
    group_ref[coords[X], me] = head_in
    xcopy.wait()

    def p_copy(ck, slot):
        return remote(part.at[ck, slot], got.at[ck, slot], ssem.at[ck, slot], rsem.at[ck, slot], peer)

    def update(ck, slot):
        p_copy(ck, slot).wait()
        total = part[ck, slot] + got[ck, slot]
        h[ck] = (h[ck].astype(F32) + total.astype(BF16).astype(F32)).astype(BF16)

    def layer_step(layer, _):
        slot = lax.rem(layer, len(PAIR))
        ws = lax.rem(layer, slots_w)
        for ck in range(rows):
            first, last = ck == 0, ck == rows - 1

            @pl.when(layer > 0)
            def _():
                update(ck, 1 - slot)

            @pl.when((layer == feat_at) & (me == ck))
            def _():
                feat_ref[...] = h[ck]

            unit, _ = rms_unit(h[ck].astype(F32))
            nrm[...] = (unit * gain_ref[pl.ds(layer, 1), :]).astype(BF16)
            if first:
                up_copy(layer, ws).wait()
            act[...] = gelu_act(dot(nrm[...], wu[ws])).astype(BF16)
            if last:
                @pl.when(layer + slots_w < n_layers)
                def _():
                    up_copy(layer + slots_w, ws).start()
            if first:
                down_copy(layer, ws).wait()
            part[ck, slot] = dot(act[...], wd[ws])
            p_copy(ck, slot).start()
            if last:
                @pl.when(layer + slots_w < n_layers)
                def _():
                    down_copy(layer + slots_w, ws).start()
        return 0

    lax.fori_loop(0, n_layers, layer_step, 0)
    for ck in range(rows):
        update(ck, (n_layers - 1) % len(PAIR))

        @pl.when(me == ck)
        def _():
            last_ref[...] = h[ck]

        state_ref[ck] = rms_unit(h[ck].astype(F32))[0].astype(BF16)
    for copy in r_copies:
        copy.wait()


def teacher(x_teach, x_stud, gain_s, w_up_s, w_down_s, gain_t, w_up_t, w_down_t, feat_at, collective_id, slots_w=3):
    n_layers, d_model, d_ff = w_up_t.shape
    rows, seq_half, _ = x_teach.shape
    n_tok = len(PAIR) * seq_half
    n_peers = SIDE * len(PAIR) - 1
    feat = jax.ShapeDtypeStruct((n_tok, d_model), BF16)
    slots = (rows, len(PAIR))
    weights = n_layers * d_model * d_ff
    return pl.pallas_call(
        functools.partial(teacher_kernel, feat_at, slots_w),
        out_shape=(feat, feat, jax.ShapeDtypeStruct((rows, n_tok, d_model), BF16),
                   jax.ShapeDtypeStruct((SIDE, len(PAIR)) + x_stud.shape, BF16)),
        in_specs=[IN_VMEM] * 6 + [IN_HBM] * len(PAIR),
        out_specs=(IN_VMEM,) * SIDE,
        scratch_shapes=[
            pltpu.VMEM((rows, n_tok, d_model), BF16), pltpu.VMEM((n_tok, d_model), BF16), pltpu.VMEM((n_tok, d_ff), BF16),
            pltpu.VMEM((slots_w, d_model, d_ff), BF16), pltpu.VMEM((slots_w, d_ff, d_model), BF16),
            pltpu.VMEM(slots + (n_tok, d_model), F32), pltpu.VMEM(slots + (n_tok, d_model), F32),
            pltpu.VMEM(x_stud.shape, BF16),
            DMA((slots_w,)), DMA((slots_w,)), DMA, DMA, DMA(slots), DMA(slots), DMA((n_peers,)), DMA((n_peers,)),
        ],
        compiler_params=pltpu.CompilerParams(collective_id=collective_id, has_side_effects=True, vmem_limit_bytes=52 * MIB),
        cost_estimate=pl.CostEstimate(flops=SIDE * rows * n_tok * weights, bytes_accessed=SIDE * weights, transcendentals=0),
        name='teacher',
    )(x_teach, x_stud, gain_s, w_up_s, w_down_s, gain_t, w_up_t, w_down_t)


NEG = -1e38
MAX_T, SUM_T, MAX_S, SUM_S = STATS = range(SIDE)
TEACH, STUD = PAIR


def heads_kernel(kl_coef, chunk,
                 t_ref, r_ref, ht_hbm, hs_hbm,
                 dw_hbm, dx, kl_ref,
                 tg, rt, ht, hs, zt, zs, mx, sm, st_send, st_all, lcol, grad,
                 ht_sem, hs_sem, ring_send, ring_recv, peer_send, peer_recv, st_send_sem, st_recv_sem, out_sem):
    coords = chip_coords()
    x = coords[X]
    core = lax.axis_index('tp')
    peer = device(coords, 1 - core)
    rows, n_tok, d_model = t_ref.shape
    d_stud, cols = hs.shape
    n_tiles = cols // LANES
    blk = rows * n_tok
    n_all = SIDE * blk
    half_tile = LANES // 2
    last_x = SIDE - 1

    first_tile = n_tiles * x + core * (n_tiles * SIDE - 1)
    hs_copy = pltpu.make_async_copy(hs_hbm.at[:, pl.ds(pl.multiple_of(first_tile * LANES, LANES), cols)], hs, hs_sem)
    hs_copy.start()
    cut_low = (core == 1) & (x == 0)
    cut_high = (core == 0) & (x == last_x)

    def ht_copy(src, dst, n):
        return pltpu.make_async_copy(ht_hbm.at[pl.ds(src, n)], ht.at[pl.ds(dst, n)], ht_sem)

    def each_ht(act):
        @pl.when(jnp.logical_not(cut_low | cut_high))
        def _():
            act(ht_copy(pl.multiple_of(cols * x - half_tile * core, half_tile), 0, cols))

        @pl.when(cut_low)
        def _():
            act(ht_copy(0, half_tile, cols - half_tile))

        @pl.when(cut_high)
        def _():
            act(ht_copy(last_x * cols, 0, cols - half_tile))

    each_ht(lambda copy: copy.start())
    targets = group_targets(coords, core)
    greet(targets)

    far_rows = n_tok // 2

    def at(step):
        return lax.rem(x + step, SIDE)

    def ring(k, src, dst, step):
        return remote(src, dst, ring_send.at[k], ring_recv.at[k], device(moved(coords, X, step), core))

    def onward(k, step, way):
        piece = tg.at[at(step), core, pl.ds(k * far_rows, far_rows)]
        return ring(k + len(PAIR), piece, piece, way)

    def first(k, step, way):
        return ring(k, t_ref.at[core], tg.at[at(step), core], way)

    def across(step, side):
        piece = tg.at[at(step), side]
        return remote(piece, piece, peer_send.at[step - 1], peer_recv.at[step - 1], peer)

    opposite = (LEFT, RIGHT)
    for k, way in enumerate(WAYS):
        first(k, HERE, way).start()
    tg[x] = t_ref[...]
    rt[...] = r_ref[...].T
    lane = lax.broadcasted_iota(jnp.int32, (blk, LANES), 1)
    low = jnp.where(cut_low, half_tile, 0)
    high = jnp.where(cut_high, half_tile, LANES)

    def finish(kind, b, ref):
        head, tail = lane_slice(0, LANES), lane_slice(n_tiles - 1, LANES)
        ref[b, :, head] = jnp.where(lane >= low, ref[b, :, head], NEG)
        ref[b, :, tail] = jnp.where(lane < high, ref[b, :, tail], NEG)
        tiles = [lane_slice(k, LANES) for k in range(n_tiles)]
        peak = functools.reduce(jnp.maximum, [ref[b, :, t] for t in tiles])
        mx[kind, b] = peak
        sm[kind, b] = functools.reduce(jnp.add, [jnp.exp(ref[b, :, t] - peak) for t in tiles])

    def tokens(b):
        return pl.ds(pl.multiple_of(b * blk, blk), blk)

    def student_logits(b, _):
        zs[b] = dot(r_ref[tokens(b), :], hs[...])
        finish(STUD, b, zs)
        return 0

    hs_copy.wait()
    lax.fori_loop(0, FAR, student_logits, 0)
    for k, way in enumerate(WAYS):
        first(k, opposite[k], way).wait_recv()
        onward(k, opposite[k], way).start()
        across(opposite[k], core).start()
    lax.fori_loop(FAR, SIDE, student_logits, 0)
    each_ht(lambda copy: copy.wait())

    def teacher_logits(i, _):
        for step, turn in ((RIGHT, 1), (LEFT, 2), (FAR, 3)):
            @pl.when(i == turn)
            def _():
                if step == RIGHT:
                    for k, way in enumerate(WAYS):
                        onward(k, FAR, way).wait_recv()
                    across(FAR, core).start()
                across(step, 1 - core).wait_recv()

        b = at(jnp.where(i < FAR, i, SIDE + 1 - i))
        zt[b] = dot_right_t(tg[b].reshape(blk, d_model), ht[...])
        finish(TEACH, b, zt)
        return 0

    lax.fori_loop(0, SIDE, teacher_logits, 0)

    def merge(b, _):
        out = jnp.zeros((blk, LANES), F32)
        for kind in PAIR:
            peak = jnp.max(mx[kind, b], axis=-1, keepdims=True)
            total = jnp.sum(sm[kind, b] * jnp.exp(mx[kind, b] - peak), axis=-1, keepdims=True)
            out = jnp.where(lane == 2 * kind, peak, jnp.where(lane == 2 * kind + 1, total, out))
        st_send[:, tokens(b)] = out.T[:SUBS, :]
        return 0

    lax.fori_loop(0, SIDE, merge, 0)
    n_peers = len(targets)
    stats = [remote(st_send, st_all.at[i], st_send_sem.at[i], st_recv_sem.at[i], target) for i, target in enumerate(targets)]
    for copy in stats:
        copy.start()
    st_all[n_peers] = st_send[...]
    for copy in stats:
        copy.wait()
    sub = lax.broadcasted_iota(jnp.int32, (LANES, n_all), 0)
    both = jnp.zeros((LANES, n_all), F32)
    for kind in PAIR:
        peaks, totals = st_all[:, 2 * kind, :], st_all[:, 2 * kind + 1, :]
        peak = jnp.max(peaks, axis=0, keepdims=True)
        norm = peak + jnp.log(jnp.sum(totals * jnp.exp(peaks - peak), axis=0, keepdims=True))
        both = jnp.where(sub == kind, norm, both)
    lcol[...] = both.T
    kl_ref[...] = jnp.zeros_like(kl_ref)
    dx[...] = jnp.zeros_like(dx)

    def grad_step(j, _):
        lanes = pl.ds(pl.multiple_of(j * chunk, LANES), chunk)

        def block(b, _):
            tok = tokens(b)
            log_pt = zt[b, :, lanes] - lcol[tok, TEACH:TEACH + 1]
            log_ps = zs[b, :, lanes] - lcol[tok, STUD:STUD + 1]
            pt = jnp.exp(log_pt)
            grad[tok, :] = (kl_coef * (jnp.exp(log_ps) - pt)).astype(BF16)
            kl = pt * (log_pt - log_ps)
            kl = functools.reduce(jnp.add, [kl[:, lane_slice(k, LANES)] for k in range(chunk // LANES)])
            kl_ref[...] += functools.reduce(jnp.add, [kl[lane_slice(k, SUBS)] for k in range(blk // SUBS)])
            return 0

        lax.fori_loop(0, SIDE, block, 0)
        dw = dot(rt[...], grad[...])
        zt[0, :, lanes] = dw[:blk]
        zt[1, :d_stud - blk, lanes] = dw[blk:]
        dx[...] += dot_right_t(grad[...], hs[:, lanes])
        return 0

    lax.fori_loop(0, cols // chunk, grad_step, 0)
    outs = [pltpu.make_async_copy(zt.at[k, pl.ds(0, n)], dw_hbm.at[pl.ds(k * blk, n)], out_sem.at[k])
            for k, n in enumerate((blk, d_stud - blk))]
    for copy in outs:
        copy.start()

    for k, way in enumerate(WAYS):
        first(k, HERE, way).wait_send()
        onward(k, opposite[k], way).wait_send()
    for step in (RIGHT, FAR, LEFT):
        across(step, core).wait_send()
    for copy in outs:
        copy.wait()


def heads(states, stud_all, head_t, head_s, kl_coef, collective_id, chunk=768):
    rows, n_tok, d_model = states.shape
    n_all, d_stud = stud_all.shape
    cols = -(-head_t.shape[1] // (LANES * SIDE)) * LANES
    blk = rows * n_tok
    n_peers = SIDE * len(PAIR) - 1
    v = pltpu.VMEM
    hops = (SIDE - 1,)
    return pl.pallas_call(
        functools.partial(heads_kernel, kl_coef, chunk),
        out_shape=(jax.ShapeDtypeStruct((d_stud, cols), F32), jax.ShapeDtypeStruct((n_all, d_stud), F32),
                   jax.ShapeDtypeStruct((SUBS, LANES), F32)),
        in_specs=[IN_VMEM, IN_VMEM, IN_HBM, IN_HBM],
        out_specs=(IN_HBM, IN_VMEM, IN_VMEM),
        scratch_shapes=[
            v((SIDE, rows, n_tok, d_model), BF16), v((d_stud, n_all), BF16), v((cols, d_model), BF16), v((d_stud, cols), BF16),
            v((SIDE, blk, cols), F32), v((SIDE, blk, cols), F32),
            v((len(PAIR), SIDE, blk, LANES), F32), v((len(PAIR), SIDE, blk, LANES), F32),
            v((SUBS, n_all), F32), v((n_peers + 1, SUBS, n_all), F32), v((n_all, LANES), F32),
            v((n_all, chunk), BF16),
            DMA, DMA, DMA((SIDE,)), DMA((SIDE,)), DMA(hops), DMA(hops), DMA((n_peers,)), DMA((n_peers,)), DMA((len(PAIR),)),
        ],
        compiler_params=pltpu.CompilerParams(collective_id=collective_id, has_side_effects=True, vmem_limit_bytes=63 * MIB),
        cost_estimate=pl.CostEstimate(flops=d_model * n_all * cols, bytes_accessed=d_model * cols, transcendentals=0),
        name='heads',
    )(states, stud_all, head_t.T, head_s)


class RingSum:
    def __init__(self, coords, core, src, dims, order, lanes, bufs):
        self.coords, self.core, self.order, self.lanes = coords, core, order, lanes
        self.phases = []
        for axis, (half, full, mid, send, recv) in zip(order, bufs):
            self.phases.append((src, dims, axis, half, full, mid, send, recv))
            src, dims = mid, tuple(d for d in dims if d != axis)

    @staticmethod
    def shapes(dims, order, rows, width):
        out = []
        for _ in order:
            dims = dims[1:]
            lead = (SIDE,) * len(dims)
            part = (SIDE // 2,) + lead[1:] + (rows, width) if lead else (rows, -(-width // (2 * LANES)) * LANES)
            out += [pltpu.VMEM(PAIR_DIM + part, F32), pltpu.VMEM(PAIR_DIM + lead + (rows, width), F32),
                    pltpu.VMEM(lead + (rows, width), F32), DMA((3 * len(PAIR),)), DMA((3 * len(PAIR),))]
        return out

    def place(self, axis, step):
        return lax.rem(self.coords[axis] + step, SIDE)

    def split(self, k, side):
        _, dims, _, half, full, _, _, _ = self.phases[k]
        width, cut = full.shape[-1], half.shape[-1]
        if len(dims) > 1:
            return (pl.ds(side * (SIDE // 2), SIDE // 2),) + (slice(None),) * (len(dims) - 2), (0, width)
        return (), ((cut, width - cut) if side else (0, cut))

    def pick(self, k, at, side):
        src, dims, axis = self.phases[k][:3]
        lead, (lo, n) = ((slice(None),) * (len(dims) - 1), (0, self.phases[k][4].shape[-1])) if side is None else self.split(k, side)
        lead = list(lead)
        lead.insert(dims.index(axis), at)
        base = self.lanes if k == 0 else 0
        return src, tuple(lead) + (slice(None), pl.ds(base + lo, n))

    def copy(self, k, turn, d):
        _, _, axis, half, full, _, send, recv = self.phases[k]
        way = WAYS[d]
        i = turn * len(PAIR) + d
        side = d if turn != 1 else 1 - d
        lead, (lo, n) = self.split(k, side)
        window = (slice(None), pl.ds(lo, n))
        if turn == 0:
            ref, idx = self.pick(k, self.place(axis, FAR), side)
            src, dst = ref.at[idx], half.at[d, ..., pl.ds(0, n)]
        elif turn == 1:
            ref, idx = self.pick(k, self.place(axis, way), side)
            src, dst = ref.at[idx], full.at[(d,) + lead + window]
        else:
            src, dst = half.at[d, ..., pl.ds(0, n)], full.at[(d,) + lead + window]
        return remote(src, dst, send.at[i], recv.at[i], device(moved(self.coords, axis, way), self.core))

    def start(self, k, turns=PAIR):
        for turn in turns:
            for d in PAIR:
                self.copy(k, turn, d).start()

    def middle(self, k):
        _, _, axis, half, _, _, _, _ = self.phases[k]
        for d in PAIR:
            self.copy(k, 0, d).wait_recv()
            ref, idx = self.pick(k, self.place(axis, WAYS[d]), d)
            n = self.split(k, d)[1][1]
            half[d, ..., :n] = half[d, ..., :n] + ref[idx]
            self.copy(k, len(PAIR), d).start()

    def finish(self, k):
        _, _, axis, _, full, mid, _, _ = self.phases[k]
        for d in PAIR:
            for turn in (1, len(PAIR)):
                self.copy(k, turn, d).wait_recv()
        ref, idx = self.pick(k, self.coords[axis], None)
        mid[...] = ref[idx] + full[0] + full[1]

    def drain(self):
        for k in range(len(self.order)):
            for turn in range(3):
                for d in PAIR:
                    self.copy(k, turn, d).wait_send()


PAIR_DIM = (len(PAIR),)


def small_places(n_feat, d_in, d_mid, d_teach):
    groups_up = d_in // SUBS
    yz = SIDE * SIDE
    per_up = n_feat * groups_up // yz
    lanes_u, lanes_p = d_mid // SIDE, d_teach // SIDE
    per_p = groups_up // yz
    span = per_up // per_p * lanes_u + lanes_p
    return groups_up, yz, per_up, lanes_u, lanes_p, per_p, span


def reduce_kernel(feat_coef, kl_coef, small_parts,
                  dw, dx_ref, feat_a, feat_b, xs_ref, gs_ref, ups_ref, dns_ref, proj_ref, kl_ref,
                  own, small, got, part_in, swap_send, swap_recv, in_send, in_recv, *bufs):
    coords = chip_coords()
    core = lax.axis_index('tp')
    peer = device(coords, 1 - core)
    greet(near_targets(coords, core))
    cols = dw.shape[-1]
    bufs = list(bufs)

    def take(n):
        out = [tuple(bufs[5 * i:5 * i + 5]) for i in range(n)]
        del bufs[:5 * n]
        return out

    head_jobs = [RingSum(coords, core, dw, (Y, Z), order, k * (cols // 2), take(2)) for k, order in enumerate(((Y, Z), (Z, Y)))]
    in_job = RingSum(coords, core, part_in, (X,), (X,), 0, take(1))
    for job in head_jobs:
        job.start(0)
    in_swap = remote(dx_ref.at[:, 1 - core], part_in, in_send, in_recv, peer)
    in_swap.start()

    saved, _ = student_layers(xs_ref, gs_ref, ups_ref, dns_ref)
    in_swap.wait()
    part_in[...] = part_in[...] + dx_ref[:, core]
    in_job.start(0)
    feats = (feat_a, feat_b)
    n_feat, d_in, d_mid = ups_ref.shape
    groups, yz, per_up, lanes_u, lanes_p, per_p, span = small_places(n_feat, d_in, d_mid, proj_ref.shape[-1])
    two = per_up // per_p
    err_rows = jnp.zeros((SUBS, LANES), F32)
    out_grads, gain_rows = [], []

    def put(keep, chip_x, group, per, base, lanes, value):
        block, g = divmod(group, per)
        y, z = divmod(block, SIDE)
        part, q = divmod(g, per // per_p)
        small[keep, chip_x, y, z, :, part * span + base + q * lanes:part * span + base + q * lanes + lanes] = value

    for j in range(n_feat):
        proj_in = saved[j][5].astype(BF16)
        err = dot(proj_in, proj_ref[j]) - feats[j][...].astype(F32)
        sq = err * err
        sq = functools.reduce(jnp.add, [sq[:, lane_slice(k, LANES)] for k in range(sq.shape[1] // LANES)])
        err_rows = err_rows + functools.reduce(jnp.add, [sq[lane_slice(k, SUBS)] for k in range(sq.shape[0] // SUBS)])
        err_grad = ((2 * feat_coef) * err).astype(BF16)
        g_proj = dot_left_t(proj_in, err_grad)
        for i in range(groups):
            for cx in range(SIDE):
                put(j, cx, i, per_p, two * lanes_u, lanes_p, g_proj[lane_slice(i, SUBS), lane_slice(cx, lanes_p)])
        out_grads.append(dot_right_t(err_grad, proj_ref[j]))
    in_job.middle(0)
    for job in head_jobs:
        job.middle(0)
    in_job.finish(0)
    out_grads[-1] = out_grads[-1] + in_job.phases[-1][5][...]
    resid_grad = None
    for j in reversed(range(n_feat)):
        unit, inv, normed, pre, act, unit_next, inv_next = saved[j]
        step_grad = rms_back(unit_next, inv_next, out_grads[j])
        resid_grad = step_grad if resid_grad is None else resid_grad + step_grad
        resid_bf = resid_grad.astype(BF16)
        g_down = dot_left_t(act, resid_bf)
        n_down = d_mid // SUBS
        for i in range(n_down):
            cx, rest = divmod(j * n_down + i, n_feat * n_down // SIDE)
            put(1, cx, rest, per_up, 0, lanes_u, g_down[lane_slice(i, SUBS), :])
        pre_grad = (gelu_slope(pre) * dot_right_t(resid_bf, dns_ref[j])).astype(BF16)
        g_up = dot_left_t(normed, pre_grad)
        for i in range(groups):
            for cx in range(SIDE):
                put(0, cx, j * groups + i, per_up, 0, lanes_u, g_up[lane_slice(i, SUBS), lane_slice(cx, lanes_u)])
        norm_grad = dot_right_t(pre_grad, ups_ref[j])
        g_gain = jnp.sum(norm_grad * unit, axis=0, keepdims=True)
        gain_rows = [g_gain[:, lane_slice(k, LANES)] for k in range(d_in // LANES)] + gain_rows
        if j > 0:
            resid_grad = resid_grad + rms_back(unit, inv, norm_grad * gs_ref[j:j + 1, :])

    def swap(step):
        cx = lax.rem(coords[X] + step, SIDE)
        return remote(small.at[1 - core, cx], got.at[cx], swap_send.at[step], swap_recv.at[step], peer)

    order_in = (FAR, RIGHT, LEFT, HERE)
    for step in order_in:
        swap(step).start()
    lo = 0
    small_jobs = []
    for order, width in zip(ORDERS, small_parts):
        small_jobs.append(RingSum(coords, core, got, AXES, order, lo, take(3)))
        lo += width
    first, rest = small_jobs[0], small_jobs[1:]
    for step in order_in:
        swap(step).wait()
        cx = lax.rem(coords[X] + step, SIDE)
        got[cx] = got[cx] + small[core, cx]
        if step in (FAR, LEFT):
            first.start(0, PAIR[step == LEFT:][:1])
    for job in rest:
        job.start(0)
    for job in head_jobs:
        job.finish(0)
        job.start(1)
    for job in small_jobs:
        job.middle(0)
    for job in head_jobs:
        job.middle(1)
    for job in small_jobs:
        job.finish(0)
        job.start(1)
    for job in head_jobs:
        job.finish(1)
    for k in (1, 2):
        for job in small_jobs:
            job.middle(k)
        for job in small_jobs:
            job.finish(k)
            if k < 2:
                job.start(k + 1)
    for p in PARTS:
        for k, job in enumerate(head_jobs):
            own[p, :, lane_slice(k, cols // 2)] = job.phases[-1][5][lane_slice(p, SUBS), :]
    pieces = [(order_i, t) for order_i, width in enumerate(small_parts) for t in range(width // LANES)]
    for n, (which, t) in enumerate(pieces):
        p, at = divmod(n * LANES, span)
        own[p, :, cols + at:cols + at + LANES] = small_jobs[which].phases[-1][5][:, lane_slice(t, LANES)]
    loss_row = jnp.sum(feat_coef * err_rows + kl_coef * kl_ref[...], axis=0, keepdims=True)
    for p in PARTS:
        own[p, :, cols + span:] = jnp.zeros((SUBS, LANES), F32)
    for i, row in enumerate(gain_rows + [loss_row]):
        own[0, i:i + 1, cols + span:] = row
    for job in head_jobs + small_jobs + [in_job]:
        job.drain()


def reduce_grads(dw, dx, feats, x_stud, gain_s, w_up_s, w_down_s, proj_s, kl_tiles, feat_coef, kl_coef, collective_id,
                 small_parts=(1280, 896, 896)):
    rows, cols = dw.shape[2:]
    span = sum(small_parts) // len(PARTS)
    width = cols // 2
    xs_shape = x_stud.shape
    scratch = [pltpu.VMEM((len(PAIR), SIDE, SIDE, SIDE, SUBS, sum(small_parts)), F32),
               pltpu.VMEM((SIDE, SIDE, SIDE, SUBS, sum(small_parts)), F32), pltpu.VMEM((SIDE,) + xs_shape, F32),
               DMA((SIDE,)), DMA((SIDE,)), DMA, DMA]
    for _ in PAIR:
        scratch += RingSum.shapes((Y, Z), (Y, Z), rows, width)
    scratch += RingSum.shapes((X,), (X,), *xs_shape)
    for part in small_parts:
        scratch += RingSum.shapes(AXES, AXES, SUBS, part)
    return pl.pallas_call(
        functools.partial(reduce_kernel, feat_coef, kl_coef, small_parts),
        out_shape=jax.ShapeDtypeStruct((len(PARTS), SUBS, cols + span + LANES), F32),
        in_specs=[IN_VMEM] * 10,
        out_specs=IN_VMEM,
        scratch_shapes=scratch,
        compiler_params=pltpu.CompilerParams(collective_id=collective_id, has_side_effects=True, vmem_limit_bytes=62 * MIB),
        cost_estimate=pl.CostEstimate(flops=MIB * MIB, bytes_accessed=dw.size, transcendentals=0),
        name='reduce',
    )(dw, dx, *feats, x_stud, gain_s, w_up_s, w_down_s, proj_s, kl_tiles)


ALL = pl.ds(0, SIDE)
WHOLE, LOW, HIGH = range(SIDE - 1)
SOURCE = (LEFT, RIGHT)
ARRIVAL = (HERE, LEFT, RIGHT, FAR)


def gather_kernel(cut, own_ref, full, own_sem, send_sem, recv_sem, peer_send, peer_recv):
    coords = chip_coords()
    core = lax.axis_index('tp')
    peer = device(coords, 1 - core)
    width = own_ref.shape[-1]
    widths = (width, width - LANES, width - LANES)
    here = [pltpu.make_async_copy(own_ref.at[p], full.at[(core,) + coords + (p,)], own_sem.at[p]) for p in PARTS]
    for copy in here:
        copy.start()
    greet(near_targets(coords, core))

    def lanes(part, span):
        return pl.ds(cut if span == HIGH else 0, (widths[part], cut, widths[part] - cut)[span])

    def block(part, steps, span=WHOLE):
        idx = list(coords)
        for axis, step in zip(ORDERS[part], steps):
            idx[axis] = ALL if step is ALL else lax.rem(coords[axis] + step, SIDE)
        return full.at[(core,) + tuple(idx) + (part, slice(None), lanes(part, span))]

    def steps_of(phase, sub, step):
        return ((step,), (sub, step), (ALL, sub, step))[phase]

    def ring(part, phase, sub, slot, step, span):
        dst = block(part, steps_of(phase, sub, step), span)
        mine = step == HERE and (phase == 0 or (phase == 1 and sub == HERE))
        src = own_ref.at[part, :, lanes(part, span)] if mine else dst
        at = (part, phase, sub, slot)
        return remote(src, dst, send_sem.at[at], recv_sem.at[at], device(moved(coords, ORDERS[part][phase], WAYS[slot % 2]), core))

    def first(part, phase, sub, d, step):
        return ring(part, phase, sub, d, step, WHOLE)

    def onward(part, phase, sub, d, step):
        return ring(part, phase, sub, d + 2, step, (LOW, HIGH)[d])

    def send(part, phase, sub):
        for d in PAIR:
            first(part, phase, sub, d, HERE).start()

    def relay(part, phase, sub, d):
        first(part, phase, sub, d, SOURCE[d]).wait_recv()
        onward(part, phase, sub, d, SOURCE[d]).start()

    def far_in(part, phase, sub):
        for d in PAIR:
            onward(part, phase, sub, d, FAR).wait_recv()

    def across(part, phase, sub, step):
        dst = block(part, ((step,), (ALL, step), (ALL, sub, step))[phase])
        src = own_ref.at[part, :, lanes(part, WHOLE)] if phase == 0 and step == HERE else dst
        at = (part, phase, sub, step)
        return remote(src, dst, peer_send.at[at], peer_recv.at[at], peer)

    for part in PARTS:
        send(part, 0, HERE)
    for part in PARTS:
        send(part, 1, HERE)
        across(part, 0, HERE, HERE).start()
    for part in PARTS:
        for d in PAIR:
            relay(part, 0, HERE, d)
            send(part, 1, SOURCE[d])
            across(part, 0, HERE, SOURCE[d]).start()
    for part in PARTS:
        far_in(part, 0, HERE)
        send(part, 1, FAR)
        across(part, 0, HERE, FAR).start()
        here[part].wait()
        send(part, 2, HERE)
    for sub in ARRIVAL:
        for part in PARTS:
            for d in PAIR:
                relay(part, 1, sub, d)
                if sub == FAR:
                    send(part, 2, SOURCE[d])
                    across(part, 1, HERE, SOURCE[d]).start()
    for part in PARTS:
        for sub in ARRIVAL:
            far_in(part, 1, sub)
        send(part, 2, FAR)
        across(part, 1, HERE, FAR).start()
    for sub in ARRIVAL:
        for part in PARTS:
            for d in PAIR:
                relay(part, 2, sub, d)
                across(part, 2, sub, SOURCE[d]).start()
    for sub in ARRIVAL:
        for part in PARTS:
            far_in(part, 2, sub)
            across(part, 2, sub, FAR).start()
    for part in PARTS:
        for phase in AXES:
            for sub in ARRIVAL if phase else (HERE,):
                for d in PAIR:
                    first(part, phase, sub, d, HERE).wait_send()
                    onward(part, phase, sub, d, SOURCE[d]).wait_send()
                for step in ARRIVAL if phase == 0 else (LEFT, RIGHT, FAR):
                    if phase != 1 or sub == HERE:
                        across(part, phase, sub, step).wait()


def gather_blocks(own, cut, collective_id):
    sems = DMA((len(PARTS), len(AXES), SIDE, SIDE))
    return pl.pallas_call(
        functools.partial(gather_kernel, cut),
        out_shape=pltpu.VMEM((len(PAIR), SIDE, SIDE, SIDE) + own.shape, F32),
        in_specs=[IN_VMEM],
        out_specs=IN_HBM,
        scratch_shapes=[DMA((len(PARTS),)), sems, sems, sems, sems],
        compiler_params=pltpu.CompilerParams(collective_id=collective_id, has_side_effects=True, vmem_limit_bytes=MIB),
        cost_estimate=pl.CostEstimate(flops=MIB * MIB, bytes_accessed=SIDE * LANES * own.size, transcendentals=0),
        name='gather',
    )(own)


def place_kernel(n_head, lanes_u, lanes_p,
                 full, head, up, down, proj, total,
                 edge, head_sem, edge_sem, wide_sem, narrow_sem):
    last_x = SIDE - 1
    per = up.shape[3]
    copy = pltpu.make_async_copy
    narrow_at = n_head + per * lanes_u
    copies = []
    for c in CORES:
        for x in range(SIDE):
            src = full.at[c, x]
            lo = LANES if (c, x) == PAIR[::-1] else 0
            hi = n_head - LANES if (c, x) == (0, last_x) else n_head
            at = (c * SIDE + x) * n_head - c * LANES
            copies.append(copy(src.at[:, :, :, :, pl.ds(lo, hi - lo)], head.at[:, :, :, :, pl.ds(at + lo, hi - lo)], head_sem.at[c, x]))
            for q in range(per):
                dst = down.at[x, :, :, :, q] if c else up.at[:, :, :, q, :, pl.ds(x * lanes_u, lanes_u)]
                copies.append(copy(src.at[:, :, :, :, pl.ds(n_head + q * lanes_u, lanes_u)], dst, wide_sem.at[c, x, q]))
            copies.append(copy(src.at[:, :, :, :, pl.ds(narrow_at, lanes_p)], proj.at[c, :, :, :, :, pl.ds(x * lanes_p, lanes_p)],
                               narrow_sem.at[c, x]))
    for one in copies:
        one.start()
    edge[...] = full[0, last_x, :, :, :, :, n_head - LANES:n_head] + full[1, 0, :, :, :, :, :LANES]
    edge_copy = copy(edge, head.at[:, :, :, :, pl.ds(SIDE * n_head - LANES, LANES)], edge_sem)
    edge_copy.start()
    tiles = full[:, :, :, :, 0, :, narrow_at + lanes_p:narrow_at + lanes_p + LANES]
    total[...] = jnp.sum(tiles.reshape(-1, SUBS, LANES), axis=0)
    edge_copy.wait()
    for one in copies:
        one.wait()


def place_blocks(full, n_head, lanes_u, lanes_p, vocab):
    n_part, subs, _ = full.shape[4:]
    per = len(PAIR)
    pair = (len(PAIR),)
    owners = pair + (SIDE,)
    yz = (SIDE, SIDE)
    shapes = (yz + (n_part, subs, vocab), yz + (n_part, per, subs, SIDE * lanes_u), (SIDE,) + yz + (n_part, per, subs, lanes_u),
              pair + yz + (n_part, subs, SIDE * lanes_p), (subs, LANES))
    return pl.pallas_call(
        functools.partial(place_kernel, n_head, lanes_u, lanes_p),
        out_shape=tuple(jax.ShapeDtypeStruct(s, F32) for s in shapes),
        in_specs=[IN_VMEM],
        out_specs=(IN_HBM,) * SIDE + (IN_VMEM,),
        scratch_shapes=[pltpu.VMEM(yz + (n_part, subs, LANES), F32), DMA(owners), DMA, DMA(owners + (per,)), DMA(owners)],
        compiler_params=pltpu.CompilerParams(has_side_effects=True, vmem_limit_bytes=MIB),
        name='place',
    )(pltpu.with_memory_space_constraint(full, pltpu.VMEM))


def solution(mesh):
    n_dev = mesh.shape['dp'] * mesh.shape['tp']

    def local_step(x_teach, x_stud, w_up_t, w_down_t, gain_t, head_t, w_up_s, w_down_s, gain_s, proj_s, head_s):
        n_feat, d_in, d_mid = w_up_s.shape
        d_teach = proj_s.shape[-1]
        n_tokens = x_stud.shape[0] * x_stud.shape[1] * n_dev
        feat_coef = 1.0 / (n_feat * n_tokens * d_teach)
        kl_coef = 1.0 / n_tokens
        xs = x_stud[0]
        feat_one, feat_two, states, stud_all = teacher(x_teach, xs, gain_s, w_up_s, w_down_s, gain_t, w_up_t, w_down_t,
                                                       w_up_t.shape[0] // n_feat, 0)
        head_part, in_part, kl_tiles = heads(states, stud_all.reshape(-1, d_in), head_t, head_s, kl_coef, 1)
        cols = head_part.shape[1]
        own = reduce_grads(head_part.reshape(SIDE, SIDE, -1, cols), in_part.reshape((SIDE, -1) + xs.shape), (feat_one, feat_two), xs, gain_s, w_up_s, w_down_s,
                           proj_s, kl_tiles, feat_coef, kl_coef, 2)
        blocks = gather_blocks(own, 20 * LANES, 3)
        head_grad, up, down, proj, total = place_blocks(blocks, cols, d_mid // SIDE, d_teach // SIDE, head_s.shape[1])
        n_gain = n_feat * d_in // LANES
        return (jnp.sum(total[n_gain]), up.reshape(w_up_s.shape), down.reshape(w_down_s.shape), total[:n_gain].reshape(gain_s.shape),
                proj.reshape(proj_s.shape), head_grad.reshape(head_s.shape))

    in_specs = (P('dp', 'tp', None), P(('dp', 'tp'), None, None), P(None, None, 'tp'), P(None, 'tp', None),
                P(), P(None, 'tp'), P(), P(), P(), P(), P())
    out_specs = (P(), P(), P(), P(), P(), P())
    return jax.shard_map(local_step, mesh=mesh, in_specs=in_specs, out_specs=out_specs, check_vma=False)
```

```python
import functools

import jax
import jax.numpy as jnp
from jax import lax
from jax.experimental import pallas as pl
from jax.experimental.pallas import tpu as pltpu
from jax.sharding import PartitionSpec as P

NORM_EPS = 1e-6
MESH = pl.DeviceIdType.MESH
F32, BF16 = jnp.float32, jnp.bfloat16
DMA = pltpu.SemaphoreType.DMA
IN_VMEM = pl.BlockSpec(memory_space=pltpu.VMEM)
IN_HBM = pl.BlockSpec(memory_space=pl.ANY)
LANES = 128
SUBS = 8
SIDE = 4
MIB = 1 << 20
HERE, RIGHT, FAR, LEFT = range(SIDE)
X, Y, Z = AXES = tuple(range(SIDE - RIGHT))
PARTS = AXES
ORDERS = ((X, Y, Z), (Y, Z, X), (Z, X, Y))
CORES = PAIR = (0, 1)
WAYS = (RIGHT, LEFT)


def chip_coords():
    chip = lax.axis_index('dp')
    return lax.rem(chip, SIDE), lax.rem(chip // SIDE, SIDE), chip // (SIDE * SIDE)


def device(coords, core):
    x, y, z = coords
    return {'dp': (z * SIDE + y) * SIDE + x, 'tp': core}


def moved(coords, axis, step):
    out = list(coords)
    out[axis] = lax.rem(out[axis] + step, SIDE)
    return tuple(out)


def remote(src, dst, send_sem, recv_sem, target):
    return pltpu.make_async_remote_copy(src_ref=src, dst_ref=dst, send_sem=send_sem, recv_sem=recv_sem,
                                        device_id=target, device_id_type=MESH)


def greet(targets):
    barrier = pltpu.get_barrier_semaphore()
    for target in targets:
        pl.semaphore_signal(barrier, device_id=target, device_id_type=MESH)
    pl.semaphore_wait(barrier, len(targets))


def group_targets(coords, core):
    return [device(moved(coords, X, step), abs(core - flip)) for step in range(SIDE) for flip in CORES if step or flip]


def near_targets(coords, core):
    return [device(moved(coords, axis, step), core) for axis in AXES for step in WAYS] + [device(coords, 1 - core)]


def lane_slice(k, width):
    return slice(k * width, k * width + width)


def rms_unit(values):
    inv = lax.rsqrt(jnp.mean(values * values, axis=-1, keepdims=True) + NORM_EPS)
    return values * inv, inv


def rms_back(normed, inv_rms, grad_out):
    return inv_rms * (grad_out - normed * jnp.mean(grad_out * normed, axis=-1, keepdims=True))


GELU_C = 0.7978845608028654
GELU_K = 0.044715


def gelu_act(u):
    half = 0.5 * u
    return half + half * jnp.tanh(u * (GELU_C + (GELU_C * GELU_K) * (u * u)))


def gelu_of_half(v):
    return v + v * jnp.tanh(v * (2 * GELU_C + (8 * GELU_C * GELU_K) * (v * v)))


def gelu_slope(u):
    sq = u * u
    t = jnp.tanh(u * (GELU_C + (GELU_C * GELU_K) * sq))
    return 0.5 * (1 + t) + (0.5 * u) * (1 - t * t) * (GELU_C + (3 * GELU_C * GELU_K) * sq)


def dot(a, b):
    return jnp.dot(a, b, preferred_element_type=F32)


def dot_right_t(a, b):
    return lax.dot_general(a, b, (((1,), (1,)), ((), ())), preferred_element_type=F32)


def dot_left_t(a, b):
    return lax.dot_general(a, b, (((0,), (0,)), ((), ())), preferred_element_type=F32)


def student_layers(x_ref, gain_ref, up_ref, down_ref):
    residual = x_ref[...].astype(F32)
    unit, inv = rms_unit(residual)
    saved = []
    for j in range(up_ref.shape[0]):
        normed = (unit * gain_ref[j:j + 1, :]).astype(BF16)
        pre = dot(normed, up_ref[j])
        act = gelu_act(pre).astype(BF16)
        residual = residual + dot(act, down_ref[j])
        unit_next, inv_next = rms_unit(residual)
        saved.append((unit, inv, normed, pre, act, unit_next, inv_next))
        unit, inv = unit_next, inv_next
    return saved, unit.astype(BF16)


def teacher_kernel(feat_at, slots_w,
                   x_hbm, xs_hbm, gs_hbm, ups_hbm, dns_hbm, gain_hbm, wup_hbm, wdn_hbm,
                   feat_hbm, last_hbm, state_hbm, group_hbm,
                   xs_ref, gs_ref, ups_ref, dns_ref, gain_ref, feat_ref, last_ref, state_ref, h, nrm, wu, wd, part, got, r_own,
                   in_sems, out_sems, usem, dsem, xown, xsend, xrecv, ssem, rsem, gsend, grecv):
    me = lax.axis_index('tp')
    coords = chip_coords()
    peer = device(coords, 1 - me)
    n_layers = gain_ref.shape[0]
    rows, seq_half, d_model = x_hbm.shape
    d_ff = wu.shape[-1]

    def up_copy(layer, slot):
        return pltpu.make_async_copy(wup_hbm.at[layer], wu.at[slot], usem.at[slot])

    def down_copy(layer, slot):
        return pltpu.make_async_copy(wdn_hbm.at[layer], wd.at[slot], dsem.at[slot])

    ins = [pltpu.make_async_copy(src, dst, in_sems.at[i]) for i, (src, dst) in enumerate((
        (xs_hbm, xs_ref), (gs_hbm, gs_ref), (ups_hbm, ups_ref), (dns_hbm, dns_ref), (gain_hbm, gain_ref)))]
    mine = pl.ds(pl.multiple_of(me * seq_half, seq_half), seq_half)
    xcopy_own = pltpu.make_async_copy(x_hbm, h.at[:, mine], xown)
    for copy in ins + [xcopy_own]:
        copy.start()
    for i in range(slots_w):
        up_copy(i, i).start()
        down_copy(i, i).start()
    targets = group_targets(coords, me)
    greet(targets)
    xcopy = remote(x_hbm, h.at[:, mine], xsend, xrecv, peer)
    xcopy.start()
    for copy in ins:
        copy.wait()

    _, head_in = student_layers(xs_ref, gs_ref, ups_ref, dns_ref)
    r_own[...] = head_in
    r_copies = [remote(r_own, group_hbm.at[coords[X], me], gsend.at[i], grecv.at[i], target) for i, target in enumerate(targets)]
    for copy in r_copies:
        copy.start()
    r_keep = pltpu.make_async_copy(r_own, group_hbm.at[coords[X], me], out_sems.at[SIDE - 1])
    r_keep.start()
    xcopy.wait()
    xcopy_own.wait()

    def p_copy(ck, slot):
        return remote(part.at[ck, slot], got.at[ck, slot], ssem.at[ck, slot], rsem.at[ck, slot], peer)

    def update(ck, slot):
        p_copy(ck, slot).wait()
        total = part[ck, slot] + got[ck, slot]
        h[ck] = h[ck] + total.astype(BF16)

    def layer_step(layer, _):
        slot = lax.rem(layer, len(PAIR))
        ws = lax.rem(layer, slots_w)
        for ck in range(rows):
            first, last = ck == 0, ck == rows - 1

            @pl.when(layer > 0)
            def _():
                update(ck, 1 - slot)

            @pl.when((layer == feat_at) & (me == ck))
            def _():
                feat_ref[...] = h[ck]

            unit, _ = rms_unit(h[ck].astype(F32))
            nrm[...] = (unit * (0.5 * gain_ref[pl.ds(layer, 1), :])).astype(BF16)
            if first:
                up_copy(layer, ws).wait()
                down_copy(layer, ws).wait()
            halves = []
            for piece in (slice(None, d_ff // 2), slice(d_ff // 2, None)):
                act = gelu_of_half(dot(nrm[...], wu[ws, :, piece])).astype(BF16)
                halves.append(dot(act, wd[ws, piece, :]))
            part[ck, slot] = halves[0] + halves[1]
            p_copy(ck, slot).start()
            if last:
                @pl.when(layer + slots_w < n_layers)
                def _():
                    up_copy(layer + slots_w, ws).start()
                    down_copy(layer + slots_w, ws).start()
        return 0

    lax.fori_loop(0, n_layers, layer_step, 0)
    for ck in range(rows):
        update(ck, (n_layers - 1) % len(PAIR))

        @pl.when(me == ck)
        def _():
            last_ref[...] = h[ck]

        state_ref[ck] = rms_unit(h[ck].astype(F32))[0].astype(BF16)
    outs = [pltpu.make_async_copy(src, dst, out_sems.at[i])
            for i, (src, dst) in enumerate(((feat_ref, feat_hbm), (last_ref, last_hbm), (state_ref, state_hbm)))]
    for copy in outs:
        copy.start()
    for copy in r_copies + outs + [r_keep]:
        copy.wait()


def teacher(x_teach, x_stud, gain_s, w_up_s, w_down_s, gain_t, w_up_t, w_down_t, feat_at, collective_id, slots_w=3):
    n_layers, d_model, d_ff = w_up_t.shape
    rows, seq_half, _ = x_teach.shape
    n_tok = len(PAIR) * seq_half
    n_peers = SIDE * len(PAIR) - 1
    feat = jax.ShapeDtypeStruct((n_tok, d_model), BF16)
    slots = (rows, len(PAIR))
    weights = n_layers * d_model * d_ff
    args = (x_teach, x_stud, gain_s, w_up_s, w_down_s, gain_t, w_up_t, w_down_t)
    return pl.pallas_call(
        functools.partial(teacher_kernel, feat_at, slots_w),
        out_shape=(feat, feat, jax.ShapeDtypeStruct((rows, n_tok, d_model), BF16),
                   jax.ShapeDtypeStruct((SIDE, len(PAIR)) + x_stud.shape, BF16)),
        in_specs=[IN_HBM] * len(args),
        out_specs=(IN_HBM,) * SIDE,
        scratch_shapes=[pltpu.VMEM(a.shape, a.dtype) for a in args[1:-len(PAIR)]] + [
            pltpu.VMEM((n_tok, d_model), BF16), pltpu.VMEM((n_tok, d_model), BF16), pltpu.VMEM((rows, n_tok, d_model), BF16),
            pltpu.VMEM((rows, n_tok, d_model), BF16), pltpu.VMEM((n_tok, d_model), BF16),
            pltpu.VMEM((slots_w, d_model, d_ff), BF16), pltpu.VMEM((slots_w, d_ff, d_model), BF16),
            pltpu.VMEM(slots + (n_tok, d_model), F32), pltpu.VMEM(slots + (n_tok, d_model), F32),
            pltpu.VMEM(x_stud.shape, BF16),
            DMA((len(args),)), DMA((SIDE,)), DMA((slots_w,)), DMA((slots_w,)), DMA, DMA, DMA, DMA(slots), DMA(slots), DMA((n_peers,)), DMA((n_peers,)),
        ],
        compiler_params=pltpu.CompilerParams(collective_id=collective_id, has_side_effects=True, vmem_limit_bytes=63 * MIB),
        cost_estimate=pl.CostEstimate(flops=SIDE * rows * n_tok * weights, bytes_accessed=SIDE * weights, transcendentals=0),
        name='teacher',
    )(*args)


NEG = -1e38
MAX_T, SUM_T, MAX_S, SUM_S = STATS = range(SIDE)
TEACH, STUD = PAIR


def heads_kernel(kl_coef, chunk,
                 t_hbm, r_hbm, ht_hbm, hs_hbm,
                 dw_hbm, dx, kl_ref,
                 r_ref, tg, rt, ht, hs, zt, zs, mx, sm, st_send, st_all, lcol, grad,
                 ht_sem, hs_sem, t_sem, r_sem, ring_send, ring_recv, peer_send, peer_recv, st_send_sem, st_recv_sem, out_sem):
    coords = chip_coords()
    x = coords[X]
    core = lax.axis_index('tp')
    peer = device(coords, 1 - core)
    rows, n_tok, d_model = t_hbm.shape
    d_stud, cols = hs.shape
    n_tiles = cols // LANES
    blk = rows * n_tok
    n_all = SIDE * blk
    half_tile = LANES // 2
    last_x = SIDE - 1

    first_tile = n_tiles * x + core * (n_tiles * SIDE - 1)
    hs_copy = pltpu.make_async_copy(hs_hbm.at[:, pl.ds(pl.multiple_of(first_tile * LANES, LANES), cols)], hs, hs_sem)
    hs_copy.start()
    r_copy = pltpu.make_async_copy(r_hbm, r_ref, r_sem)
    r_copy.start()
    t_copy = pltpu.make_async_copy(t_hbm, tg.at[x], t_sem)
    t_copy.start()
    cut_low = (core == 1) & (x == 0)
    cut_high = (core == 0) & (x == last_x)

    def ht_copy(src, dst, n):
        return pltpu.make_async_copy(ht_hbm.at[pl.ds(src, n)], ht.at[pl.ds(dst, n)], ht_sem)

    def each_ht(act):
        @pl.when(jnp.logical_not(cut_low | cut_high))
        def _():
            act(ht_copy(pl.multiple_of(cols * x - half_tile * core, half_tile), 0, cols))

        @pl.when(cut_low)
        def _():
            act(ht_copy(0, half_tile, cols - half_tile))

        @pl.when(cut_high)
        def _():
            act(ht_copy(last_x * cols, 0, cols - half_tile))

    each_ht(lambda copy: copy.start())
    targets = group_targets(coords, core)
    greet(targets)

    far_rows = n_tok // 2

    def at(step):
        return lax.rem(x + step, SIDE)

    def ring(k, src, dst, step):
        return remote(src, dst, ring_send.at[k], ring_recv.at[k], device(moved(coords, X, step), core))

    def onward(k, step, way):
        piece = tg.at[at(step), core, pl.ds(k * far_rows, far_rows)]
        return ring(k + len(PAIR), piece, piece, way)

    def first(k, step, way):
        return ring(k, t_hbm.at[core], tg.at[at(step), core], way)

    def across(step, side):
        piece = tg.at[at(step), side]
        return remote(piece, piece, peer_send.at[step - 1], peer_recv.at[step - 1], peer)

    opposite = (LEFT, RIGHT)
    for k, way in enumerate(WAYS):
        first(k, HERE, way).start()
    r_copy.wait()
    rt[...] = r_ref[...].T
    lane = lax.broadcasted_iota(jnp.int32, (blk, LANES), 1)
    low = jnp.where(cut_low, half_tile, 0)
    high = jnp.where(cut_high, half_tile, LANES)

    def finish(kind, b, ref):
        head, tail = lane_slice(0, LANES), lane_slice(n_tiles - 1, LANES)
        ref[b, :, head] = jnp.where(lane >= low, ref[b, :, head], NEG)
        ref[b, :, tail] = jnp.where(lane < high, ref[b, :, tail], NEG)
        tiles = [lane_slice(k, LANES) for k in range(n_tiles)]
        peak = functools.reduce(jnp.maximum, [ref[b, :, t] for t in tiles])
        mx[kind, b] = peak
        sm[kind, b] = functools.reduce(jnp.add, [jnp.exp(ref[b, :, t] - peak) for t in tiles])

    def tokens(b):
        return pl.ds(pl.multiple_of(b * blk, blk), blk)

    def student_logits(b, _):
        zs[b] = dot(r_ref[tokens(b), :], hs[...])
        finish(STUD, b, zs)
        return 0

    hs_copy.wait()
    lax.fori_loop(0, FAR, student_logits, 0)
    for k, way in enumerate(WAYS):
        first(k, opposite[k], way).wait_recv()
        onward(k, opposite[k], way).start()
        across(opposite[k], core).start()
    lax.fori_loop(FAR, SIDE, student_logits, 0)
    each_ht(lambda copy: copy.wait())
    t_copy.wait()

    def teacher_logits(i, _):
        for step, turn in ((RIGHT, 1), (LEFT, 2), (FAR, 3)):
            @pl.when(i == turn)
            def _():
                if step == RIGHT:
                    for k, way in enumerate(WAYS):
                        onward(k, FAR, way).wait_recv()
                    across(FAR, core).start()
                across(step, 1 - core).wait_recv()

        b = at(jnp.where(i < FAR, i, SIDE + 1 - i))
        zt[b] = dot_right_t(tg[b].reshape(blk, d_model), ht[...])
        finish(TEACH, b, zt)
        return 0

    lax.fori_loop(0, SIDE, teacher_logits, 0)

    def merge(b, _):
        out = jnp.zeros((blk, LANES), F32)
        for kind in PAIR:
            peak = jnp.max(mx[kind, b], axis=-1, keepdims=True)
            total = jnp.sum(sm[kind, b] * jnp.exp(mx[kind, b] - peak), axis=-1, keepdims=True)
            out = jnp.where(lane == 2 * kind, peak, jnp.where(lane == 2 * kind + 1, total, out))
        st_send[:, tokens(b)] = out.T[:SUBS, :]
        return 0

    lax.fori_loop(0, SIDE, merge, 0)
    n_peers = len(targets)
    stats = [remote(st_send, st_all.at[i], st_send_sem.at[i], st_recv_sem.at[i], target) for i, target in enumerate(targets)]
    for copy in stats:
        copy.start()
    st_all[n_peers] = st_send[...]
    for copy in stats:
        copy.wait()
    sub = lax.broadcasted_iota(jnp.int32, (LANES, n_all), 0)
    both = jnp.zeros((LANES, n_all), F32)
    for kind in PAIR:
        peaks, totals = st_all[:, 2 * kind, :], st_all[:, 2 * kind + 1, :]
        peak = jnp.max(peaks, axis=0, keepdims=True)
        norm = peak + jnp.log(jnp.sum(totals * jnp.exp(peaks - peak), axis=0, keepdims=True))
        both = jnp.where(sub == kind, norm, both)
    lcol[...] = both.T
    kl_ref[...] = jnp.zeros_like(kl_ref)
    dx[...] = jnp.zeros_like(dx)

    def grad_step(j, _):
        lanes = pl.ds(pl.multiple_of(j * chunk, LANES), chunk)

        def block(b, _):
            tok = tokens(b)
            log_pt = zt[b, :, lanes] - lcol[tok, TEACH:TEACH + 1]
            log_ps = zs[b, :, lanes] - lcol[tok, STUD:STUD + 1]
            pt = jnp.exp(log_pt)
            grad[tok, :] = (kl_coef * (jnp.exp(log_ps) - pt)).astype(BF16)
            kl = pt * (log_pt - log_ps)
            kl = functools.reduce(jnp.add, [kl[:, lane_slice(k, LANES)] for k in range(chunk // LANES)])
            kl_ref[...] += functools.reduce(jnp.add, [kl[lane_slice(k, SUBS)] for k in range(blk // SUBS)])
            return 0

        lax.fori_loop(0, SIDE, block, 0)
        dw = dot(rt[...], grad[...])
        zt[0, :, lanes] = dw[:blk]
        zt[1, :d_stud - blk, lanes] = dw[blk:]
        dx[...] += dot_right_t(grad[...], hs[:, lanes])
        return 0

    lax.fori_loop(0, cols // chunk, grad_step, 0)
    outs = [pltpu.make_async_copy(zt.at[k, pl.ds(0, n)], dw_hbm.at[pl.ds(k * blk, n)], out_sem.at[k])
            for k, n in enumerate((blk, d_stud - blk))]
    for copy in outs:
        copy.start()

    for k, way in enumerate(WAYS):
        first(k, HERE, way).wait_send()
        onward(k, opposite[k], way).wait_send()
    for step in (RIGHT, FAR, LEFT):
        across(step, core).wait_send()
    for copy in outs:
        copy.wait()


def heads(states, stud_all, head_t, head_s, kl_coef, collective_id, chunk=768):
    rows, n_tok, d_model = states.shape
    n_all, d_stud = stud_all.shape
    cols = -(-head_t.shape[1] // (LANES * SIDE)) * LANES
    blk = rows * n_tok
    n_peers = SIDE * len(PAIR) - 1
    v = pltpu.VMEM
    hops = (SIDE - 1,)
    return pl.pallas_call(
        functools.partial(heads_kernel, kl_coef, chunk),
        out_shape=(jax.ShapeDtypeStruct((d_stud, cols), F32), jax.ShapeDtypeStruct((n_all, d_stud), F32),
                   jax.ShapeDtypeStruct((SUBS, LANES), F32)),
        in_specs=[IN_HBM] * SIDE,
        out_specs=(IN_HBM, IN_VMEM, IN_VMEM),
        scratch_shapes=[
            v((n_all, d_stud), BF16), v((SIDE, rows, n_tok, d_model), BF16), v((d_stud, n_all), BF16), v((cols, d_model), BF16), v((d_stud, cols), BF16),
            v((SIDE, blk, cols), F32), v((SIDE, blk, cols), F32),
            v((len(PAIR), SIDE, blk, LANES), F32), v((len(PAIR), SIDE, blk, LANES), F32),
            v((SUBS, n_all), F32), v((n_peers + 1, SUBS, n_all), F32), v((n_all, LANES), F32),
            v((n_all, chunk), BF16),
            DMA, DMA, DMA, DMA, DMA((SIDE,)), DMA((SIDE,)), DMA(hops), DMA(hops), DMA((n_peers,)), DMA((n_peers,)), DMA((len(PAIR),)),
        ],
        compiler_params=pltpu.CompilerParams(collective_id=collective_id, has_side_effects=True, vmem_limit_bytes=63 * MIB),
        cost_estimate=pl.CostEstimate(flops=d_model * n_all * cols, bytes_accessed=d_model * cols, transcendentals=0),
        name='heads',
    )(states, stud_all, head_t.T, head_s)


class RingSum:
    def __init__(self, coords, core, src, dims, order, lanes, bufs, loads=None):
        self.coords, self.core, self.order, self.lanes = coords, core, order, lanes
        self.loads = src if loads is None else loads
        self.phases = []
        for axis, (half, full, mid, send, recv) in zip(order, bufs):
            self.phases.append((src, dims, axis, half, full, mid, send, recv))
            src, dims = mid, tuple(d for d in dims if d != axis)

    @staticmethod
    def shapes(dims, order, rows, width):
        out = []
        for _ in order:
            dims = dims[1:]
            lead = (SIDE,) * len(dims)
            part = (SIDE // 2,) + lead[1:] + (rows, width) if lead else (rows, -(-width // (2 * LANES)) * LANES)
            out += [pltpu.VMEM(PAIR_DIM + part, F32), pltpu.VMEM(PAIR_DIM + lead + (rows, width), F32),
                    pltpu.VMEM(lead + (rows, width), F32), DMA((3 * len(PAIR),)), DMA((3 * len(PAIR),))]
        return out

    def place(self, axis, step):
        return lax.rem(self.coords[axis] + step, SIDE)

    def split(self, k, side):
        _, dims, _, half, full, _, _, _ = self.phases[k]
        width, cut = full.shape[-1], half.shape[-1]
        if len(dims) > 1:
            return (pl.ds(side * (SIDE // 2), SIDE // 2),) + (slice(None),) * (len(dims) - 2), (0, width)
        return (), ((cut, width - cut) if side else (0, cut))

    def pick(self, k, at, side):
        src, dims, axis = self.phases[k][:3]
        lead, (lo, n) = ((slice(None),) * (len(dims) - 1), (0, self.phases[k][4].shape[-1])) if side is None else self.split(k, side)
        lead = list(lead)
        lead.insert(dims.index(axis), at)
        base = self.lanes if k == 0 else 0
        return src, tuple(lead) + (slice(None), pl.ds(base + lo, n))

    def held(self, k, at, side):
        src, idx = self.pick(k, at, side)
        return (src if k else self.loads), idx

    def copy(self, k, turn, d):
        _, _, axis, half, full, _, send, recv = self.phases[k]
        way = WAYS[d]
        i = turn * len(PAIR) + d
        side = d if turn != 1 else 1 - d
        lead, (lo, n) = self.split(k, side)
        window = (slice(None), pl.ds(lo, n))
        if turn == 0:
            ref, idx = self.pick(k, self.place(axis, FAR), side)
            src, dst = ref.at[idx], half.at[d, ..., pl.ds(0, n)]
        elif turn == 1:
            ref, idx = self.pick(k, self.place(axis, way), side)
            src, dst = ref.at[idx], full.at[(d,) + lead + window]
        else:
            src, dst = half.at[d, ..., pl.ds(0, n)], full.at[(d,) + lead + window]
        return remote(src, dst, send.at[i], recv.at[i], device(moved(self.coords, axis, way), self.core))

    def start(self, k, turns=PAIR):
        for turn in turns:
            for d in PAIR:
                self.copy(k, turn, d).start()

    def middle(self, k):
        _, _, axis, half, _, _, _, _ = self.phases[k]
        for d in PAIR:
            self.copy(k, 0, d).wait_recv()
            ref, idx = self.held(k, self.place(axis, WAYS[d]), d)
            n = self.split(k, d)[1][1]
            half[d, ..., :n] = half[d, ..., :n] + ref[idx]
            self.copy(k, len(PAIR), d).start()

    def finish(self, k):
        _, _, axis, _, full, mid, _, _ = self.phases[k]
        for d in PAIR:
            for turn in (1, len(PAIR)):
                self.copy(k, turn, d).wait_recv()
        ref, idx = self.held(k, self.coords[axis], None)
        mid[...] = ref[idx] + full[0] + full[1]

    def drain(self):
        for k in range(len(self.order)):
            for turn in range(3):
                for d in PAIR:
                    self.copy(k, turn, d).wait_send()


PAIR_DIM = (len(PAIR),)


def small_places(n_feat, d_in, d_mid, d_teach):
    groups_up = d_in // SUBS
    yz = SIDE * SIDE
    per_up = n_feat * groups_up // yz
    lanes_u, lanes_p = d_mid // SIDE, d_teach // SIDE
    per_p = groups_up // yz
    span = per_up // per_p * lanes_u + lanes_p
    return groups_up, yz, per_up, lanes_u, lanes_p, per_p, span


def reduce_kernel(feat_coef, kl_coef, small_parts,
                  dw_hbm, feat_a_hbm, feat_b_hbm, xs_hbm, gs_hbm, ups_hbm, dns_hbm, proj_hbm, dx_ref, kl_ref,
                  own, dw, feat_a, feat_b, xs_ref, gs_ref, ups_ref, dns_ref, proj_ref, in_sems, small, got, part_in, swap_send, swap_recv, in_send, in_recv, *bufs):
    coords = chip_coords()
    core = lax.axis_index('tp')
    peer = device(coords, 1 - core)
    loads = [pltpu.make_async_copy(src, dst, in_sems.at[i]) for i, (src, dst) in enumerate((
        (dw_hbm, dw), (feat_a_hbm, feat_a), (feat_b_hbm, feat_b), (xs_hbm, xs_ref), (gs_hbm, gs_ref), (ups_hbm, ups_ref),
        (dns_hbm, dns_ref), (proj_hbm, proj_ref)))]
    for copy in loads[::-1]:
        copy.start()
    greet(near_targets(coords, core))
    cols = dw.shape[-1]
    bufs = list(bufs)

    def take(n):
        out = [tuple(bufs[5 * i:5 * i + 5]) for i in range(n)]
        del bufs[:5 * n]
        return out

    head_jobs = [RingSum(coords, core, dw_hbm, (Y, Z), order, k * (cols // 2), take(2), dw) for k, order in enumerate(((Y, Z), (Z, Y)))]
    in_job = RingSum(coords, core, part_in, (X,), (X,), 0, take(1))
    for job in head_jobs:
        job.start(0)
    in_swap = remote(dx_ref.at[:, 1 - core], part_in, in_send, in_recv, peer)
    in_swap.start()

    for copy in loads:
        copy.wait()
    saved, _ = student_layers(xs_ref, gs_ref, ups_ref, dns_ref)
    in_swap.wait()
    part_in[...] = part_in[...] + dx_ref[:, core]
    in_job.start(0)
    feats = (feat_a, feat_b)
    n_feat, d_in, d_mid = ups_ref.shape
    groups, yz, per_up, lanes_u, lanes_p, per_p, span = small_places(n_feat, d_in, d_mid, proj_ref.shape[-1])
    two = per_up // per_p
    err_rows = jnp.zeros((SUBS, LANES), F32)
    out_grads, gain_rows = [], []

    def put(keep, chip_x, group, per, base, lanes, value):
        block, g = divmod(group, per)
        y, z = divmod(block, SIDE)
        part, q = divmod(g, per // per_p)
        small[keep, chip_x, y, z, :, part * span + base + q * lanes:part * span + base + q * lanes + lanes] = value

    for j in range(n_feat):
        proj_in = saved[j][5].astype(BF16)
        err = dot(proj_in, proj_ref[j]) - feats[j][...].astype(F32)
        sq = err * err
        sq = functools.reduce(jnp.add, [sq[:, lane_slice(k, LANES)] for k in range(sq.shape[1] // LANES)])
        err_rows = err_rows + functools.reduce(jnp.add, [sq[lane_slice(k, SUBS)] for k in range(sq.shape[0] // SUBS)])
        err_grad = ((2 * feat_coef) * err).astype(BF16)
        g_proj = dot_left_t(proj_in, err_grad)
        for i in range(groups):
            for cx in range(SIDE):
                put(j, cx, i, per_p, two * lanes_u, lanes_p, g_proj[lane_slice(i, SUBS), lane_slice(cx, lanes_p)])
        out_grads.append(dot_right_t(err_grad, proj_ref[j]))
    in_job.middle(0)
    for job in head_jobs:
        job.middle(0)
    in_job.finish(0)
    out_grads[-1] = out_grads[-1] + in_job.phases[-1][5][...]
    resid_grad = None
    for j in reversed(range(n_feat)):
        unit, inv, normed, pre, act, unit_next, inv_next = saved[j]
        step_grad = rms_back(unit_next, inv_next, out_grads[j])
        resid_grad = step_grad if resid_grad is None else resid_grad + step_grad
        resid_bf = resid_grad.astype(BF16)
        g_down = dot_left_t(act, resid_bf)
        n_down = d_mid // SUBS
        for i in range(n_down):
            cx, rest = divmod(j * n_down + i, n_feat * n_down // SIDE)
            put(1, cx, rest, per_up, 0, lanes_u, g_down[lane_slice(i, SUBS), :])
        pre_grad = (gelu_slope(pre) * dot_right_t(resid_bf, dns_ref[j])).astype(BF16)
        g_up = dot_left_t(normed, pre_grad)
        for i in range(groups):
            for cx in range(SIDE):
                put(0, cx, j * groups + i, per_up, 0, lanes_u, g_up[lane_slice(i, SUBS), lane_slice(cx, lanes_u)])
        norm_grad = dot_right_t(pre_grad, ups_ref[j])
        g_gain = jnp.sum(norm_grad * unit, axis=0, keepdims=True)
        gain_rows = [g_gain[:, lane_slice(k, LANES)] for k in range(d_in // LANES)] + gain_rows
        if j > 0:
            resid_grad = resid_grad + rms_back(unit, inv, norm_grad * gs_ref[j:j + 1, :])

    def swap(step):
        cx = lax.rem(coords[X] + step, SIDE)
        return remote(small.at[1 - core, cx], got.at[cx], swap_send.at[step], swap_recv.at[step], peer)

    order_in = (FAR, RIGHT, LEFT, HERE)
    for step in order_in:
        swap(step).start()
    lo = 0
    small_jobs = []
    for order, width in zip(ORDERS, small_parts):
        small_jobs.append(RingSum(coords, core, got, AXES, order, lo, take(3)))
        lo += width
    first, rest = small_jobs[0], small_jobs[1:]
    for job in head_jobs:
        job.finish(0)
        job.start(1)
    for step in order_in:
        swap(step).wait()
        cx = lax.rem(coords[X] + step, SIDE)
        got[cx] = got[cx] + small[core, cx]
        if step in (FAR, LEFT):
            first.start(0, PAIR[step == LEFT:][:1])
    for job in head_jobs:
        job.middle(1)
    for job in rest:
        job.start(0)
    for job in small_jobs:
        job.middle(0)
    for job in head_jobs:
        job.finish(1)
    for job in small_jobs:
        job.finish(0)
        job.start(1)
    for k in (1, 2):
        for job in small_jobs:
            job.middle(k)
        for job in small_jobs:
            job.finish(k)
            if k < 2:
                job.start(k + 1)
    for p in PARTS:
        for k, job in enumerate(head_jobs):
            own[p, :, lane_slice(k, cols // 2)] = job.phases[-1][5][lane_slice(p, SUBS), :]
    pieces = [(order_i, t) for order_i, width in enumerate(small_parts) for t in range(width // LANES)]
    for n, (which, t) in enumerate(pieces):
        p, at = divmod(n * LANES, span)
        own[p, :, cols + at:cols + at + LANES] = small_jobs[which].phases[-1][5][:, lane_slice(t, LANES)]
    loss_row = jnp.sum(feat_coef * err_rows + kl_coef * kl_ref[...], axis=0, keepdims=True)
    for p in PARTS:
        own[p, :, cols + span:] = jnp.zeros((SUBS, LANES), F32)
    for i, row in enumerate(gain_rows + [loss_row]):
        own[0, i:i + 1, cols + span:] = row
    for job in head_jobs + small_jobs + [in_job]:
        job.drain()


def reduce_grads(dw, dx, feats, x_stud, gain_s, w_up_s, w_down_s, proj_s, kl_tiles, feat_coef, kl_coef, collective_id,
                 small_parts=(1280, 896, 896)):
    rows, cols = dw.shape[2:]
    span = sum(small_parts) // len(PARTS)
    width = cols // 2
    xs_shape = x_stud.shape
    args = (dw, *feats, x_stud, gain_s, w_up_s, w_down_s, proj_s)
    scratch = [pltpu.VMEM(a.shape, a.dtype) for a in args]
    scratch += [DMA((len(args),)), pltpu.VMEM((len(PAIR), SIDE, SIDE, SIDE, SUBS, sum(small_parts)), F32),
               pltpu.VMEM((SIDE, SIDE, SIDE, SUBS, sum(small_parts)), F32), pltpu.VMEM((SIDE,) + xs_shape, F32),
               DMA((SIDE,)), DMA((SIDE,)), DMA, DMA]
    for _ in PAIR:
        scratch += RingSum.shapes((Y, Z), (Y, Z), rows, width)
    scratch += RingSum.shapes((X,), (X,), *xs_shape)
    for part in small_parts:
        scratch += RingSum.shapes(AXES, AXES, SUBS, part)
    return pl.pallas_call(
        functools.partial(reduce_kernel, feat_coef, kl_coef, small_parts),
        out_shape=jax.ShapeDtypeStruct((len(PARTS), SUBS, cols + span + LANES), F32),
        in_specs=[IN_HBM] * len(args) + [IN_VMEM] * len(PAIR),
        out_specs=IN_VMEM,
        scratch_shapes=scratch,
        compiler_params=pltpu.CompilerParams(collective_id=collective_id, has_side_effects=True, vmem_limit_bytes=63 * MIB),
        cost_estimate=pl.CostEstimate(flops=MIB * MIB, bytes_accessed=dw.size, transcendentals=0),
        name='reduce',
    )(*args, dx, kl_tiles)


ALL = pl.ds(0, SIDE)
WHOLE, LOW, HIGH = range(SIDE - 1)
SOURCE = (LEFT, RIGHT)
ARRIVAL = (HERE, LEFT, RIGHT, FAR)


def gather_kernel(cut, own_ref, full, own_sem, send_sem, recv_sem, peer_send, peer_recv):
    coords = chip_coords()
    core = lax.axis_index('tp')
    peer = device(coords, 1 - core)
    width = own_ref.shape[-1]
    widths = (width, width - LANES, width - LANES)
    here = [pltpu.make_async_copy(own_ref.at[p], full.at[(core,) + coords + (p,)], own_sem.at[p]) for p in PARTS]
    for copy in here:
        copy.start()
    greet(near_targets(coords, core))

    def lanes(part, span):
        return pl.ds(cut if span == HIGH else 0, (widths[part], cut, widths[part] - cut)[span])

    def block(part, steps, span=WHOLE):
        idx = list(coords)
        for axis, step in zip(ORDERS[part], steps):
            idx[axis] = ALL if step is ALL else lax.rem(coords[axis] + step, SIDE)
        return full.at[(core,) + tuple(idx) + (part, slice(None), lanes(part, span))]

    def steps_of(phase, sub, step):
        return ((step,), (sub, step), (ALL, sub, step))[phase]

    def ring(part, phase, sub, slot, step, span):
        dst = block(part, steps_of(phase, sub, step), span)
        mine = step == HERE and (phase == 0 or (phase == 1 and sub == HERE))
        src = own_ref.at[part, :, lanes(part, span)] if mine else dst
        at = (part, phase, sub, slot)
        return remote(src, dst, send_sem.at[at], recv_sem.at[at], device(moved(coords, ORDERS[part][phase], WAYS[slot % 2]), core))

    def first(part, phase, sub, d, step):
        return ring(part, phase, sub, d, step, WHOLE)

    def onward(part, phase, sub, d, step):
        return ring(part, phase, sub, d + 2, step, (LOW, HIGH)[d])

    def send(part, phase, sub):
        for d in PAIR:
            first(part, phase, sub, d, HERE).start()

    def relay(part, phase, sub, d):
        first(part, phase, sub, d, SOURCE[d]).wait_recv()
        onward(part, phase, sub, d, SOURCE[d]).start()

    def far_in(part, phase, sub):
        for d in PAIR:
            onward(part, phase, sub, d, FAR).wait_recv()

    def across(part, phase, sub, step):
        dst = block(part, ((step,), (ALL, step), (ALL, sub, step))[phase])
        src = own_ref.at[part, :, lanes(part, WHOLE)] if phase == 0 and step == HERE else dst
        at = (part, phase, sub, step)
        return remote(src, dst, peer_send.at[at], peer_recv.at[at], peer)

    for part in PARTS:
        send(part, 0, HERE)
    for part in PARTS:
        send(part, 1, HERE)
        across(part, 0, HERE, HERE).start()
    for part in PARTS:
        for d in PAIR:
            relay(part, 0, HERE, d)
            send(part, 1, SOURCE[d])
            across(part, 0, HERE, SOURCE[d]).start()
    for part in PARTS:
        far_in(part, 0, HERE)
        send(part, 1, FAR)
        across(part, 0, HERE, FAR).start()
        here[part].wait()
        send(part, 2, HERE)
    for sub in ARRIVAL:
        for part in PARTS:
            for d in PAIR:
                relay(part, 1, sub, d)
                if sub == FAR:
                    send(part, 2, SOURCE[d])
                    across(part, 1, HERE, SOURCE[d]).start()
    for part in PARTS:
        for sub in ARRIVAL:
            far_in(part, 1, sub)
        send(part, 2, FAR)
        across(part, 1, HERE, FAR).start()
    for sub in ARRIVAL:
        for part in PARTS:
            for d in PAIR:
                relay(part, 2, sub, d)
                across(part, 2, sub, SOURCE[d]).start()
    for sub in ARRIVAL:
        for part in PARTS:
            far_in(part, 2, sub)
            across(part, 2, sub, FAR).start()
    for part in PARTS:
        for phase in AXES:
            for sub in ARRIVAL if phase else (HERE,):
                for d in PAIR:
                    first(part, phase, sub, d, HERE).wait_send()
                    onward(part, phase, sub, d, SOURCE[d]).wait_send()
                for step in ARRIVAL if phase == 0 else (LEFT, RIGHT, FAR):
                    if phase != 1 or sub == HERE:
                        across(part, phase, sub, step).wait()


def gather_blocks(own, cut, collective_id):
    sems = DMA((len(PARTS), len(AXES), SIDE, SIDE))
    return pl.pallas_call(
        functools.partial(gather_kernel, cut),
        out_shape=pltpu.VMEM((len(PAIR), SIDE, SIDE, SIDE) + own.shape, F32),
        in_specs=[IN_VMEM],
        out_specs=IN_HBM,
        scratch_shapes=[DMA((len(PARTS),)), sems, sems, sems, sems],
        compiler_params=pltpu.CompilerParams(collective_id=collective_id, has_side_effects=True, vmem_limit_bytes=MIB),
        cost_estimate=pl.CostEstimate(flops=MIB * MIB, bytes_accessed=SIDE * LANES * own.size, transcendentals=0),
        name='gather',
    )(own)


def place_kernel(n_head, lanes_u, lanes_p,
                 full, head, up, down, proj, total,
                 edge, head_sem, edge_sem, wide_sem, narrow_sem):
    last_x = SIDE - 1
    per = up.shape[3]
    copy = pltpu.make_async_copy
    narrow_at = n_head + per * lanes_u
    copies = []
    for c in CORES:
        for x in range(SIDE):
            src = full.at[c, x]
            lo = LANES if (c, x) == PAIR[::-1] else 0
            hi = n_head - LANES if (c, x) == (0, last_x) else n_head
            at = (c * SIDE + x) * n_head - c * LANES
            copies.append(copy(src.at[:, :, :, :, pl.ds(lo, hi - lo)], head.at[:, :, :, :, pl.ds(at + lo, hi - lo)], head_sem.at[c, x]))
            for q in range(per):
                dst = down.at[x, :, :, :, q] if c else up.at[:, :, :, q, :, pl.ds(x * lanes_u, lanes_u)]
                copies.append(copy(src.at[:, :, :, :, pl.ds(n_head + q * lanes_u, lanes_u)], dst, wide_sem.at[c, x, q]))
            copies.append(copy(src.at[:, :, :, :, pl.ds(narrow_at, lanes_p)], proj.at[c, :, :, :, :, pl.ds(x * lanes_p, lanes_p)],
                               narrow_sem.at[c, x]))
    for one in copies:
        one.start()
    edge[...] = full[0, last_x, :, :, :, :, n_head - LANES:n_head] + full[1, 0, :, :, :, :, :LANES]
    edge_copy = copy(edge, head.at[:, :, :, :, pl.ds(SIDE * n_head - LANES, LANES)], edge_sem)
    edge_copy.start()
    tiles = full[:, :, :, :, 0, :, narrow_at + lanes_p:narrow_at + lanes_p + LANES]
    total[...] = jnp.sum(tiles.reshape(-1, SUBS, LANES), axis=0)
    edge_copy.wait()
    for one in copies:
        one.wait()


def place_blocks(full, n_head, lanes_u, lanes_p, vocab):
    n_part, subs, _ = full.shape[4:]
    per = len(PAIR)
    pair = (len(PAIR),)
    owners = pair + (SIDE,)
    yz = (SIDE, SIDE)
    shapes = (yz + (n_part, subs, vocab), yz + (n_part, per, subs, SIDE * lanes_u), (SIDE,) + yz + (n_part, per, subs, lanes_u),
              pair + yz + (n_part, subs, SIDE * lanes_p), (subs, LANES))
    return pl.pallas_call(
        functools.partial(place_kernel, n_head, lanes_u, lanes_p),
        out_shape=tuple(jax.ShapeDtypeStruct(s, F32) for s in shapes),
        in_specs=[IN_VMEM],
        out_specs=(IN_HBM,) * SIDE + (IN_VMEM,),
        scratch_shapes=[pltpu.VMEM(yz + (n_part, subs, LANES), F32), DMA(owners), DMA, DMA(owners + (per,)), DMA(owners)],
        compiler_params=pltpu.CompilerParams(has_side_effects=True, vmem_limit_bytes=MIB),
        name='place',
    )(pltpu.with_memory_space_constraint(full, pltpu.VMEM))


def solution(mesh):
    n_dev = mesh.shape['dp'] * mesh.shape['tp']

    def local_step(x_teach, x_stud, w_up_t, w_down_t, gain_t, head_t, w_up_s, w_down_s, gain_s, proj_s, head_s):
        n_feat, d_in, d_mid = w_up_s.shape
        d_teach = proj_s.shape[-1]
        n_tokens = x_stud.shape[0] * x_stud.shape[1] * n_dev
        feat_coef = 1.0 / (n_feat * n_tokens * d_teach)
        kl_coef = 1.0 / n_tokens
        xs = x_stud[0]
        feat_one, feat_two, states, stud_all = teacher(x_teach, xs, gain_s, w_up_s, w_down_s, gain_t, w_up_t, w_down_t,
                                                       w_up_t.shape[0] // n_feat, 0)
        head_part, in_part, kl_tiles = heads(states, stud_all.reshape(-1, d_in), head_t, head_s, kl_coef, 1)
        cols = head_part.shape[1]
        own = reduce_grads(head_part.reshape(SIDE, SIDE, -1, cols), in_part.reshape((SIDE, -1) + xs.shape), (feat_one, feat_two), xs, gain_s, w_up_s, w_down_s,
                           proj_s, kl_tiles, feat_coef, kl_coef, 2)
        blocks = gather_blocks(own, 20 * LANES, 3)
        head_grad, up, down, proj, total = place_blocks(blocks, cols, d_mid // SIDE, d_teach // SIDE, head_s.shape[1])
        n_gain = n_feat * d_in // LANES
        return (jnp.sum(total[n_gain]), up.reshape(w_up_s.shape), down.reshape(w_down_s.shape), total[:n_gain].reshape(gain_s.shape),
                proj.reshape(proj_s.shape), head_grad.reshape(head_s.shape))

    in_specs = (P('dp', 'tp', None), P(('dp', 'tp'), None, None), P(None, None, 'tp'), P(None, 'tp', None),
                P(), P(None, 'tp'), P(), P(), P(), P(), P())
    out_specs = (P(), P(), P(), P(), P(), P())
    return jax.shard_map(local_step, mesh=mesh, in_specs=in_specs, out_specs=out_specs, check_vma=False)
```

```python
import functools

import jax
import jax.numpy as jnp
from jax import lax
from jax.experimental import pallas as pl
from jax.experimental.pallas import tpu as pltpu
from jax.sharding import PartitionSpec as P

NORM_EPS = 1e-6
MESH = pl.DeviceIdType.MESH
F32, BF16 = jnp.float32, jnp.bfloat16
DMA = pltpu.SemaphoreType.DMA
IN_VMEM = pl.BlockSpec(memory_space=pltpu.VMEM)
IN_HBM = pl.BlockSpec(memory_space=pl.ANY)
LANES = 128
SUBS = 8
SIDE = 4
MIB = 1 << 20
HERE, RIGHT, FAR, LEFT = range(SIDE)
X, Y, Z = AXES = tuple(range(SIDE - RIGHT))
PARTS = AXES
ORDERS = ((X, Y, Z), (Y, Z, X), (Z, X, Y))
CORES = PAIR = (0, 1)
WAYS = (RIGHT, LEFT)


def chip_coords():
    chip = lax.axis_index('dp')
    return lax.rem(chip, SIDE), lax.rem(chip // SIDE, SIDE), chip // (SIDE * SIDE)


def device(coords, core):
    x, y, z = coords
    return {'dp': (z * SIDE + y) * SIDE + x, 'tp': core}


def moved(coords, axis, step):
    out = list(coords)
    out[axis] = lax.rem(out[axis] + step, SIDE)
    return tuple(out)


def remote(src, dst, send_sem, recv_sem, target):
    return pltpu.make_async_remote_copy(src_ref=src, dst_ref=dst, send_sem=send_sem, recv_sem=recv_sem,
                                        device_id=target, device_id_type=MESH)


def greet(targets):
    barrier = pltpu.get_barrier_semaphore()
    for target in targets:
        pl.semaphore_signal(barrier, device_id=target, device_id_type=MESH)
    pl.semaphore_wait(barrier, len(targets))


def group_targets(coords, core):
    return [device(moved(coords, X, step), abs(core - flip)) for step in range(SIDE) for flip in CORES if step or flip]


def near_targets(coords, core):
    return [device(moved(coords, axis, step), core) for axis in AXES for step in WAYS] + [device(coords, 1 - core)]


def lane_slice(k, width):
    return slice(k * width, k * width + width)


def rms_unit(values):
    inv = lax.rsqrt(jnp.mean(values * values, axis=-1, keepdims=True) + NORM_EPS)
    return values * inv, inv


def rms_back(normed, inv_rms, grad_out):
    return inv_rms * (grad_out - normed * jnp.mean(grad_out * normed, axis=-1, keepdims=True))


GELU_C = 0.7978845608028654
GELU_K = 0.044715


def gelu_act(u):
    half = 0.5 * u
    return half + half * jnp.tanh(u * (GELU_C + (GELU_C * GELU_K) * (u * u)))


def gelu_of_half(v):
    return v + v * jnp.tanh(v * (2 * GELU_C + (8 * GELU_C * GELU_K) * (v * v)))


def gelu_slope(u):
    sq = u * u
    t = jnp.tanh(u * (GELU_C + (GELU_C * GELU_K) * sq))
    return 0.5 * (1 + t) + (0.5 * u) * (1 - t * t) * (GELU_C + (3 * GELU_C * GELU_K) * sq)


def dot(a, b):
    return jnp.dot(a, b, preferred_element_type=F32)


def dot_right_t(a, b):
    return lax.dot_general(a, b, (((1,), (1,)), ((), ())), preferred_element_type=F32)


def dot_left_t(a, b):
    return lax.dot_general(a, b, (((0,), (0,)), ((), ())), preferred_element_type=F32)


def student_layers(x_ref, gain_ref, up_ref, down_ref):
    residual = x_ref[...].astype(F32)
    unit, inv = rms_unit(residual)
    saved = []
    for j in range(up_ref.shape[0]):
        normed = (unit * gain_ref[j:j + 1, :]).astype(BF16)
        pre = dot(normed, up_ref[j])
        act = gelu_act(pre).astype(BF16)
        residual = residual + dot(act, down_ref[j])
        unit_next, inv_next = rms_unit(residual)
        saved.append((unit, inv, normed, pre, act, unit_next, inv_next))
        unit, inv = unit_next, inv_next
    return saved, unit.astype(BF16)


def teacher_kernel(feat_at, slots_w,
                   x_hbm, xs_hbm, gs_hbm, ups_hbm, dns_hbm, gain_hbm, wup_hbm, wdn_hbm,
                   feat_hbm, last_hbm, state_hbm, group_hbm,
                   xs_ref, gs_ref, ups_ref, dns_ref, gain_ref, feat_ref, last_ref, state_ref, h, nrm, wu, wd, part, got, r_own,
                   in_sems, out_sems, usem, dsem, xown, xsend, xrecv, ssem, rsem, gsend, grecv):
    me = lax.axis_index('tp')
    coords = chip_coords()
    peer = device(coords, 1 - me)
    n_layers = gain_ref.shape[0]
    rows, seq_half, d_model = x_hbm.shape
    d_ff = wu.shape[-1]

    def up_copy(layer, slot):
        return pltpu.make_async_copy(wup_hbm.at[layer], wu.at[slot], usem.at[slot])

    def down_copy(layer, slot):
        return pltpu.make_async_copy(wdn_hbm.at[layer], wd.at[slot], dsem.at[slot])

    ins = [pltpu.make_async_copy(src, dst, in_sems.at[i]) for i, (src, dst) in enumerate((
        (xs_hbm, xs_ref), (gs_hbm, gs_ref), (ups_hbm, ups_ref), (dns_hbm, dns_ref), (gain_hbm, gain_ref)))]
    mine = pl.ds(pl.multiple_of(me * seq_half, seq_half), seq_half)
    xcopy_own = pltpu.make_async_copy(x_hbm, h.at[:, mine], xown)
    for copy in ins + [xcopy_own]:
        copy.start()
    for i in range(slots_w):
        up_copy(i, i).start()
        down_copy(i, i).start()
    targets = group_targets(coords, me)
    greet(targets)
    xcopy = remote(x_hbm, h.at[:, mine], xsend, xrecv, peer)
    xcopy.start()
    for copy in ins:
        copy.wait()

    _, head_in = student_layers(xs_ref, gs_ref, ups_ref, dns_ref)
    r_own[...] = head_in
    r_copies = [remote(r_own, group_hbm.at[coords[X], me], gsend.at[i], grecv.at[i], target) for i, target in enumerate(targets)]
    for copy in r_copies:
        copy.start()
    r_keep = pltpu.make_async_copy(r_own, group_hbm.at[coords[X], me], out_sems.at[SIDE - 1])
    r_keep.start()
    xcopy.wait()
    xcopy_own.wait()

    def p_copy(ck, slot):
        return remote(part.at[ck, slot], got.at[ck, slot], ssem.at[ck, slot], rsem.at[ck, slot], peer)

    def update(ck, slot):
        p_copy(ck, slot).wait()
        total = part[ck, slot] + got[ck, slot]
        h[ck] = h[ck] + total.astype(BF16)

    def layer_step(layer, _):
        slot = lax.rem(layer, len(PAIR))
        ws = lax.rem(layer, slots_w)
        for ck in range(rows):
            first, last = ck == 0, ck == rows - 1

            @pl.when(layer > 0)
            def _():
                update(ck, 1 - slot)

            @pl.when((layer == feat_at) & (me == ck))
            def _():
                feat_ref[...] = h[ck]

            unit, _ = rms_unit(h[ck].astype(F32))
            nrm[...] = (unit * (0.5 * gain_ref[pl.ds(layer, 1), :])).astype(BF16)
            if first:
                up_copy(layer, ws).wait()
                down_copy(layer, ws).wait()
            halves = []
            for piece in (slice(None, d_ff // 2), slice(d_ff // 2, None)):
                act = gelu_of_half(dot(nrm[...], wu[ws, :, piece])).astype(BF16)
                halves.append(dot(act, wd[ws, piece, :]))
            part[ck, slot] = halves[0] + halves[1]
            p_copy(ck, slot).start()
            if last:
                @pl.when(layer + slots_w < n_layers)
                def _():
                    up_copy(layer + slots_w, ws).start()
                    down_copy(layer + slots_w, ws).start()
        return 0

    lax.fori_loop(0, n_layers, layer_step, 0)
    for ck in range(rows):
        update(ck, (n_layers - 1) % len(PAIR))

        @pl.when(me == ck)
        def _():
            last_ref[...] = h[ck]

        state_ref[ck] = rms_unit(h[ck].astype(F32))[0].astype(BF16)
    outs = [pltpu.make_async_copy(src, dst, out_sems.at[i])
            for i, (src, dst) in enumerate(((feat_ref, feat_hbm), (last_ref, last_hbm), (state_ref, state_hbm)))]
    for copy in outs:
        copy.start()
    for copy in r_copies + outs + [r_keep]:
        copy.wait()


def teacher(x_teach, x_stud, gain_s, w_up_s, w_down_s, gain_t, w_up_t, w_down_t, feat_at, collective_id, slots_w=3):
    n_layers, d_model, d_ff = w_up_t.shape
    rows, seq_half, _ = x_teach.shape
    n_tok = len(PAIR) * seq_half
    n_peers = SIDE * len(PAIR) - 1
    feat = jax.ShapeDtypeStruct((n_tok, d_model), BF16)
    slots = (rows, len(PAIR))
    weights = n_layers * d_model * d_ff
    args = (x_teach, x_stud, gain_s, w_up_s, w_down_s, gain_t, w_up_t, w_down_t)
    return pl.pallas_call(
        functools.partial(teacher_kernel, feat_at, slots_w),
        out_shape=(feat, feat, jax.ShapeDtypeStruct((rows, n_tok, d_model), BF16),
                   jax.ShapeDtypeStruct((SIDE, len(PAIR)) + x_stud.shape, BF16)),
        in_specs=[IN_HBM] * len(args),
        out_specs=(IN_HBM,) * SIDE,
        scratch_shapes=[pltpu.VMEM(a.shape, a.dtype) for a in args[1:-len(PAIR)]] + [
            pltpu.VMEM((n_tok, d_model), BF16), pltpu.VMEM((n_tok, d_model), BF16), pltpu.VMEM((rows, n_tok, d_model), BF16),
            pltpu.VMEM((rows, n_tok, d_model), BF16), pltpu.VMEM((n_tok, d_model), BF16),
            pltpu.VMEM((slots_w, d_model, d_ff), BF16), pltpu.VMEM((slots_w, d_ff, d_model), BF16),
            pltpu.VMEM(slots + (n_tok, d_model), F32), pltpu.VMEM(slots + (n_tok, d_model), F32),
            pltpu.VMEM(x_stud.shape, BF16),
            DMA((len(args),)), DMA((SIDE,)), DMA((slots_w,)), DMA((slots_w,)), DMA, DMA, DMA, DMA(slots), DMA(slots), DMA((n_peers,)), DMA((n_peers,)),
        ],
        compiler_params=pltpu.CompilerParams(collective_id=collective_id, has_side_effects=True, vmem_limit_bytes=63 * MIB),
        cost_estimate=pl.CostEstimate(flops=SIDE * rows * n_tok * weights, bytes_accessed=SIDE * weights, transcendentals=0),
        name='teacher',
    )(*args)


NEG = -1e38
MAX_T, SUM_T, MAX_S, SUM_S = STATS = range(SIDE)
TEACH, STUD = PAIR


def heads_kernel(kl_coef, chunk, strip,
                 t_hbm, r_hbm, ht_hbm, hs_hbm,
                 dw_hbm, dx, kl_ref,
                 r_ref, tg, rt, ht, hs, zt, zs, mx, sm, st_send, st_all, lcol, grad_a, grad_b, dw_out,
                 ht_sem, hs_sem, t_sem, r_sem, ring_send, ring_recv, peer_send, peer_recv, st_send_sem, st_recv_sem, out_sem):
    coords = chip_coords()
    x = coords[X]
    core = lax.axis_index('tp')
    peer = device(coords, 1 - core)
    rows, n_tok, d_model = t_hbm.shape
    d_stud, cols = hs.shape
    n_tiles = cols // LANES
    blk = rows * n_tok
    n_all = SIDE * blk
    half_tile = LANES // 2
    last_x = SIDE - 1

    first_tile = n_tiles * x + core * (n_tiles * SIDE - 1)
    hs_copy = pltpu.make_async_copy(hs_hbm.at[:, pl.ds(pl.multiple_of(first_tile * LANES, LANES), cols)], hs, hs_sem)
    hs_copy.start()
    r_copy = pltpu.make_async_copy(r_hbm, r_ref, r_sem)
    r_copy.start()
    t_copy = pltpu.make_async_copy(t_hbm, tg.at[x], t_sem)
    t_copy.start()
    cut_low = (core == 1) & (x == 0)
    cut_high = (core == 0) & (x == last_x)

    def ht_copy(src, dst, n):
        return pltpu.make_async_copy(ht_hbm.at[pl.ds(src, n)], ht.at[pl.ds(dst, n)], ht_sem)

    def each_ht(act):
        @pl.when(jnp.logical_not(cut_low | cut_high))
        def _():
            act(ht_copy(pl.multiple_of(cols * x - half_tile * core, half_tile), 0, cols))

        @pl.when(cut_low)
        def _():
            act(ht_copy(0, half_tile, cols - half_tile))

        @pl.when(cut_high)
        def _():
            act(ht_copy(last_x * cols, 0, cols - half_tile))

    each_ht(lambda copy: copy.start())
    targets = group_targets(coords, core)
    greet(targets)

    far_rows = n_tok // 2

    def at(step):
        return lax.rem(x + step, SIDE)

    def ring(k, src, dst, step):
        return remote(src, dst, ring_send.at[k], ring_recv.at[k], device(moved(coords, X, step), core))

    def onward(k, step, way):
        piece = tg.at[at(step), core, pl.ds(k * far_rows, far_rows)]
        return ring(k + len(PAIR), piece, piece, way)

    def first(k, step, way):
        return ring(k, t_hbm.at[core], tg.at[at(step), core], way)

    def across(step, side):
        piece = tg.at[at(step), side]
        return remote(piece, piece, peer_send.at[step - 1], peer_recv.at[step - 1], peer)

    opposite = (LEFT, RIGHT)
    for k, way in enumerate(WAYS):
        first(k, HERE, way).start()
    r_copy.wait()
    rt[...] = r_ref[...].T
    lane = lax.broadcasted_iota(jnp.int32, (blk, LANES), 1)
    low = jnp.where(cut_low, half_tile, 0)
    high = jnp.where(cut_high, half_tile, LANES)

    def logits(kind, b, ref, product):
        peak = total = None
        for c in range(cols // chunk):
            lanes = lane_slice(c, chunk)
            z = product(lanes)
            tiles = [z[:, lane_slice(k, LANES)] for k in range(chunk // LANES)]
            if c == 0:
                tiles[0] = jnp.where(lane >= low, tiles[0], NEG)
            if lanes.stop == cols:
                tiles[-1] = jnp.where(lane < high, tiles[-1], NEG)
            for k, tile in enumerate(tiles):
                ref[b, :, lane_slice(c * len(tiles) + k, LANES)] = tile
            top = functools.reduce(jnp.maximum, tiles if peak is None else [peak] + tiles)
            sums = [jnp.exp(tile - top) for tile in tiles]
            total = functools.reduce(jnp.add, sums if peak is None else [total * jnp.exp(peak - top)] + sums)
            peak = top
        mx[kind, b] = peak
        sm[kind, b] = total

    def tokens(b):
        return pl.ds(pl.multiple_of(b * blk, blk), blk)

    def student_logits(b, _):
        states = r_ref[tokens(b), :]
        logits(STUD, b, zs, lambda lanes: dot(states, hs[:, lanes]))
        return 0

    hs_copy.wait()
    lax.fori_loop(0, FAR, student_logits, 0)
    for k, way in enumerate(WAYS):
        first(k, opposite[k], way).wait_recv()
        onward(k, opposite[k], way).start()
        across(opposite[k], core).start()
    lax.fori_loop(FAR, SIDE, student_logits, 0)
    each_ht(lambda copy: copy.wait())
    t_copy.wait()

    def teacher_logits(i, _):
        for step, turn in ((RIGHT, 1), (LEFT, 2), (FAR, 3)):
            @pl.when(i == turn)
            def _():
                if step == LEFT:
                    for k, way in enumerate(WAYS):
                        onward(k, FAR, way).wait_recv()
                    across(FAR, core).start()
                across(step, 1 - core).wait_recv()

        b = at(jnp.where(i < FAR, i, SIDE + 1 - i))
        states = tg[b].reshape(blk, d_model)
        logits(TEACH, b, zt, lambda lanes: dot_right_t(states, ht[lanes, :]))
        return 0

    lax.fori_loop(0, SIDE, teacher_logits, 0)

    def merge(b, _):
        out = jnp.zeros((blk, LANES), F32)
        for kind in PAIR:
            peak = jnp.max(mx[kind, b], axis=-1, keepdims=True)
            total = jnp.sum(sm[kind, b] * jnp.exp(mx[kind, b] - peak), axis=-1, keepdims=True)
            out = jnp.where(lane == 2 * kind, peak, jnp.where(lane == 2 * kind + 1, total, out))
        st_send[:, tokens(b)] = out.T[:SUBS, :]
        return 0

    lax.fori_loop(0, SIDE, merge, 0)
    n_peers = len(targets)
    stats = [remote(st_send, st_all.at[i], st_send_sem.at[i], st_recv_sem.at[i], target) for i, target in enumerate(targets)]
    for copy in stats:
        copy.start()
    st_all[n_peers] = st_send[...]
    for copy in stats:
        copy.wait()
    sub = lax.broadcasted_iota(jnp.int32, (LANES, n_all), 0)
    both = jnp.zeros((LANES, n_all), F32)
    for kind in PAIR:
        peaks, totals = st_all[:, 2 * kind, :], st_all[:, 2 * kind + 1, :]
        peak = jnp.max(peaks, axis=0, keepdims=True)
        norm = peak + jnp.log(jnp.sum(totals * jnp.exp(peaks - peak), axis=0, keepdims=True))
        both = jnp.where(sub == kind, norm, both)
    lcol[...] = both.T
    kl_ref[...] = jnp.zeros_like(kl_ref)
    dx[...] = jnp.zeros_like(dx)

    n_steps = cols // chunk

    def lanes_of(j):
        return pl.ds(pl.multiple_of(j * chunk, LANES), chunk)

    def logit_grads(j, dst):
        lanes = lanes_of(j)
        total = kl_ref[...]
        for i in range(n_all // strip):
            b, k = divmod(i, blk // strip)
            tok, row = lane_slice(i, strip), lane_slice(k, strip)
            log_pt = zt[b, row, lanes] - lcol[tok, TEACH:TEACH + 1]
            log_ps = zs[b, row, lanes] - lcol[tok, STUD:STUD + 1]
            pt = jnp.exp(log_pt)
            dst[tok, :] = (kl_coef * (jnp.exp(log_ps) - pt)).astype(BF16)
            kl = pt * (log_pt - log_ps)
            kl = functools.reduce(jnp.add, [kl[:, lane_slice(k, LANES)] for k in range(chunk // LANES)])
            total = total + functools.reduce(jnp.add, [kl[lane_slice(k, SUBS)] for k in range(strip // SUBS)])
        kl_ref[...] = total

    def out_copy(j):
        return pltpu.make_async_copy(dw_out, dw_hbm.at[:, lanes_of(j)], out_sem)

    def products(j, src):
        dw_out[...] = dot(rt[...], src[...])
        out_copy(j).start()
        dx[...] += dot_right_t(src[...], hs[:, lanes_of(j)])

    def two_steps(i, _):
        j = 2 * i

        @pl.when(i > 0)
        def _():
            out_copy(j - 1).wait()

        logit_grads(j + 1, grad_b)
        products(j, grad_a)
        out_copy(j).wait()
        logit_grads(j + 2, grad_a)
        products(j + 1, grad_b)
        return 0

    logit_grads(0, grad_a)
    lax.fori_loop(0, n_steps // 2, two_steps, 0)
    out_copy(n_steps - 2).wait()
    products(n_steps - 1, grad_a)
    for k, way in enumerate(WAYS):
        first(k, HERE, way).wait_send()
        onward(k, opposite[k], way).wait_send()
    for step in (RIGHT, FAR, LEFT):
        across(step, core).wait_send()
    out_copy(n_steps - 1).wait()


def heads(states, stud_all, head_t, head_s, kl_coef, collective_id, chunk=768, strip=16):
    rows, n_tok, d_model = states.shape
    n_all, d_stud = stud_all.shape
    cols = -(-head_t.shape[1] // (LANES * SIDE)) * LANES
    blk = rows * n_tok
    n_peers = SIDE * len(PAIR) - 1
    v = pltpu.VMEM
    hops = (SIDE - 1,)
    return pl.pallas_call(
        functools.partial(heads_kernel, kl_coef, chunk, strip),
        out_shape=(jax.ShapeDtypeStruct((d_stud, cols), F32), jax.ShapeDtypeStruct((n_all, d_stud), F32),
                   jax.ShapeDtypeStruct((SUBS, LANES), F32)),
        in_specs=[IN_HBM] * SIDE,
        out_specs=(IN_HBM, IN_VMEM, IN_VMEM),
        scratch_shapes=[
            v((n_all, d_stud), BF16), v((SIDE, rows, n_tok, d_model), BF16), v((d_stud, n_all), BF16), v((cols, d_model), BF16), v((d_stud, cols), BF16),
            v((SIDE, blk, cols), F32), v((SIDE, blk, cols), F32),
            v((len(PAIR), SIDE, blk, LANES), F32), v((len(PAIR), SIDE, blk, LANES), F32),
            v((SUBS, n_all), F32), v((n_peers + 1, SUBS, n_all), F32), v((n_all, LANES), F32),
            v((n_all, chunk), BF16), v((n_all, chunk), BF16), v((d_stud, chunk), F32),
            DMA, DMA, DMA, DMA, DMA((SIDE,)), DMA((SIDE,)), DMA(hops), DMA(hops), DMA((n_peers,)), DMA((n_peers,)), DMA,
        ],
        compiler_params=pltpu.CompilerParams(collective_id=collective_id, has_side_effects=True, vmem_limit_bytes=63 * MIB),
        cost_estimate=pl.CostEstimate(flops=d_model * n_all * cols, bytes_accessed=d_model * cols, transcendentals=0),
        name='heads',
    )(states, stud_all, head_t.T, head_s)


class RingSum:
    def __init__(self, coords, core, src, dims, order, lanes, bufs, loads=None):
        self.coords, self.core, self.order, self.lanes = coords, core, order, lanes
        self.loads = src if loads is None else loads
        self.phases = []
        for axis, (half, full, mid, send, recv) in zip(order, bufs):
            self.phases.append((src, dims, axis, half, full, mid, send, recv))
            src, dims = mid, tuple(d for d in dims if d != axis)

    @staticmethod
    def shapes(dims, order, rows, width):
        out = []
        for _ in order:
            dims = dims[1:]
            lead = (SIDE,) * len(dims)
            part = (SIDE // 2,) + lead[1:] + (rows, width) if lead else (rows, -(-width // (2 * LANES)) * LANES)
            out += [pltpu.VMEM(PAIR_DIM + part, F32), pltpu.VMEM(PAIR_DIM + lead + (rows, width), F32),
                    pltpu.VMEM(lead + (rows, width), F32), DMA((3 * len(PAIR),)), DMA((3 * len(PAIR),))]
        return out

    def place(self, axis, step):
        return lax.rem(self.coords[axis] + step, SIDE)

    def split(self, k, side):
        _, dims, _, half, full, _, _, _ = self.phases[k]
        width, cut = full.shape[-1], half.shape[-1]
        if len(dims) > 1:
            return (pl.ds(side * (SIDE // 2), SIDE // 2),) + (slice(None),) * (len(dims) - 2), (0, width)
        return (), ((cut, width - cut) if side else (0, cut))

    def pick(self, k, at, side):
        src, dims, axis = self.phases[k][:3]
        lead, (lo, n) = ((slice(None),) * (len(dims) - 1), (0, self.phases[k][4].shape[-1])) if side is None else self.split(k, side)
        lead = list(lead)
        lead.insert(dims.index(axis), at)
        base = self.lanes if k == 0 else 0
        return src, tuple(lead) + (slice(None), pl.ds(base + lo, n))

    def held(self, k, at, side):
        src, idx = self.pick(k, at, side)
        return (src if k else self.loads), idx

    def copy(self, k, turn, d):
        _, _, axis, half, full, _, send, recv = self.phases[k]
        way = WAYS[d]
        i = turn * len(PAIR) + d
        side = d if turn != 1 else 1 - d
        lead, (lo, n) = self.split(k, side)
        window = (slice(None), pl.ds(lo, n))
        if turn == 0:
            ref, idx = self.pick(k, self.place(axis, FAR), side)
            src, dst = ref.at[idx], half.at[d, ..., pl.ds(0, n)]
        elif turn == 1:
            ref, idx = self.pick(k, self.place(axis, way), side)
            src, dst = ref.at[idx], full.at[(d,) + lead + window]
        else:
            src, dst = half.at[d, ..., pl.ds(0, n)], full.at[(d,) + lead + window]
        return remote(src, dst, send.at[i], recv.at[i], device(moved(self.coords, axis, way), self.core))

    def start(self, k, turns=PAIR):
        for turn in turns:
            for d in PAIR:
                self.copy(k, turn, d).start()

    def middle(self, k):
        _, _, axis, half, _, _, _, _ = self.phases[k]
        for d in PAIR:
            self.copy(k, 0, d).wait_recv()
            ref, idx = self.held(k, self.place(axis, WAYS[d]), d)
            n = self.split(k, d)[1][1]
            half[d, ..., :n] = half[d, ..., :n] + ref[idx]
            self.copy(k, len(PAIR), d).start()

    def finish(self, k):
        _, _, axis, _, full, mid, _, _ = self.phases[k]
        for d in PAIR:
            for turn in (1, len(PAIR)):
                self.copy(k, turn, d).wait_recv()
        ref, idx = self.held(k, self.coords[axis], None)
        mid[...] = ref[idx] + full[0] + full[1]

    def drain(self):
        for k in range(len(self.order)):
            for turn in range(3):
                for d in PAIR:
                    self.copy(k, turn, d).wait_send()


PAIR_DIM = (len(PAIR),)


def small_places(n_feat, d_in, d_mid, d_teach):
    groups_up = d_in // SUBS
    yz = SIDE * SIDE
    per_up = n_feat * groups_up // yz
    lanes_u, lanes_p = d_mid // SIDE, d_teach // SIDE
    per_p = groups_up // yz
    span = per_up // per_p * lanes_u + lanes_p
    return groups_up, yz, per_up, lanes_u, lanes_p, per_p, span


def reduce_kernel(feat_coef, kl_coef, small_parts,
                  dw_hbm, feat_a_hbm, feat_b_hbm, xs_hbm, gs_hbm, ups_hbm, dns_hbm, proj_hbm, dx_ref, kl_ref,
                  own, dw, feat_a, feat_b, xs_ref, gs_ref, ups_ref, dns_ref, proj_ref, in_sems, small, got, part_in, swap_send, swap_recv, in_send, in_recv, *bufs):
    coords = chip_coords()
    core = lax.axis_index('tp')
    peer = device(coords, 1 - core)
    loads = [pltpu.make_async_copy(src, dst, in_sems.at[i]) for i, (src, dst) in enumerate((
        (dw_hbm, dw), (feat_a_hbm, feat_a), (feat_b_hbm, feat_b), (xs_hbm, xs_ref), (gs_hbm, gs_ref), (ups_hbm, ups_ref),
        (dns_hbm, dns_ref), (proj_hbm, proj_ref)))]
    dw_load = loads.pop(0)
    for copy in loads + [dw_load]:
        copy.start()
    greet(near_targets(coords, core))
    cols = dw.shape[-1]
    bufs = list(bufs)

    def take(n):
        out = [tuple(bufs[5 * i:5 * i + 5]) for i in range(n)]
        del bufs[:5 * n]
        return out

    head_jobs = [RingSum(coords, core, dw_hbm, (Y, Z), order, k * (cols // 2), take(2), dw) for k, order in enumerate(((Y, Z), (Z, Y)))]
    in_job = RingSum(coords, core, part_in, (X,), (X,), 0, take(1))
    for job in head_jobs:
        job.start(0)
    in_swap = remote(dx_ref.at[:, 1 - core], part_in, in_send, in_recv, peer)
    in_swap.start()

    for copy in loads:
        copy.wait()
    saved, _ = student_layers(xs_ref, gs_ref, ups_ref, dns_ref)
    in_swap.wait()
    part_in[...] = part_in[...] + dx_ref[:, core]
    in_job.start(0)
    feats = (feat_a, feat_b)
    n_feat, d_in, d_mid = ups_ref.shape
    groups, yz, per_up, lanes_u, lanes_p, per_p, span = small_places(n_feat, d_in, d_mid, proj_ref.shape[-1])
    two = per_up // per_p
    err_rows = jnp.zeros((SUBS, LANES), F32)
    out_grads, gain_rows = [], []

    def put(keep, chip_x, group, per, base, lanes, value):
        block, g = divmod(group, per)
        y, z = divmod(block, SIDE)
        part, q = divmod(g, per // per_p)
        small[keep, chip_x, y, z, :, part * span + base + q * lanes:part * span + base + q * lanes + lanes] = value

    half_side = SIDE // n_feat
    swaps = []

    def swap(k, rows_y, base, lanes):
        for p in PARTS:
            window = (slice(None), rows_y, slice(None), slice(None), pl.ds(p * span + base, lanes))
            copy = remote(small.at[(1 - core,) + window], got.at[window], swap_send.at[k, p], swap_recv.at[k, p], peer)
            copy.start()
            swaps.append((copy, window))

    for j in range(n_feat):
        proj_in = saved[j][5].astype(BF16)
        err = dot(proj_in, proj_ref[j]) - feats[j][...].astype(F32)
        sq = err * err
        sq = functools.reduce(jnp.add, [sq[:, lane_slice(k, LANES)] for k in range(sq.shape[1] // LANES)])
        err_rows = err_rows + functools.reduce(jnp.add, [sq[lane_slice(k, SUBS)] for k in range(sq.shape[0] // SUBS)])
        err_grad = ((2 * feat_coef) * err).astype(BF16)
        g_proj = dot_left_t(proj_in, err_grad)
        for i in range(groups):
            for cx in range(SIDE):
                put(j, cx, i, per_p, two * lanes_u, lanes_p, g_proj[lane_slice(i, SUBS), lane_slice(cx, lanes_p)])
        out_grads.append(dot_right_t(err_grad, proj_ref[j]))
    swap(n_feat, slice(None), two * lanes_u, lanes_p)
    in_job.middle(0)
    dw_load.wait()
    for job in head_jobs:
        job.middle(0)
    in_job.finish(0)
    out_grads[-1] = out_grads[-1] + in_job.phases[-1][5][...]
    resid_grad = None
    for j in reversed(range(n_feat)):
        unit, inv, normed, pre, act, unit_next, inv_next = saved[j]
        step_grad = rms_back(unit_next, inv_next, out_grads[j])
        resid_grad = step_grad if resid_grad is None else resid_grad + step_grad
        resid_bf = resid_grad.astype(BF16)
        g_down = dot_left_t(act, resid_bf)
        n_down = d_mid // SUBS
        for i in range(n_down):
            cx, rest = divmod(i, groups)
            put(1, cx, j * groups + rest, per_up, 0, lanes_u, g_down[lane_slice(i, SUBS), :])
        pre_grad = (gelu_slope(pre) * dot_right_t(resid_bf, dns_ref[j])).astype(BF16)
        g_up = dot_left_t(normed, pre_grad)
        for i in range(groups):
            for cx in range(SIDE):
                put(0, cx, j * groups + i, per_up, 0, lanes_u, g_up[lane_slice(i, SUBS), lane_slice(cx, lanes_u)])
        swap(j, pl.ds(half_side * j, half_side), 0, two * lanes_u)
        norm_grad = dot_right_t(pre_grad, ups_ref[j])
        g_gain = jnp.sum(norm_grad * unit, axis=0, keepdims=True)
        gain_rows = [g_gain[:, lane_slice(k, LANES)] for k in range(d_in // LANES)] + gain_rows
        if j > 0:
            resid_grad = resid_grad + rms_back(unit, inv, norm_grad * gs_ref[j:j + 1, :])

    lo = 0
    small_jobs = []
    for order, width in zip(ORDERS, small_parts):
        small_jobs.append(RingSum(coords, core, got, AXES, order, lo, take(3)))
        lo += width
    for copy, window in swaps:
        copy.wait()
        got[window] = got[window] + small[(core,) + window]
    for turn in PAIR:
        for job in small_jobs:
            job.start(0, (turn,))
    for job in head_jobs:
        job.finish(0)
        job.start(1)
    for job in head_jobs:
        job.middle(1)
    for job in small_jobs:
        job.middle(0)
    for job in head_jobs:
        job.finish(1)
    for job in small_jobs:
        job.finish(0)
        job.start(1)
    for k in (1, 2):
        for job in small_jobs:
            job.middle(k)
        for job in small_jobs:
            job.finish(k)
            if k < 2:
                job.start(k + 1)
    for p in PARTS:
        for k, job in enumerate(head_jobs):
            own[p, :, lane_slice(k, cols // 2)] = job.phases[-1][5][lane_slice(p, SUBS), :]
    pieces = [(order_i, t) for order_i, width in enumerate(small_parts) for t in range(width // LANES)]
    for n, (which, t) in enumerate(pieces):
        p, at = divmod(n * LANES, span)
        own[p, :, cols + at:cols + at + LANES] = small_jobs[which].phases[-1][5][:, lane_slice(t, LANES)]
    loss_row = jnp.sum(feat_coef * err_rows + kl_coef * kl_ref[...], axis=0, keepdims=True)
    for p in PARTS:
        own[p, :, cols + span:] = jnp.zeros((SUBS, LANES), F32)
    for i, row in enumerate(gain_rows + [loss_row]):
        own[0, i:i + 1, cols + span:] = row
    for job in head_jobs + small_jobs + [in_job]:
        job.drain()


def reduce_grads(dw, dx, feats, x_stud, gain_s, w_up_s, w_down_s, proj_s, kl_tiles, feat_coef, kl_coef, collective_id,
                 small_parts=(1280, 896, 896)):
    rows, cols = dw.shape[2:]
    span = sum(small_parts) // len(PARTS)
    width = cols // 2
    xs_shape = x_stud.shape
    args = (dw, *feats, x_stud, gain_s, w_up_s, w_down_s, proj_s)
    scratch = [pltpu.VMEM(a.shape, a.dtype) for a in args]
    scratch += [DMA((len(args),)), pltpu.VMEM((len(PAIR), SIDE, SIDE, SIDE, SUBS, sum(small_parts)), F32),
               pltpu.VMEM((SIDE, SIDE, SIDE, SUBS, sum(small_parts)), F32), pltpu.VMEM((SIDE,) + xs_shape, F32),
               DMA((SIDE, SIDE)), DMA((SIDE, SIDE)), DMA, DMA]
    for _ in PAIR:
        scratch += RingSum.shapes((Y, Z), (Y, Z), rows, width)
    scratch += RingSum.shapes((X,), (X,), *xs_shape)
    for part in small_parts:
        scratch += RingSum.shapes(AXES, AXES, SUBS, part)
    return pl.pallas_call(
        functools.partial(reduce_kernel, feat_coef, kl_coef, small_parts),
        out_shape=jax.ShapeDtypeStruct((len(PARTS), SUBS, cols + span + LANES), F32),
        in_specs=[IN_HBM] * len(args) + [IN_VMEM] * len(PAIR),
        out_specs=IN_VMEM,
        scratch_shapes=scratch,
        compiler_params=pltpu.CompilerParams(collective_id=collective_id, has_side_effects=True, vmem_limit_bytes=63 * MIB),
        cost_estimate=pl.CostEstimate(flops=MIB * MIB, bytes_accessed=dw.size, transcendentals=0),
        name='reduce',
    )(*args, dx, kl_tiles)


ALL = pl.ds(0, SIDE)
WHOLE, LOW, HIGH = range(SIDE - 1)
SOURCE = (LEFT, RIGHT)
ARRIVAL = (HERE, LEFT, RIGHT, FAR)


def gather_kernel(cut, own_ref, full, own_sem, send_sem, recv_sem, peer_send, peer_recv):
    coords = chip_coords()
    core = lax.axis_index('tp')
    peer = device(coords, 1 - core)
    width = own_ref.shape[-1]
    widths = (width, width - LANES, width - LANES)
    here = [pltpu.make_async_copy(own_ref.at[p], full.at[(core,) + coords + (p,)], own_sem.at[p]) for p in PARTS]
    for copy in here:
        copy.start()
    greet(near_targets(coords, core))

    def lanes(part, span):
        return pl.ds(cut if span == HIGH else 0, (widths[part], cut, widths[part] - cut)[span])

    def block(part, steps, span=WHOLE):
        idx = list(coords)
        for axis, step in zip(ORDERS[part], steps):
            idx[axis] = ALL if step is ALL else lax.rem(coords[axis] + step, SIDE)
        return full.at[(core,) + tuple(idx) + (part, slice(None), lanes(part, span))]

    def steps_of(phase, sub, step):
        return ((step,), (sub, step), (ALL, sub, step))[phase]

    def ring(part, phase, sub, slot, step, span):
        dst = block(part, steps_of(phase, sub, step), span)
        mine = step == HERE and (phase == 0 or (phase == 1 and sub == HERE))
        src = own_ref.at[part, :, lanes(part, span)] if mine else dst
        at = (part, phase, sub, slot)
        return remote(src, dst, send_sem.at[at], recv_sem.at[at], device(moved(coords, ORDERS[part][phase], WAYS[slot % 2]), core))

    def first(part, phase, sub, d, step):
        return ring(part, phase, sub, d, step, WHOLE)

    def onward(part, phase, sub, d, step):
        return ring(part, phase, sub, d + 2, step, (LOW, HIGH)[d])

    def send(part, phase, sub):
        for d in PAIR:
            first(part, phase, sub, d, HERE).start()

    def relay(part, phase, sub, d):
        first(part, phase, sub, d, SOURCE[d]).wait_recv()
        onward(part, phase, sub, d, SOURCE[d]).start()

    def far_in(part, phase, sub):
        for d in PAIR:
            onward(part, phase, sub, d, FAR).wait_recv()

    def across(part, phase, sub, step):
        dst = block(part, ((step,), (ALL, step), (ALL, sub, step))[phase])
        src = own_ref.at[part, :, lanes(part, WHOLE)] if phase == 0 and step == HERE else dst
        at = (part, phase, sub, step)
        return remote(src, dst, peer_send.at[at], peer_recv.at[at], peer)

    for part in PARTS:
        send(part, 0, HERE)
    for part in PARTS:
        send(part, 1, HERE)
        across(part, 0, HERE, HERE).start()
    for part in PARTS:
        for d in PAIR:
            relay(part, 0, HERE, d)
            send(part, 1, SOURCE[d])
            across(part, 0, HERE, SOURCE[d]).start()
    for part in PARTS:
        far_in(part, 0, HERE)
        send(part, 1, FAR)
        across(part, 0, HERE, FAR).start()
        here[part].wait()
        send(part, 2, HERE)
    for sub in ARRIVAL:
        for part in PARTS:
            for d in PAIR:
                relay(part, 1, sub, d)
                if sub == FAR:
                    send(part, 2, SOURCE[d])
                    across(part, 1, HERE, SOURCE[d]).start()
    for part in PARTS:
        for sub in ARRIVAL:
            far_in(part, 1, sub)
        send(part, 2, FAR)
        across(part, 1, HERE, FAR).start()
    for sub in ARRIVAL:
        for part in PARTS:
            for d in PAIR:
                relay(part, 2, sub, d)
                across(part, 2, sub, SOURCE[d]).start()
    for sub in ARRIVAL:
        for part in PARTS:
            far_in(part, 2, sub)
            across(part, 2, sub, FAR).start()
    for part in PARTS:
        for phase in AXES:
            for sub in ARRIVAL if phase else (HERE,):
                for d in PAIR:
                    first(part, phase, sub, d, HERE).wait_send()
                    onward(part, phase, sub, d, SOURCE[d]).wait_send()
                for step in ARRIVAL if phase == 0 else (LEFT, RIGHT, FAR):
                    if phase != 1 or sub == HERE:
                        across(part, phase, sub, step).wait()


def gather_blocks(own, cut, collective_id):
    sems = DMA((len(PARTS), len(AXES), SIDE, SIDE))
    return pl.pallas_call(
        functools.partial(gather_kernel, cut),
        out_shape=pltpu.VMEM((len(PAIR), SIDE, SIDE, SIDE) + own.shape, F32),
        in_specs=[IN_VMEM],
        out_specs=IN_HBM,
        scratch_shapes=[DMA((len(PARTS),)), sems, sems, sems, sems],
        compiler_params=pltpu.CompilerParams(collective_id=collective_id, has_side_effects=True, vmem_limit_bytes=MIB),
        cost_estimate=pl.CostEstimate(flops=MIB * MIB, bytes_accessed=SIDE * LANES * own.size, transcendentals=0),
        name='gather',
    )(own)


def place_kernel(n_head, lanes_u, lanes_p,
                 full, head, up, down, proj, gain, loss,
                 total, edge, head_sem, edge_sem, up_sem, down_sem, narrow_sem):
    last_x = SIDE - 1
    per = up.shape[3]
    n_feat, _, half_side = down.shape[:3]
    copy = pltpu.make_async_copy
    narrow_at = n_head + per * lanes_u
    copies = []
    for c in CORES:
        for x in range(SIDE):
            src = full.at[c, x]
            lo = LANES if (c, x) == PAIR[::-1] else 0
            hi = n_head - LANES if (c, x) == (0, last_x) else n_head
            at = (c * SIDE + x) * n_head - c * LANES
            copies.append(copy(src.at[:, :, :, :, pl.ds(lo, hi - lo)], head.at[:, :, :, :, pl.ds(at + lo, hi - lo)], head_sem.at[c, x]))
            for q in range(per):
                lanes = pl.ds(n_head + q * lanes_u, lanes_u)
                if c:
                    for j in range(n_feat):
                        copies.append(copy(src.at[pl.ds(j * half_side, half_side), :, :, :, lanes], down.at[j, x, :, :, :, q],
                                           down_sem.at[x, q, j]))
                else:
                    copies.append(copy(src.at[:, :, :, :, lanes], up.at[:, :, :, q, :, pl.ds(x * lanes_u, lanes_u)], up_sem.at[x, q]))
            copies.append(copy(src.at[:, :, :, :, pl.ds(narrow_at, lanes_p)], proj.at[c, :, :, :, :, pl.ds(x * lanes_p, lanes_p)],
                               narrow_sem.at[c, x]))
    for one in copies:
        one.start()
    edge[...] = full[0, last_x, :, :, :, :, n_head - LANES:n_head] + full[1, 0, :, :, :, :, :LANES]
    edge_copy = copy(edge, head.at[:, :, :, :, pl.ds(SIDE * n_head - LANES, LANES)], edge_sem)
    edge_copy.start()
    tiles = full[:, :, :, :, 0, :, narrow_at + lanes_p:narrow_at + lanes_p + LANES]
    total[...] = jnp.sum(tiles.reshape(-1, SUBS, LANES), axis=0)
    rows = gain.shape[1] // LANES
    for j in range(n_feat):
        for k in range(rows):
            gain[j:j + 1, lane_slice(k, LANES)] = total[j * rows + k:j * rows + k + 1, :]
    loss[...] = jnp.sum(total[n_feat * rows:n_feat * rows + 1, :], axis=-1, keepdims=True)
    edge_copy.wait()
    for one in copies:
        one.wait()


def place_blocks(full, n_head, lanes_u, lanes_p, vocab, gain_shape):
    n_part, subs, _ = full.shape[4:]
    per = len(PAIR)
    n_feat = gain_shape[0]
    pair = (len(PAIR),)
    owners = pair + (SIDE,)
    yz = (SIDE, SIDE)
    shapes = (yz + (n_part, subs, vocab), yz + (n_part, per, subs, SIDE * lanes_u), (n_feat, SIDE, SIDE // n_feat, SIDE, n_part, per, subs, lanes_u),
              pair + yz + (n_part, subs, SIDE * lanes_p), gain_shape, (1, 1))
    return pl.pallas_call(
        functools.partial(place_kernel, n_head, lanes_u, lanes_p),
        out_shape=tuple(jax.ShapeDtypeStruct(s, F32) for s in shapes),
        in_specs=[IN_VMEM],
        out_specs=(IN_HBM,) * SIDE + (IN_VMEM, IN_VMEM),
        scratch_shapes=[pltpu.VMEM((subs, LANES), F32), pltpu.VMEM(yz + (n_part, subs, LANES), F32), DMA(owners), DMA,
                        DMA((SIDE, per)), DMA((SIDE, per, n_feat)), DMA(owners)],
        compiler_params=pltpu.CompilerParams(has_side_effects=True, vmem_limit_bytes=MIB),
        name='place',
    )(pltpu.with_memory_space_constraint(full, pltpu.VMEM))


def solution(mesh):
    n_dev = mesh.shape['dp'] * mesh.shape['tp']

    def local_step(x_teach, x_stud, w_up_t, w_down_t, gain_t, head_t, w_up_s, w_down_s, gain_s, proj_s, head_s):
        n_feat, d_in, d_mid = w_up_s.shape
        d_teach = proj_s.shape[-1]
        n_tokens = x_stud.shape[0] * x_stud.shape[1] * n_dev
        feat_coef = 1.0 / (n_feat * n_tokens * d_teach)
        kl_coef = 1.0 / n_tokens
        xs = x_stud[0]
        feat_one, feat_two, states, stud_all = teacher(x_teach, xs, gain_s, w_up_s, w_down_s, gain_t, w_up_t, w_down_t,
                                                       w_up_t.shape[0] // n_feat, 0)
        head_part, in_part, kl_tiles = heads(states, stud_all.reshape(-1, d_in), head_t, head_s, kl_coef, 1)
        cols = head_part.shape[1]
        own = reduce_grads(head_part.reshape(SIDE, SIDE, -1, cols), in_part.reshape((SIDE, -1) + xs.shape), (feat_one, feat_two), xs, gain_s, w_up_s, w_down_s,
                           proj_s, kl_tiles, feat_coef, kl_coef, 2)
        blocks = gather_blocks(own, 20 * LANES, 3)
        head_grad, up, down, proj, gain, loss = place_blocks(blocks, cols, d_mid // SIDE, d_teach // SIDE, head_s.shape[1], gain_s.shape)
        return (loss.reshape(()), up.reshape(w_up_s.shape), down.reshape(w_down_s.shape), gain,
                proj.reshape(proj_s.shape), head_grad.reshape(head_s.shape))

    in_specs = (P('dp', 'tp', None), P(('dp', 'tp'), None, None), P(None, None, 'tp'), P(None, 'tp', None),
                P(), P(None, 'tp'), P(), P(), P(), P(), P())
    out_specs = (P(), P(), P(), P(), P(), P())
    return jax.shard_map(local_step, mesh=mesh, in_specs=in_specs, out_specs=out_specs, check_vma=False)
```

```python
import functools

import jax
import jax.numpy as jnp
from jax import lax
from jax.experimental import pallas as pl
from jax.experimental.pallas import tpu as pltpu
from jax.sharding import PartitionSpec as P

NORM_EPS = 1e-6
MESH = pl.DeviceIdType.MESH
F32, BF16 = jnp.float32, jnp.bfloat16
DMA = pltpu.SemaphoreType.DMA
IN_VMEM = pl.BlockSpec(memory_space=pltpu.VMEM)
IN_HBM = pl.BlockSpec(memory_space=pl.ANY)
LANES = 128
SUBS = 8
SIDE = 4
MIB = 1 << 20
HERE, RIGHT, FAR, LEFT = range(SIDE)
X, Y, Z = AXES = tuple(range(SIDE - RIGHT))
PARTS = AXES
ORDERS = ((X, Y, Z), (Y, Z, X), (Z, X, Y))
CORES = PAIR = (0, 1)
WAYS = (RIGHT, LEFT)


def chip_coords():
    chip = lax.axis_index('dp')
    return lax.rem(chip, SIDE), lax.rem(chip // SIDE, SIDE), chip // (SIDE * SIDE)


def device(coords, core):
    x, y, z = coords
    return {'dp': (z * SIDE + y) * SIDE + x, 'tp': core}


def moved(coords, axis, step):
    out = list(coords)
    out[axis] = lax.rem(out[axis] + step, SIDE)
    return tuple(out)


def remote(src, dst, send_sem, recv_sem, target):
    return pltpu.make_async_remote_copy(src_ref=src, dst_ref=dst, send_sem=send_sem, recv_sem=recv_sem,
                                        device_id=target, device_id_type=MESH)


def greet(targets):
    barrier = pltpu.get_barrier_semaphore()
    for target in targets:
        pl.semaphore_signal(barrier, device_id=target, device_id_type=MESH)
    pl.semaphore_wait(barrier, len(targets))


def group_targets(coords, core):
    return [device(moved(coords, X, step), abs(core - flip)) for step in range(SIDE) for flip in CORES if step or flip]


def near_targets(coords, core):
    return [device(moved(coords, axis, step), core) for axis in AXES for step in WAYS] + [device(coords, 1 - core)]


def lane_slice(k, width):
    return slice(k * width, k * width + width)


def rms_unit(values):
    inv = lax.rsqrt(jnp.mean(values * values, axis=-1, keepdims=True) + NORM_EPS)
    return values * inv, inv


def rms_back(normed, inv_rms, grad_out):
    return inv_rms * (grad_out - normed * jnp.mean(grad_out * normed, axis=-1, keepdims=True))


GELU_C = 0.7978845608028654
GELU_K = 0.044715


def gelu_act(u):
    half = 0.5 * u
    return half + half * jnp.tanh(u * (GELU_C + (GELU_C * GELU_K) * (u * u)))


def gelu_of_half(v):
    return v + v * jnp.tanh(v * (2 * GELU_C + (8 * GELU_C * GELU_K) * (v * v)))


def gelu_slope(u):
    sq = u * u
    t = jnp.tanh(u * (GELU_C + (GELU_C * GELU_K) * sq))
    return 0.5 * (1 + t) + (0.5 * u) * (1 - t * t) * (GELU_C + (3 * GELU_C * GELU_K) * sq)


def dot(a, b):
    return jnp.dot(a, b, preferred_element_type=F32)


def dot_right_t(a, b):
    return lax.dot_general(a, b, (((1,), (1,)), ((), ())), preferred_element_type=F32)


def dot_left_t(a, b):
    return lax.dot_general(a, b, (((0,), (0,)), ((), ())), preferred_element_type=F32)


def student_layers(x_ref, gain_ref, up_ref, down_ref):
    residual = x_ref[...].astype(F32)
    unit, inv = rms_unit(residual)
    saved = []
    for j in range(up_ref.shape[0]):
        normed = (unit * gain_ref[j:j + 1, :]).astype(BF16)
        pre = dot(normed, up_ref[j])
        act = gelu_act(pre).astype(BF16)
        residual = residual + dot(act, down_ref[j])
        unit_next, inv_next = rms_unit(residual)
        saved.append((unit, inv, normed, pre, act, unit_next, inv_next))
        unit, inv = unit_next, inv_next
    return saved, unit.astype(BF16)


def teacher_kernel(feat_at, slots_w,
                   x_hbm, xs_hbm, gs_hbm, ups_hbm, dns_hbm, gain_hbm, wup_hbm, wdn_hbm,
                   feat_hbm, last_hbm, state_hbm, group_hbm,
                   xs_ref, gs_ref, ups_ref, dns_ref, gain_ref, feat_ref, last_ref, state_ref, h, nrm, wu, wd, part, got, r_own,
                   in_sems, out_sems, usem, dsem, xown, xsend, xrecv, ssem, rsem, gsend, grecv):
    me = lax.axis_index('tp')
    coords = chip_coords()
    peer = device(coords, 1 - me)
    n_layers = gain_ref.shape[0]
    rows, seq_half, d_model = x_hbm.shape

    def up_copy(layer, slot):
        return pltpu.make_async_copy(wup_hbm.at[layer], wu.at[slot], usem.at[slot])

    def down_copy(layer, slot):
        return pltpu.make_async_copy(wdn_hbm.at[layer], wd.at[slot], dsem.at[slot])

    ins = [pltpu.make_async_copy(src, dst, in_sems.at[i]) for i, (src, dst) in enumerate((
        (xs_hbm, xs_ref), (gs_hbm, gs_ref), (ups_hbm, ups_ref), (dns_hbm, dns_ref), (gain_hbm, gain_ref)))]
    mine = pl.ds(pl.multiple_of(me * seq_half, seq_half), seq_half)
    xcopy_own = pltpu.make_async_copy(x_hbm, h.at[:, mine], xown)
    for copy in ins + [xcopy_own]:
        copy.start()
    for i in range(slots_w):
        up_copy(i, i).start()
        down_copy(i, i).start()
    targets = group_targets(coords, me)
    greet(targets)
    xcopy = remote(x_hbm, h.at[:, mine], xsend, xrecv, peer)
    xcopy.start()
    for copy in ins:
        copy.wait()

    _, head_in = student_layers(xs_ref, gs_ref, ups_ref, dns_ref)
    r_own[...] = head_in
    r_copies = [remote(r_own, group_hbm.at[coords[X], me], gsend.at[i], grecv.at[i], target) for i, target in enumerate(targets)]
    for copy in r_copies:
        copy.start()
    r_keep = pltpu.make_async_copy(r_own, group_hbm.at[coords[X], me], out_sems.at[SIDE - 1])
    r_keep.start()
    xcopy.wait()
    xcopy_own.wait()

    def p_copy(ck, slot):
        return remote(part.at[ck, slot], got.at[ck, slot], ssem.at[ck, slot], rsem.at[ck, slot], peer)

    def update(ck, slot):
        p_copy(ck, slot).wait()
        total = part[ck, slot] + got[ck, slot]
        h[ck] = h[ck] + total.astype(BF16)

    def layer_step(layer, _):
        slot = lax.rem(layer, len(PAIR))
        ws = lax.rem(layer, slots_w)
        for ck in range(rows):
            first, last = ck == 0, ck == rows - 1

            @pl.when(layer > 0)
            def _():
                update(ck, 1 - slot)

            @pl.when((layer == feat_at) & (me == ck))
            def _():
                feat_ref[...] = h[ck]

            unit, _ = rms_unit(h[ck].astype(F32))
            nrm[...] = (unit * (0.5 * gain_ref[pl.ds(layer, 1), :])).astype(BF16)
            if first:
                up_copy(layer, ws).wait()
                down_copy(layer, ws).wait()
            act = gelu_of_half(dot(nrm[...], wu[ws])).astype(BF16)
            part[ck, slot] = dot(act, wd[ws])
            p_copy(ck, slot).start()
            if last:
                @pl.when(layer + slots_w < n_layers)
                def _():
                    up_copy(layer + slots_w, ws).start()
                    down_copy(layer + slots_w, ws).start()
        return 0

    lax.fori_loop(0, n_layers, layer_step, 0)
    for ck in range(rows):
        update(ck, (n_layers - 1) % len(PAIR))

        @pl.when(me == ck)
        def _():
            last_ref[...] = h[ck]

        state_ref[ck] = rms_unit(h[ck].astype(F32))[0].astype(BF16)
    outs = [pltpu.make_async_copy(src, dst, out_sems.at[i])
            for i, (src, dst) in enumerate(((feat_ref, feat_hbm), (last_ref, last_hbm), (state_ref, state_hbm)))]
    for copy in outs:
        copy.start()
    for copy in r_copies + outs + [r_keep]:
        copy.wait()


def teacher(x_teach, x_stud, gain_s, w_up_s, w_down_s, gain_t, w_up_t, w_down_t, feat_at, collective_id, slots_w=3):
    n_layers, d_model, d_ff = w_up_t.shape
    rows, seq_half, _ = x_teach.shape
    n_tok = len(PAIR) * seq_half
    n_peers = SIDE * len(PAIR) - 1
    feat = jax.ShapeDtypeStruct((n_tok, d_model), BF16)
    slots = (rows, len(PAIR))
    weights = n_layers * d_model * d_ff
    args = (x_teach, x_stud, gain_s, w_up_s, w_down_s, gain_t, w_up_t, w_down_t)
    return pl.pallas_call(
        functools.partial(teacher_kernel, feat_at, slots_w),
        out_shape=(feat, feat, jax.ShapeDtypeStruct((rows, n_tok, d_model), BF16),
                   jax.ShapeDtypeStruct((SIDE, len(PAIR)) + x_stud.shape, BF16)),
        in_specs=[IN_HBM] * len(args),
        out_specs=(IN_HBM,) * SIDE,
        scratch_shapes=[pltpu.VMEM(a.shape, a.dtype) for a in args[1:-len(PAIR)]] + [
            pltpu.VMEM((n_tok, d_model), BF16), pltpu.VMEM((n_tok, d_model), BF16), pltpu.VMEM((rows, n_tok, d_model), BF16),
            pltpu.VMEM((rows, n_tok, d_model), BF16), pltpu.VMEM((n_tok, d_model), BF16),
            pltpu.VMEM((slots_w, d_model, d_ff), BF16), pltpu.VMEM((slots_w, d_ff, d_model), BF16),
            pltpu.VMEM(slots + (n_tok, d_model), F32), pltpu.VMEM(slots + (n_tok, d_model), F32),
            pltpu.VMEM(x_stud.shape, BF16),
            DMA((len(args),)), DMA((SIDE,)), DMA((slots_w,)), DMA((slots_w,)), DMA, DMA, DMA, DMA(slots), DMA(slots), DMA((n_peers,)), DMA((n_peers,)),
        ],
        compiler_params=pltpu.CompilerParams(collective_id=collective_id, has_side_effects=True, vmem_limit_bytes=63 * MIB),
        cost_estimate=pl.CostEstimate(flops=SIDE * rows * n_tok * weights, bytes_accessed=SIDE * weights, transcendentals=0),
        name='teacher',
    )(*args)


NEG = -1e38
MAX_T, SUM_T, MAX_S, SUM_S = STATS = range(SIDE)
TEACH, STUD = PAIR


def heads_kernel(kl_coef, chunk, strip,
                 t_hbm, r_hbm, ht_hbm, hs_hbm,
                 dw_hbm, dx, kl_ref,
                 r_ref, tg, rt, ht, hs, zt, zs, mx, sm, st_send, st_all, lcol, grad_a, grad_b, dw_out,
                 ht_sem, hs_sem, t_sem, r_sem, ring_send, ring_recv, peer_send, peer_recv, st_send_sem, st_recv_sem, out_sem):
    coords = chip_coords()
    x = coords[X]
    core = lax.axis_index('tp')
    peer = device(coords, 1 - core)
    rows, n_tok, d_model = t_hbm.shape
    d_stud, cols = hs.shape
    n_tiles = cols // LANES
    blk = rows * n_tok
    n_all = SIDE * blk
    half_tile = LANES // 2
    last_x = SIDE - 1

    first_tile = n_tiles * x + core * (n_tiles * SIDE - 1)
    hs_copy = pltpu.make_async_copy(hs_hbm.at[:, pl.ds(pl.multiple_of(first_tile * LANES, LANES), cols)], hs, hs_sem)
    hs_copy.start()
    r_copy = pltpu.make_async_copy(r_hbm, r_ref, r_sem)
    r_copy.start()
    t_copy = pltpu.make_async_copy(t_hbm, tg.at[x], t_sem)
    t_copy.start()
    cut_low = (core == 1) & (x == 0)
    cut_high = (core == 0) & (x == last_x)

    def ht_copy(src, dst, n):
        return pltpu.make_async_copy(ht_hbm.at[pl.ds(src, n)], ht.at[pl.ds(dst, n)], ht_sem)

    def each_ht(act):
        @pl.when(jnp.logical_not(cut_low | cut_high))
        def _():
            act(ht_copy(pl.multiple_of(cols * x - half_tile * core, half_tile), 0, cols))

        @pl.when(cut_low)
        def _():
            act(ht_copy(0, half_tile, cols - half_tile))

        @pl.when(cut_high)
        def _():
            act(ht_copy(last_x * cols, 0, cols - half_tile))

    each_ht(lambda copy: copy.start())
    targets = group_targets(coords, core)
    greet(targets)

    far_rows = n_tok // 2

    def at(step):
        return lax.rem(x + step, SIDE)

    def ring(k, src, dst, step):
        return remote(src, dst, ring_send.at[k], ring_recv.at[k], device(moved(coords, X, step), core))

    def onward(k, step, way):
        piece = tg.at[at(step), core, pl.ds(k * far_rows, far_rows)]
        return ring(k + len(PAIR), piece, piece, way)

    def first(k, step, way):
        return ring(k, t_hbm.at[core], tg.at[at(step), core], way)

    def across(step, side):
        piece = tg.at[at(step), side]
        return remote(piece, piece, peer_send.at[step - 1], peer_recv.at[step - 1], peer)

    opposite = (LEFT, RIGHT)
    for k, way in enumerate(WAYS):
        first(k, HERE, way).start()
    r_copy.wait()
    rt[...] = r_ref[...].T
    lane = lax.broadcasted_iota(jnp.int32, (blk, LANES), 1)
    low = jnp.where(cut_low, half_tile, 0)
    high = jnp.where(cut_high, half_tile, LANES)

    def logits(kind, b, ref, product):
        peak = total = None
        for c in range(cols // chunk):
            lanes = lane_slice(c, chunk)
            z = product(lanes)
            tiles = [z[:, lane_slice(k, LANES)] for k in range(chunk // LANES)]
            if c == 0:
                tiles[0] = jnp.where(lane >= low, tiles[0], NEG)
            if lanes.stop == cols:
                tiles[-1] = jnp.where(lane < high, tiles[-1], NEG)
            for k, tile in enumerate(tiles):
                ref[b, :, lane_slice(c * len(tiles) + k, LANES)] = tile
            top = functools.reduce(jnp.maximum, tiles if peak is None else [peak] + tiles)
            sums = [jnp.exp(tile - top) for tile in tiles]
            total = functools.reduce(jnp.add, sums if peak is None else [total * jnp.exp(peak - top)] + sums)
            peak = top
        mx[kind, b] = peak
        sm[kind, b] = total

    def tokens(b):
        return pl.ds(pl.multiple_of(b * blk, blk), blk)

    def student_logits(b, _):
        states = r_ref[tokens(b), :]
        logits(STUD, b, zs, lambda lanes: dot(states, hs[:, lanes]))
        return 0

    hs_copy.wait()
    lax.fori_loop(0, FAR, student_logits, 0)
    for k, way in enumerate(WAYS):
        first(k, opposite[k], way).wait_recv()
        onward(k, opposite[k], way).start()
        across(opposite[k], core).start()
    lax.fori_loop(FAR, SIDE, student_logits, 0)
    each_ht(lambda copy: copy.wait())
    t_copy.wait()

    def teacher_logits(i, _):
        for step, turn in ((RIGHT, 1), (LEFT, 2), (FAR, 3)):
            @pl.when(i == turn)
            def _():
                if step == LEFT:
                    for k, way in enumerate(WAYS):
                        onward(k, FAR, way).wait_recv()
                    across(FAR, core).start()
                across(step, 1 - core).wait_recv()

        b = at(jnp.where(i < FAR, i, SIDE + 1 - i))
        states = tg[b].reshape(blk, d_model)
        logits(TEACH, b, zt, lambda lanes: dot_right_t(states, ht[lanes, :]))
        return 0

    lax.fori_loop(0, SIDE, teacher_logits, 0)

    def merge(b, _):
        out = jnp.zeros((blk, LANES), F32)
        for kind in PAIR:
            peak = jnp.max(mx[kind, b], axis=-1, keepdims=True)
            total = jnp.sum(sm[kind, b] * jnp.exp(mx[kind, b] - peak), axis=-1, keepdims=True)
            out = jnp.where(lane == 2 * kind, peak, jnp.where(lane == 2 * kind + 1, total, out))
        st_send[:, tokens(b)] = out.T[:SUBS, :]
        return 0

    lax.fori_loop(0, SIDE, merge, 0)
    n_peers = len(targets)
    stats = [remote(st_send, st_all.at[i], st_send_sem.at[i], st_recv_sem.at[i], target) for i, target in enumerate(targets)]
    for copy in stats:
        copy.start()
    st_all[n_peers] = st_send[...]
    for copy in stats:
        copy.wait()
    sub = lax.broadcasted_iota(jnp.int32, (LANES, n_all), 0)
    both = jnp.zeros((LANES, n_all), F32)
    for kind in PAIR:
        peaks, totals = st_all[:, 2 * kind, :], st_all[:, 2 * kind + 1, :]
        peak = jnp.max(peaks, axis=0, keepdims=True)
        norm = peak + jnp.log(jnp.sum(totals * jnp.exp(peaks - peak), axis=0, keepdims=True))
        both = jnp.where(sub == kind, norm, both)
    lcol[...] = both.T
    kl_ref[...] = jnp.zeros_like(kl_ref)
    dx[...] = jnp.zeros_like(dx)

    n_steps = cols // chunk

    def lanes_of(j):
        return pl.ds(pl.multiple_of(j * chunk, LANES), chunk)

    def logit_grads(j, dst):
        lanes = lanes_of(j)
        total = kl_ref[...]
        for i in range(n_all // strip):
            b, k = divmod(i, blk // strip)
            tok, row = lane_slice(i, strip), lane_slice(k, strip)
            log_pt = zt[b, row, lanes] - lcol[tok, TEACH:TEACH + 1]
            log_ps = zs[b, row, lanes] - lcol[tok, STUD:STUD + 1]
            pt = jnp.exp(log_pt)
            dst[tok, :] = (kl_coef * (jnp.exp(log_ps) - pt)).astype(BF16)
            kl = pt * (log_pt - log_ps)
            kl = functools.reduce(jnp.add, [kl[:, lane_slice(k, LANES)] for k in range(chunk // LANES)])
            total = total + functools.reduce(jnp.add, [kl[lane_slice(k, SUBS)] for k in range(strip // SUBS)])
        kl_ref[...] = total

    def out_copy(j):
        return pltpu.make_async_copy(dw_out, dw_hbm.at[:, lanes_of(j)], out_sem)

    def products(j, src):
        dw_out[...] = dot(rt[...], src[...])
        out_copy(j).start()
        dx[...] += dot_right_t(src[...], hs[:, lanes_of(j)])

    def two_steps(i, _):
        j = 2 * i

        @pl.when(i > 0)
        def _():
            out_copy(j - 1).wait()

        logit_grads(j + 1, grad_b)
        products(j, grad_a)
        out_copy(j).wait()
        logit_grads(j + 2, grad_a)
        products(j + 1, grad_b)
        return 0

    logit_grads(0, grad_a)
    lax.fori_loop(0, n_steps // 2, two_steps, 0)
    out_copy(n_steps - 2).wait()
    products(n_steps - 1, grad_a)
    for k, way in enumerate(WAYS):
        first(k, HERE, way).wait_send()
        onward(k, opposite[k], way).wait_send()
    for step in (RIGHT, FAR, LEFT):
        across(step, core).wait_send()
    out_copy(n_steps - 1).wait()


def heads(states, stud_all, head_t, head_s, kl_coef, collective_id, chunk=768, strip=16):
    rows, n_tok, d_model = states.shape
    n_all, d_stud = stud_all.shape
    cols = -(-head_t.shape[1] // (LANES * SIDE)) * LANES
    blk = rows * n_tok
    n_peers = SIDE * len(PAIR) - 1
    v = pltpu.VMEM
    hops = (SIDE - 1,)
    return pl.pallas_call(
        functools.partial(heads_kernel, kl_coef, chunk, strip),
        out_shape=(jax.ShapeDtypeStruct((d_stud, cols), F32), jax.ShapeDtypeStruct((n_all, d_stud), F32),
                   jax.ShapeDtypeStruct((SUBS, LANES), F32)),
        in_specs=[IN_HBM] * SIDE,
        out_specs=(IN_HBM, IN_VMEM, IN_VMEM),
        scratch_shapes=[
            v((n_all, d_stud), BF16), v((SIDE, rows, n_tok, d_model), BF16), v((d_stud, n_all), BF16), v((cols, d_model), BF16), v((d_stud, cols), BF16),
            v((SIDE, blk, cols), F32), v((SIDE, blk, cols), F32),
            v((len(PAIR), SIDE, blk, LANES), F32), v((len(PAIR), SIDE, blk, LANES), F32),
            v((SUBS, n_all), F32), v((n_peers + 1, SUBS, n_all), F32), v((n_all, LANES), F32),
            v((n_all, chunk), BF16), v((n_all, chunk), BF16), v((d_stud, chunk), F32),
            DMA, DMA, DMA, DMA, DMA((SIDE,)), DMA((SIDE,)), DMA(hops), DMA(hops), DMA((n_peers,)), DMA((n_peers,)), DMA,
        ],
        compiler_params=pltpu.CompilerParams(collective_id=collective_id, has_side_effects=True, vmem_limit_bytes=63 * MIB),
        cost_estimate=pl.CostEstimate(flops=d_model * n_all * cols, bytes_accessed=d_model * cols, transcendentals=0),
        name='heads',
    )(states, stud_all, head_t.T, head_s)


class RingSum:
    def __init__(self, coords, core, src, dims, order, lanes, bufs, loads=None):
        self.coords, self.core, self.order, self.lanes = coords, core, order, lanes
        self.loads = src if loads is None else loads
        self.phases = []
        for axis, (half, full, mid, send, recv) in zip(order, bufs):
            self.phases.append((src, dims, axis, half, full, mid, send, recv))
            src, dims = mid, tuple(d for d in dims if d != axis)

    @staticmethod
    def shapes(dims, order, rows, width):
        out = []
        for _ in order:
            dims = dims[1:]
            lead = (SIDE,) * len(dims)
            part = (SIDE // 2,) + lead[1:] + (rows, width) if lead else (rows, -(-width // (2 * LANES)) * LANES)
            out += [pltpu.VMEM(PAIR_DIM + part, F32), pltpu.VMEM(PAIR_DIM + lead + (rows, width), F32),
                    pltpu.VMEM(lead + (rows, width), F32), DMA((3 * len(PAIR),)), DMA((3 * len(PAIR),))]
        return out

    def place(self, axis, step):
        return lax.rem(self.coords[axis] + step, SIDE)

    def split(self, k, side):
        _, dims, _, half, full, _, _, _ = self.phases[k]
        width, cut = full.shape[-1], half.shape[-1]
        if len(dims) > 1:
            return (pl.ds(side * (SIDE // 2), SIDE // 2),) + (slice(None),) * (len(dims) - 2), (0, width)
        return (), ((cut, width - cut) if side else (0, cut))

    def pick(self, k, at, side):
        src, dims, axis = self.phases[k][:3]
        lead, (lo, n) = ((slice(None),) * (len(dims) - 1), (0, self.phases[k][4].shape[-1])) if side is None else self.split(k, side)
        lead = list(lead)
        lead.insert(dims.index(axis), at)
        base = self.lanes if k == 0 else 0
        return src, tuple(lead) + (slice(None), pl.ds(base + lo, n))

    def held(self, k, at, side):
        src, idx = self.pick(k, at, side)
        return (src if k else self.loads), idx

    def copy(self, k, turn, d):
        _, _, axis, half, full, _, send, recv = self.phases[k]
        way = WAYS[d]
        i = turn * len(PAIR) + d
        side = d if turn != 1 else 1 - d
        lead, (lo, n) = self.split(k, side)
        window = (slice(None), pl.ds(lo, n))
        if turn == 0:
            ref, idx = self.pick(k, self.place(axis, FAR), side)
            src, dst = ref.at[idx], half.at[d, ..., pl.ds(0, n)]
        elif turn == 1:
            ref, idx = self.pick(k, self.place(axis, way), side)
            src, dst = ref.at[idx], full.at[(d,) + lead + window]
        else:
            src, dst = half.at[d, ..., pl.ds(0, n)], full.at[(d,) + lead + window]
        return remote(src, dst, send.at[i], recv.at[i], device(moved(self.coords, axis, way), self.core))

    def start(self, k, turns=PAIR):
        for turn in turns:
            for d in PAIR:
                self.copy(k, turn, d).start()

    def middle(self, k):
        _, _, axis, half, _, _, _, _ = self.phases[k]
        for d in PAIR:
            self.copy(k, 0, d).wait_recv()
            ref, idx = self.held(k, self.place(axis, WAYS[d]), d)
            n = self.split(k, d)[1][1]
            half[d, ..., :n] = half[d, ..., :n] + ref[idx]
            self.copy(k, len(PAIR), d).start()

    def finish(self, k):
        _, _, axis, _, full, mid, _, _ = self.phases[k]
        for d in PAIR:
            for turn in (1, len(PAIR)):
                self.copy(k, turn, d).wait_recv()
        ref, idx = self.held(k, self.coords[axis], None)
        mid[...] = ref[idx] + full[0] + full[1]

    def drain(self):
        for k in range(len(self.order)):
            for turn in range(3):
                for d in PAIR:
                    self.copy(k, turn, d).wait_send()


PAIR_DIM = (len(PAIR),)


def small_places(n_feat, d_in, d_mid, d_teach):
    groups_up = d_in // SUBS
    yz = SIDE * SIDE
    per_up = n_feat * groups_up // yz
    lanes_u, lanes_p = d_mid // SIDE, d_teach // SIDE
    per_p = groups_up // yz
    span = per_up // per_p * lanes_u + lanes_p
    return groups_up, yz, per_up, lanes_u, lanes_p, per_p, span


def reduce_kernel(feat_coef, kl_coef, small_parts,
                  dw_hbm, feat_a_hbm, feat_b_hbm, xs_hbm, gs_hbm, ups_hbm, dns_hbm, proj_hbm, dx_ref, kl_ref,
                  own, dw, feat_a, feat_b, xs_ref, gs_ref, ups_ref, dns_ref, proj_ref, in_sems, small, got, part_in, swap_send, swap_recv, in_send, in_recv, *bufs):
    coords = chip_coords()
    core = lax.axis_index('tp')
    peer = device(coords, 1 - core)
    loads = [pltpu.make_async_copy(src, dst, in_sems.at[i]) for i, (src, dst) in enumerate((
        (dw_hbm, dw), (feat_a_hbm, feat_a), (feat_b_hbm, feat_b), (xs_hbm, xs_ref), (gs_hbm, gs_ref), (ups_hbm, ups_ref),
        (dns_hbm, dns_ref), (proj_hbm, proj_ref)))]
    dw_load = loads.pop(0)
    for copy in loads + [dw_load]:
        copy.start()
    greet(near_targets(coords, core))
    cols = dw.shape[-1]
    bufs = list(bufs)

    def take(n):
        out = [tuple(bufs[5 * i:5 * i + 5]) for i in range(n)]
        del bufs[:5 * n]
        return out

    head_jobs = [RingSum(coords, core, dw_hbm, (Y, Z), order, k * (cols // 2), take(2), dw) for k, order in enumerate(((Y, Z), (Z, Y)))]
    in_job = RingSum(coords, core, part_in, (X,), (X,), 0, take(1))
    for job in head_jobs:
        job.start(0)
    in_swap = remote(dx_ref.at[:, 1 - core], part_in, in_send, in_recv, peer)
    in_swap.start()

    in_swap.wait()
    part_in[...] = part_in[...] + dx_ref[:, core]
    in_job.start(0)

    for copy in loads:
        copy.wait()
    saved, _ = student_layers(xs_ref, gs_ref, ups_ref, dns_ref)
    feats = (feat_a, feat_b)
    n_feat, d_in, d_mid = ups_ref.shape
    groups, yz, per_up, lanes_u, lanes_p, per_p, span = small_places(n_feat, d_in, d_mid, proj_ref.shape[-1])
    two = per_up // per_p
    err_rows = jnp.zeros((SUBS, LANES), F32)
    out_grads, gain_rows = [], []

    def put(keep, chip_x, group, per, base, lanes, value):
        block, g = divmod(group, per)
        y, z = divmod(block, SIDE)
        part, q = divmod(g, per // per_p)
        small[keep, chip_x, y, z, :, part * span + base + q * lanes:part * span + base + q * lanes + lanes] = value

    half_side = SIDE // n_feat
    swaps = []

    def swap(k, rows_y, base, lanes):
        for p in PARTS:
            window = (slice(None), rows_y, slice(None), slice(None), pl.ds(p * span + base, lanes))
            copy = remote(small.at[(1 - core,) + window], got.at[window], swap_send.at[k, p], swap_recv.at[k, p], peer)
            copy.start()
            swaps.append((copy, window))

    for j in range(n_feat):
        proj_in = saved[j][5].astype(BF16)
        err = dot(proj_in, proj_ref[j]) - feats[j][...].astype(F32)
        sq = err * err
        sq = functools.reduce(jnp.add, [sq[:, lane_slice(k, LANES)] for k in range(sq.shape[1] // LANES)])
        err_rows = err_rows + functools.reduce(jnp.add, [sq[lane_slice(k, SUBS)] for k in range(sq.shape[0] // SUBS)])
        err_grad = ((2 * feat_coef) * err).astype(BF16)
        g_proj = dot_left_t(proj_in, err_grad)
        for i in range(groups):
            for cx in range(SIDE):
                put(j, cx, i, per_p, two * lanes_u, lanes_p, g_proj[lane_slice(i, SUBS), lane_slice(cx, lanes_p)])
        out_grads.append(dot_right_t(err_grad, proj_ref[j]))
    swap(n_feat, slice(None), two * lanes_u, lanes_p)
    in_job.middle(0)
    in_job.finish(0)
    dw_load.wait()
    for job in head_jobs:
        job.middle(0)
    out_grads[-1] = out_grads[-1] + in_job.phases[-1][5][...]
    resid_grad = None
    for j in reversed(range(n_feat)):
        unit, inv, normed, pre, act, unit_next, inv_next = saved[j]
        step_grad = rms_back(unit_next, inv_next, out_grads[j])
        resid_grad = step_grad if resid_grad is None else resid_grad + step_grad
        resid_bf = resid_grad.astype(BF16)
        g_down = dot_left_t(act, resid_bf)
        n_down = d_mid // SUBS
        for i in range(n_down):
            cx, rest = divmod(i, groups)
            put(1, cx, j * groups + rest, per_up, 0, lanes_u, g_down[lane_slice(i, SUBS), :])
        pre_grad = (gelu_slope(pre) * dot_right_t(resid_bf, dns_ref[j])).astype(BF16)
        g_up = dot_left_t(normed, pre_grad)
        for i in range(groups):
            for cx in range(SIDE):
                put(0, cx, j * groups + i, per_up, 0, lanes_u, g_up[lane_slice(i, SUBS), lane_slice(cx, lanes_u)])
        swap(j, pl.ds(half_side * j, half_side), 0, two * lanes_u)
        norm_grad = dot_right_t(pre_grad, ups_ref[j])
        g_gain = jnp.sum(norm_grad * unit, axis=0, keepdims=True)
        gain_rows = [g_gain[:, lane_slice(k, LANES)] for k in range(d_in // LANES)] + gain_rows
        if j > 0:
            resid_grad = resid_grad + rms_back(unit, inv, norm_grad * gs_ref[j:j + 1, :])

    lo = 0
    small_jobs = []
    for order, width in zip(ORDERS, small_parts):
        small_jobs.append(RingSum(coords, core, got, AXES, order, lo, take(3)))
        lo += width
    for copy, window in swaps:
        copy.wait()
        got[window] = got[window] + small[(core,) + window]
    for turn in PAIR:
        for job in small_jobs:
            job.start(0, (turn,))
    for job in head_jobs:
        job.finish(0)
        job.start(1)
    for job in head_jobs:
        job.middle(1)
    for job in small_jobs:
        job.middle(0)
    for job in head_jobs:
        job.finish(1)
    for job in small_jobs:
        job.finish(0)
        job.start(1)
    for k in (1, 2):
        for job in small_jobs:
            job.middle(k)
        for job in small_jobs:
            job.finish(k)
            if k < 2:
                job.start(k + 1)
    for p in PARTS:
        for k, job in enumerate(head_jobs):
            own[p, :, lane_slice(k, cols // 2)] = job.phases[-1][5][lane_slice(p, SUBS), :]
    pieces = [(order_i, t) for order_i, width in enumerate(small_parts) for t in range(width // LANES)]
    for n, (which, t) in enumerate(pieces):
        p, at = divmod(n * LANES, span)
        own[p, :, cols + at:cols + at + LANES] = small_jobs[which].phases[-1][5][:, lane_slice(t, LANES)]
    loss_row = jnp.sum(feat_coef * err_rows + kl_coef * kl_ref[...], axis=0, keepdims=True)
    for p in PARTS:
        own[p, :, cols + span:] = jnp.zeros((SUBS, LANES), F32)
    for i, row in enumerate(gain_rows + [loss_row]):
        own[0, i:i + 1, cols + span:] = row
    for job in head_jobs + small_jobs + [in_job]:
        job.drain()


def reduce_grads(dw, dx, feats, x_stud, gain_s, w_up_s, w_down_s, proj_s, kl_tiles, feat_coef, kl_coef, collective_id,
                 small_parts=(1280, 896, 896)):
    rows, cols = dw.shape[2:]
    span = sum(small_parts) // len(PARTS)
    width = cols // 2
    xs_shape = x_stud.shape
    args = (dw, *feats, x_stud, gain_s, w_up_s, w_down_s, proj_s)
    scratch = [pltpu.VMEM(a.shape, a.dtype) for a in args]
    scratch += [DMA((len(args),)), pltpu.VMEM((len(PAIR), SIDE, SIDE, SIDE, SUBS, sum(small_parts)), F32),
               pltpu.VMEM((SIDE, SIDE, SIDE, SUBS, sum(small_parts)), F32), pltpu.VMEM((SIDE,) + xs_shape, F32),
               DMA((SIDE, SIDE)), DMA((SIDE, SIDE)), DMA, DMA]
    for _ in PAIR:
        scratch += RingSum.shapes((Y, Z), (Y, Z), rows, width)
    scratch += RingSum.shapes((X,), (X,), *xs_shape)
    for part in small_parts:
        scratch += RingSum.shapes(AXES, AXES, SUBS, part)
    return pl.pallas_call(
        functools.partial(reduce_kernel, feat_coef, kl_coef, small_parts),
        out_shape=jax.ShapeDtypeStruct((len(PARTS), SUBS, cols + span + LANES), F32),
        in_specs=[IN_HBM] * len(args) + [IN_VMEM] * len(PAIR),
        out_specs=IN_VMEM,
        scratch_shapes=scratch,
        compiler_params=pltpu.CompilerParams(collective_id=collective_id, has_side_effects=True, vmem_limit_bytes=63 * MIB),
        cost_estimate=pl.CostEstimate(flops=MIB * MIB, bytes_accessed=dw.size, transcendentals=0),
        name='reduce',
    )(*args, dx, kl_tiles)


ALL = pl.ds(0, SIDE)
WHOLE, LOW, HIGH = range(SIDE - 1)
SOURCE = (LEFT, RIGHT)
ARRIVAL = (HERE, LEFT, RIGHT, FAR)


def gather_kernel(cut, own_ref, full, own_sem, send_sem, recv_sem, peer_send, peer_recv):
    coords = chip_coords()
    core = lax.axis_index('tp')
    peer = device(coords, 1 - core)
    width = own_ref.shape[-1]
    widths = (width, width - LANES, width - LANES)
    here = [pltpu.make_async_copy(own_ref.at[p], full.at[(core,) + coords + (p,)], own_sem.at[p]) for p in PARTS]
    for copy in here:
        copy.start()
    greet(near_targets(coords, core))

    def lanes(part, span):
        return pl.ds(cut if span == HIGH else 0, (widths[part], cut, widths[part] - cut)[span])

    def block(part, steps, span=WHOLE):
        idx = list(coords)
        for axis, step in zip(ORDERS[part], steps):
            idx[axis] = ALL if step is ALL else lax.rem(coords[axis] + step, SIDE)
        return full.at[(core,) + tuple(idx) + (part, slice(None), lanes(part, span))]

    def steps_of(phase, sub, step):
        return ((step,), (sub, step), (ALL, sub, step))[phase]

    def ring(part, phase, sub, slot, step, span):
        dst = block(part, steps_of(phase, sub, step), span)
        mine = step == HERE and (phase == 0 or (phase == 1 and sub == HERE))
        src = own_ref.at[part, :, lanes(part, span)] if mine else dst
        at = (part, phase, sub, slot)
        return remote(src, dst, send_sem.at[at], recv_sem.at[at], device(moved(coords, ORDERS[part][phase], WAYS[slot % 2]), core))

    def first(part, phase, sub, d, step):
        return ring(part, phase, sub, d, step, WHOLE)

    def onward(part, phase, sub, d, step):
        return ring(part, phase, sub, d + 2, step, (LOW, HIGH)[d])

    def send(part, phase, sub):
        for d in PAIR:
            first(part, phase, sub, d, HERE).start()

    def relay(part, phase, sub, d):
        first(part, phase, sub, d, SOURCE[d]).wait_recv()
        onward(part, phase, sub, d, SOURCE[d]).start()

    def far_in(part, phase, sub):
        for d in PAIR:
            onward(part, phase, sub, d, FAR).wait_recv()

    def across(part, phase, sub, step):
        dst = block(part, ((step,), (ALL, step), (ALL, sub, step))[phase])
        src = own_ref.at[part, :, lanes(part, WHOLE)] if phase == 0 and step == HERE else dst
        at = (part, phase, sub, step)
        return remote(src, dst, peer_send.at[at], peer_recv.at[at], peer)

    for part in PARTS:
        send(part, 0, HERE)
    for part in PARTS:
        send(part, 1, HERE)
        across(part, 0, HERE, HERE).start()
    for part in PARTS:
        for d in PAIR:
            relay(part, 0, HERE, d)
            send(part, 1, SOURCE[d])
            across(part, 0, HERE, SOURCE[d]).start()
    for part in PARTS:
        far_in(part, 0, HERE)
        send(part, 1, FAR)
        across(part, 0, HERE, FAR).start()
        here[part].wait()
        send(part, 2, HERE)
    for sub in ARRIVAL:
        for part in PARTS:
            for d in PAIR:
                relay(part, 1, sub, d)
                if sub == FAR:
                    send(part, 2, SOURCE[d])
                    across(part, 1, HERE, SOURCE[d]).start()
    for part in PARTS:
        for sub in ARRIVAL:
            far_in(part, 1, sub)
        send(part, 2, FAR)
        across(part, 1, HERE, FAR).start()
    for sub in ARRIVAL:
        for part in PARTS:
            for d in PAIR:
                relay(part, 2, sub, d)
                across(part, 2, sub, SOURCE[d]).start()
    for sub in ARRIVAL:
        for part in PARTS:
            far_in(part, 2, sub)
            across(part, 2, sub, FAR).start()
    for part in PARTS:
        for phase in AXES:
            for sub in ARRIVAL if phase else (HERE,):
                for d in PAIR:
                    first(part, phase, sub, d, HERE).wait_send()
                    onward(part, phase, sub, d, SOURCE[d]).wait_send()
                for step in ARRIVAL if phase == 0 else (LEFT, RIGHT, FAR):
                    if phase != 1 or sub == HERE:
                        across(part, phase, sub, step).wait()


def gather_blocks(own, cut, collective_id):
    sems = DMA((len(PARTS), len(AXES), SIDE, SIDE))
    return pl.pallas_call(
        functools.partial(gather_kernel, cut),
        out_shape=pltpu.VMEM((len(PAIR), SIDE, SIDE, SIDE) + own.shape, F32),
        in_specs=[IN_VMEM],
        out_specs=IN_HBM,
        scratch_shapes=[DMA((len(PARTS),)), sems, sems, sems, sems],
        compiler_params=pltpu.CompilerParams(collective_id=collective_id, has_side_effects=True, vmem_limit_bytes=MIB),
        cost_estimate=pl.CostEstimate(flops=MIB * MIB, bytes_accessed=SIDE * LANES * own.size, transcendentals=0),
        name='gather',
    )(own)


def place_kernel(n_head, lanes_u, lanes_p,
                 full, head, up, down, proj, gain, loss,
                 total, edge, head_sem, edge_sem, up_sem, down_sem, narrow_sem):
    last_x = SIDE - 1
    per = up.shape[3]
    n_feat, _, half_side = down.shape[:3]
    copy = pltpu.make_async_copy
    narrow_at = n_head + per * lanes_u
    copies = []
    for c in CORES:
        for x in range(SIDE):
            src = full.at[c, x]
            lo = LANES if (c, x) == PAIR[::-1] else 0
            hi = n_head - LANES if (c, x) == (0, last_x) else n_head
            at = (c * SIDE + x) * n_head - c * LANES
            copies.append(copy(src.at[:, :, :, :, pl.ds(lo, hi - lo)], head.at[:, :, :, :, pl.ds(at + lo, hi - lo)], head_sem.at[c, x]))
            for q in range(per):
                lanes = pl.ds(n_head + q * lanes_u, lanes_u)
                if c:
                    for j in range(n_feat):
                        copies.append(copy(src.at[pl.ds(j * half_side, half_side), :, :, :, lanes], down.at[j, x, :, :, :, q],
                                           down_sem.at[x, q, j]))
                else:
                    copies.append(copy(src.at[:, :, :, :, lanes], up.at[:, :, :, q, :, pl.ds(x * lanes_u, lanes_u)], up_sem.at[x, q]))
            copies.append(copy(src.at[:, :, :, :, pl.ds(narrow_at, lanes_p)], proj.at[c, :, :, :, :, pl.ds(x * lanes_p, lanes_p)],
                               narrow_sem.at[c, x]))
    for one in copies:
        one.start()
    edge[...] = full[0, last_x, :, :, :, :, n_head - LANES:n_head] + full[1, 0, :, :, :, :, :LANES]
    edge_copy = copy(edge, head.at[:, :, :, :, pl.ds(SIDE * n_head - LANES, LANES)], edge_sem)
    edge_copy.start()
    tiles = full[:, :, :, :, 0, :, narrow_at + lanes_p:narrow_at + lanes_p + LANES]
    total[...] = jnp.sum(tiles.reshape(-1, SUBS, LANES), axis=0)
    rows = gain.shape[1] // LANES
    for j in range(n_feat):
        for k in range(rows):
            gain[j:j + 1, lane_slice(k, LANES)] = total[j * rows + k:j * rows + k + 1, :]
    loss[...] = jnp.sum(total[n_feat * rows:n_feat * rows + 1, :], axis=-1, keepdims=True)
    edge_copy.wait()
    for one in copies:
        one.wait()


def place_blocks(full, n_head, lanes_u, lanes_p, vocab, gain_shape):
    n_part, subs, _ = full.shape[4:]
    per = len(PAIR)
    n_feat = gain_shape[0]
    pair = (len(PAIR),)
    owners = pair + (SIDE,)
    yz = (SIDE, SIDE)
    shapes = (yz + (n_part, subs, vocab), yz + (n_part, per, subs, SIDE * lanes_u), (n_feat, SIDE, SIDE // n_feat, SIDE, n_part, per, subs, lanes_u),
              pair + yz + (n_part, subs, SIDE * lanes_p), gain_shape, (1, 1))
    return pl.pallas_call(
        functools.partial(place_kernel, n_head, lanes_u, lanes_p),
        out_shape=tuple(jax.ShapeDtypeStruct(s, F32) for s in shapes),
        in_specs=[IN_VMEM],
        out_specs=(IN_HBM,) * SIDE + (IN_VMEM, IN_VMEM),
        scratch_shapes=[pltpu.VMEM((subs, LANES), F32), pltpu.VMEM(yz + (n_part, subs, LANES), F32), DMA(owners), DMA,
                        DMA((SIDE, per)), DMA((SIDE, per, n_feat)), DMA(owners)],
        compiler_params=pltpu.CompilerParams(has_side_effects=True, vmem_limit_bytes=MIB),
        name='place',
    )(pltpu.with_memory_space_constraint(full, pltpu.VMEM))


def solution(mesh):
    n_dev = mesh.shape['dp'] * mesh.shape['tp']

    def local_step(x_teach, x_stud, w_up_t, w_down_t, gain_t, head_t, w_up_s, w_down_s, gain_s, proj_s, head_s):
        n_feat, d_in, d_mid = w_up_s.shape
        d_teach = proj_s.shape[-1]
        n_tokens = x_stud.shape[0] * x_stud.shape[1] * n_dev
        feat_coef = 1.0 / (n_feat * n_tokens * d_teach)
        kl_coef = 1.0 / n_tokens
        xs = x_stud[0]
        feat_one, feat_two, states, stud_all = teacher(x_teach, xs, gain_s, w_up_s, w_down_s, gain_t, w_up_t, w_down_t,
                                                       w_up_t.shape[0] // n_feat, 0)
        head_part, in_part, kl_tiles = heads(states, stud_all.reshape(-1, d_in), head_t, head_s, kl_coef, 1)
        cols = head_part.shape[1]
        own = reduce_grads(head_part.reshape(SIDE, SIDE, -1, cols), in_part.reshape((SIDE, -1) + xs.shape), (feat_one, feat_two), xs, gain_s, w_up_s, w_down_s,
                           proj_s, kl_tiles, feat_coef, kl_coef, 2)
        blocks = gather_blocks(own, 20 * LANES, 3)
        head_grad, up, down, proj, gain, loss = place_blocks(blocks, cols, d_mid // SIDE, d_teach // SIDE, head_s.shape[1], gain_s.shape)
        return (loss.reshape(()), up.reshape(w_up_s.shape), down.reshape(w_down_s.shape), gain,
                proj.reshape(proj_s.shape), head_grad.reshape(head_s.shape))

    in_specs = (P('dp', 'tp', None), P(('dp', 'tp'), None, None), P(None, None, 'tp'), P(None, 'tp', None),
                P(), P(None, 'tp'), P(), P(), P(), P(), P())
    out_specs = (P(), P(), P(), P(), P(), P())
    return jax.shard_map(local_step, mesh=mesh, in_specs=in_specs, out_specs=out_specs, check_vma=False)
```
